32 devices in a mesh: tm: 4 (over y, x), space: 8 (over z, core).
Axes of the slice: x: 2, y: 2, z: 4, core: 2. Of those that a mesh axis runs over, the one named last changes fastest.
Arguments:
- hidden_in: bfloat16 [8, 16, 32, 5120], P('tm', 'space'), may hold values from -6 to 6
- queries: bfloat16 [8, 16, 32, 5120], P('tm', 'space'), may hold values from -250 to 250
- keys: bfloat16 [8, 16, 32, 5120], P('tm', 'space'), may hold values from -250 to 250
- values: bfloat16 [8, 16, 32, 5120], P('tm', 'space'), may hold values from -6 to 6
- query_gain: float32 [5120], replicated, may hold values from 0.5 to 3
- key_gain: float32 [5120], replicated, may hold values from 0.5 to 3
- reach_time: int32 [40], replicated, may hold values from 0 to 1
- reach_rows: int32 [40], replicated, may hold values from 0 to 1
- reach_cols: int32 [40], replicated, may hold values from 0 to 2
- out_weight: bfloat16 [5120, 5120], P('space', 'tm'), may hold values from -0.25 to 0.25
- gate: float32 [5120], replicated, may hold values from -1.5 to 1.5
Outputs:
- output: bfloat16 [8, 16, 32, 5120], P('tm', 'space')
The draws below stay inside these ranges and needn't reach their ends.
All inputs are finite; a program needn't handle non-finite values.
Results may differ from the reference program's by a relative error of at most 0.013.
The reference program's roundings to bfloat16 on the way (of `query_norm`, `key_norm`, `rounded` and `attention`) count: a program that leaves them out, or rounds other values in their place, can miss the bound.
Values may be sent and summed in bfloat16 or wider, within the bound.
A program may use at most 128 MiB of HBM per device.

```python
import math
import jax
import jax.numpy as jnp
from jax import lax

D = 5120
HEADS = 40
FR = 2
RH = 2
NW = 32
TW = 8
INNER = 5120
NF = 8
NH = 16


def lifted_field(key, salt):
    base = jax.random.normal(jax.random.fold_in(key, salt), (NF, NH, NW, INNER), jnp.float32)
    return jnp.clip(base, -6.0, 6.0)


def draw_queries(key, part):
    field = lifted_field(key, 11)
    return jnp.clip(field, -250.0, 250.0).astype(jnp.bfloat16)


def draw_keys(key, part):
    field = lifted_field(key, 21)
    return jnp.clip(field, -250.0, 250.0).astype(jnp.bfloat16)


def plant(result, own_key, least, largest):
    longest = result.shape.index(max(result.shape))
    spots = []
    for shift in (0, 1):
        where = [jax.random.randint(jax.random.fold_in(own_key, axis), (), 0, length) for axis, length in enumerate(result.shape)]
        where[longest] = (where[longest] + shift) % result.shape[longest]
        spots.append(tuple(where))
    return result.at[spots[0]].set(least).at[spots[1]].set(largest)


def shard_levels(rng, shape, shards, low, top_value):
    loudness = 1.0
    for position, shards_of in shards:
        steps = jax.random.uniform(jax.random.fold_in(jax.random.fold_in(rng, 6), position), (shards_of,), jnp.float32, low / len(shards), top_value / len(shards))
        loudness = loudness * jnp.repeat(jnp.exp(steps), shape[position] // shards_of).reshape((-1,) + (1,) * (len(shape) - 1 - position))
    return loudness


def gaussian(rng, shape, scale, limit, split=(), held_as=jnp.bfloat16):
    result = scale * jax.random.normal(rng, shape, jnp.float32)
    if split:
        result = result * shard_levels(rng, shape, split, -0.22, 0.18)
    return jnp.clip(result, -limit, limit).astype(held_as)


def setup_inputs(seed: int = 0) -> dict:
    key_list = jax.random.split(jax.random.key(seed), 12)
    hidden_in = gaussian(key_list[0], (NF, NH, NW, D), 1.0, 6.0, ((0, 4), (1, 8)))
    queries = draw_queries(jax.random.fold_in(key_list[11], 71), 0)
    keys = draw_keys(jax.random.fold_in(key_list[11], 71), 0)
    values = gaussian(key_list[3], (NF, NH, NW, INNER), 1.0, 6.0, ((0, 4), (1, 8)))
    query_gain = jnp.clip(jnp.exp(jax.random.uniform(key_list[4], (INNER,), jnp.float32, math.log(0.5), math.log(3.0))), 0.5, 3.0)
    key_gain = jnp.clip(jnp.exp(jax.random.uniform(key_list[5], (INNER,), jnp.float32, math.log(0.5), math.log(3.0))), 0.5, 3.0)
    reach_time = plant(jax.random.randint(key_list[6], (HEADS,), 0, 2), jax.random.fold_in(key_list[6], 1), 0, 1).astype(jnp.int32)
    reach_rows = plant(jax.random.randint(key_list[7], (HEADS,), 0, 2), jax.random.fold_in(key_list[7], 1), 0, 1).astype(jnp.int32)
    reach_cols = plant(jax.random.randint(key_list[8], (HEADS,), 0, 3), jax.random.fold_in(key_list[8], 1), 0, 2).astype(jnp.int32)
    out_weight = gaussian(key_list[9], (INNER, D), (INNER // 8) ** -0.5, 0.25, ((0, 8), (1, 4)))
    gate = jnp.clip(jax.random.uniform(key_list[10], (D,), jnp.float32, -1.5, 1.5), -1.5, 1.5)
    return dict(hidden_in=hidden_in, queries=queries, keys=keys, values=values, query_gain=query_gain, key_gain=key_gain, reach_time=reach_time, reach_rows=reach_rows, reach_cols=reach_cols, out_weight=out_weight, gate=gate)


def normalize(source, gain):
    values_f = source.astype(jnp.float32)
    mean_square = lax.optimization_barrier(jnp.mean(values_f * values_f, axis=-1, keepdims=True))
    return (values_f * lax.rsqrt(mean_square + 1e-06) * gain).astype(jnp.bfloat16)

def attend(query_block, key_region, value_region, first_frame, first_row, frame_count, row_count, reach_time, reach_rows, reach_cols):
    frames_here, rows_here, columns, inner = query_block.shape
    head_count = reach_time.shape[0]
    head_width = inner // head_count
    query_flat = query_block.reshape(-1, head_count, head_width).astype(jnp.float32)
    key_flat = key_region.reshape(-1, head_count, head_width).astype(jnp.float32)
    value_flat = value_region.reshape(-1, head_count, head_width).astype(jnp.float32)
    frame_q = first_frame + jnp.arange(frames_here, dtype=jnp.int32)
    frame_k = first_frame - 1 + jnp.arange(frames_here + 2, dtype=jnp.int32)
    row_q = first_row + jnp.arange(rows_here, dtype=jnp.int32)
    row_k = first_row - 1 + jnp.arange(rows_here + 2, dtype=jnp.int32)
    tiles = jnp.arange(columns, dtype=jnp.int32) // TW
    query_shape = (frames_here, rows_here, columns)
    key_shape = (frames_here + 2, rows_here + 2, columns)
    query_frame = jnp.broadcast_to(frame_q[:, None, None], query_shape).reshape(-1)
    query_row = jnp.broadcast_to(row_q[None, :, None], query_shape).reshape(-1)
    query_tile = jnp.broadcast_to(tiles[None, None, :], query_shape).reshape(-1)
    key_frame = jnp.broadcast_to(frame_k[:, None, None], key_shape).reshape(-1)
    key_row = jnp.broadcast_to(row_k[None, :, None], key_shape).reshape(-1)
    key_tile = jnp.broadcast_to(tiles[None, None, :], key_shape).reshape(-1)
    frame_gap = jnp.abs(query_frame[:, None] - key_frame[None, :])
    row_gap = jnp.abs(query_row[:, None] - key_row[None, :])
    tile_gap = jnp.abs(query_tile[:, None] - key_tile[None, :])
    inside = (key_frame >= 0) & (key_frame < frame_count) & (key_row >= 0) & (key_row < row_count)
    allowed = (frame_gap[None] <= reach_time[:, None, None]) & (row_gap[None] <= reach_rows[:, None, None])
    allowed = allowed & (tile_gap[None] <= reach_cols[:, None, None]) & inside[None, None, :]
    scores = jnp.einsum('qhd,khd->hqk', query_flat, key_flat) * head_width ** (-0.5)
    masked = jnp.where(allowed, scores, -jnp.inf)
    row_peak = lax.optimization_barrier(jnp.max(masked, axis=2, keepdims=True))
    weights = jnp.exp(masked - row_peak)
    totals = lax.optimization_barrier(jnp.sum(weights, axis=2, keepdims=True))
    rounded = weights.astype(jnp.bfloat16)
    mixed = jnp.einsum('hqk,khd->qhd', rounded.astype(jnp.float32), value_flat)
    mixed = mixed / jnp.transpose(totals, (1, 0, 2))
    return mixed.reshape(mixed.shape[0], inner).astype(jnp.bfloat16)

def reference(hidden_in, queries, keys, values, query_gain, key_gain, reach_time, reach_rows, reach_cols, out_weight, gate):
    query_norm = normalize(queries, query_gain)
    key_norm = normalize(keys, key_gain)
    padding = ((1, 1), (1, 1), (0, 0), (0, 0))
    key_pad = jnp.pad(key_norm, padding)
    value_pad = jnp.pad(values, padding)
    row_blocks = NH // RH
    block_count = NF // FR * row_blocks

    def one_block(block_index):
        first_frame = (block_index // row_blocks * FR).astype(jnp.int32)
        first_row = (block_index % row_blocks * RH).astype(jnp.int32)
        anchor = jnp.zeros((), jnp.int32)
        query_block = lax.dynamic_slice(query_norm, (first_frame, first_row, anchor, anchor), (FR, RH, NW, INNER))
        key_region = lax.dynamic_slice(key_pad, (first_frame, first_row, anchor, anchor), (FR + 2, RH + 2, NW, INNER))
        value_region = lax.dynamic_slice(value_pad, (first_frame, first_row, anchor, anchor), (FR + 2, RH + 2, NW, INNER))
        attention = attend(query_block, key_region, value_region, first_frame, first_row, NF, NH, reach_time, reach_rows, reach_cols)
        hidden_block = lax.dynamic_slice(hidden_in, (first_frame, first_row, anchor, anchor), (FR, RH, NW, D))
        hidden_flat = hidden_block.reshape(-1, D).astype(jnp.float32)
        branch = jnp.dot(attention, out_weight, preferred_element_type=jnp.float32)
        return (hidden_flat + gate * branch).astype(jnp.bfloat16).reshape(FR, RH, NW, D)
    blocks = lax.map(one_block, jnp.arange(block_count, dtype=jnp.int32))
    blocks = blocks.reshape(NF // FR, NH // RH, FR, RH, NW, D)
    return jnp.transpose(blocks, (0, 2, 1, 3, 4, 5)).reshape(NF, NH, NW, D)
```

```python
import functools
import math

import jax
import jax.numpy as jnp
import numpy as np
from jax import lax
from jax.experimental import pallas as pl
from jax.experimental.pallas import tpu as pltpu
from jax.sharding import PartitionSpec as P

TW = 8
REACHES = [(a, b, c) for a in range(2) for b in range(2) for c in range(3)]


def normalized(source, gain):
    values_f = source.astype(jnp.float32)
    mean_square = jnp.mean(values_f * values_f, axis=-1, keepdims=True)
    return (values_f * lax.rsqrt(mean_square + 1e-06) * gain).astype(jnp.bfloat16)


def places(frames, rows, columns, margin):
    grid = np.meshgrid(
        np.arange(-margin, frames + margin),
        np.arange(-margin, rows + margin),
        np.arange(columns) // TW,
        indexing="ij",
    )
    return np.stack([axis.reshape(-1) for axis in grid]).astype(np.int32)


def ring_kernel(
    heads,
    group,
    time_ref,
    rows_ref,
    cols_ref,
    raw_query_ref,
    key_ref,
    query_gain_ref,
    key_gain_ref,
    query_place_ref,
    key_place_ref,
    gate_ref,
    value_ref,
    weight_ref,
    hidden_in_ref,
    out_ref,
    query_ref,
    mask_ref,
    hidden_ref,
    region,
    weights,
    mixed,
    total,
    outgoing,
    incoming,
    local_sem,
    own_sem,
    halo_send,
    halo_recv,
    near_send,
    pair_send,
    weight_recv,
    mixed_send,
    mixed_recv,
    back_send,
    back_recv,
):
    t = lax.axis_index("tm")
    s = lax.axis_index("space")
    nt = lax.axis_size("tm")
    ns = lax.axis_size("space")
    chips = ns // 2
    frames, rows, columns, inner = value_ref.shape
    tokens = frames * rows * columns
    keys_here = (frames + 2) * (rows + 2) * columns
    width = inner // heads
    depth, cols = weight_ref.shape

    def remote(source, target, send, recv, tm, space):
        return pltpu.make_async_remote_copy(
            src_ref=source,
            dst_ref=target,
            send_sem=send,
            recv_sem=recv,
            device_id=(tm, space),
            device_id_type=pl.DeviceIdType.MESH,
        )

    has_low_t, has_high_t = t > 0, t < nt - 1
    has_low_s, has_high_s = s > 0, s < ns - 1
    own_f, own_r = pl.ds(1, frames), pl.ds(1, rows)

    def halo(i, source, target, tm, space):
        return remote(source, target, halo_send.at[i], halo_recv.at[i], tm, space)

    straight = []
    for part, whole in ((1, value_ref), (0, region.at[0, own_f, own_r])):
        straight += [
            (halo(4 * part, whole.at[frames - 1], region.at[part, 0, own_r], t + 1, s), has_high_t, has_low_t),
            (halo(4 * part + 1, whole.at[0], region.at[part, frames + 1, own_r], t - 1, s), has_low_t, has_high_t),
            (halo(4 * part + 2, whole.at[:, rows - 1], region.at[part, own_f, 0], t, s + 1), has_high_s, has_low_s),
            (halo(4 * part + 3, whole.at[:, 0], region.at[part, own_f, rows + 1], t, s - 1), has_low_s, has_high_s),
        ]
    corners = []
    for i, (frame, has_frame) in enumerate(((0, has_low_t), (frames + 1, has_high_t))):
        corners.append((
            halo(8 + 2 * i, region.at[:, frame, rows], region.at[:, frame, 0], t, s + 1),
            has_frame & has_high_s, has_frame & has_low_s,
        ))
        corners.append((
            halo(9 + 2 * i, region.at[:, frame, 1], region.at[:, frame, rows + 1], t, s - 1),
            has_frame & has_low_s, has_frame & has_high_s,
        ))
    parts, lane = weights.shape[0], weights.shape[2]

    def block(b, p):
        return weights.at[p, pl.ds(pl.multiple_of(b * depth, depth), depth)]

    def own_block(p):
        return weight_ref.at[:, pl.ds(pl.multiple_of(p * lane, lane), lane)]

    partner = s + 1 - 2 * lax.rem(s, 2)

    def near(k, b, way, p, first):
        space = s + 2 if way == 0 else s - 2
        source = own_block(p) if first else block(b, p)
        return remote(source, block(b, p), near_send.at[way, k, p], weight_recv.at[b, p], t, space)

    def pair(k, b, way, p, first):
        source = own_block(p) if first else block(b, p)
        return remote(source, block(b, p), pair_send.at[way, k, p], weight_recv.at[b, p], t, partner)

    def arrived(b, p):
        remote(block(b, p), block(b, p), pair_send.at[0, 0, p], weight_recv.at[b, p], t, partner).wait_recv()

    def each_part(low, high, run):
        def body(p, carry):
            run(p)
            return carry

        lax.fori_loop(low, high, body, 0)

    for copy, sends, _ in straight[:4]:
        pl.when(sends)(copy.start)

    def first_part(p):
        pl.when(s + 2 < ns)(near(0, s, 0, p, True).start)
        pl.when(s >= 2)(near(0, s, 1, p, True).start)
        pair(0, s, 0, p, True).start()
        pltpu.make_async_copy(own_block(p), block(s, p), own_sem.at[p]).start()

    each_part(0, parts, first_part)
    own_value = pltpu.make_async_copy(value_ref, region.at[1, own_f, own_r], local_sem.at[0])
    own_value.start()
    own_hidden = pltpu.make_async_copy(hidden_in_ref, hidden_ref, local_sem.at[1])
    own_hidden.start()

    step = 16 if columns % 16 == 0 else columns
    for frame in range(frames):
        for row in range(rows):
            for column in range(0, columns, step):
                at = slice(column, column + step)
                region[0, 1 + frame, 1 + row, at] = normalized(key_ref[frame, row, at], key_gain_ref[...])

    def query_rows(i, carry):
        at = pl.ds(pl.multiple_of(i * 16, 16), 16)
        query_ref[at] = normalized(raw_query_ref[at], query_gain_ref[...])
        return carry

    lax.fori_loop(0, tokens // 16, query_rows, 0)
    for copy, sends, _ in straight[4:]:
        pl.when(sends)(copy.start)

    def clear_frame(frame):
        def run():
            for part in range(2):
                for row in range(rows + 2):
                    region[part, frame, row] = jnp.zeros((columns, inner), jnp.bfloat16)
        return run

    def clear_row(row):
        def run():
            for part in range(2):
                for frame in range(frames + 2):
                    region[part, frame, row] = jnp.zeros((columns, inner), jnp.bfloat16)
        return run

    pl.when(jnp.logical_not(has_low_t))(clear_frame(0))
    pl.when(jnp.logical_not(has_high_t))(clear_frame(frames + 1))
    pl.when(jnp.logical_not(has_low_s))(clear_row(0))
    pl.when(jnp.logical_not(has_high_s))(clear_row(rows + 1))

    frame_k, row_k, tile_k = key_place_ref[0:1], key_place_ref[1:2], key_place_ref[2:3]
    inside = (frame_k >= -t * frames) & (frame_k < (nt - t) * frames)
    inside = inside & (row_k >= -s * rows) & (row_k < (ns - s) * rows)
    outside = jnp.where(inside, 0, 9)
    frame_gap = jnp.abs(query_place_ref[:, 0:1] - frame_k) + outside
    row_gap = jnp.abs(query_place_ref[:, 1:2] - row_k)
    tile_gap = jnp.abs(query_place_ref[:, 2:3] - tile_k)
    for i, (reach_t, reach_r, reach_c) in enumerate(REACHES):
        allowed = (frame_gap <= reach_t) & (row_gap <= reach_r) & (tile_gap <= reach_c)
        mask_ref[i] = jnp.where(allowed, 0.0, -1e30)

    def relay(k, p):
        low, high = s - 2 * k, s + 2 * k

        @pl.when(low >= 0)
        def _():
            arrived(low, p)
            pl.when(s + 2 < ns)(near(k, low, 0, p, False).start)
            pair(k, low, 0, p, False).start()

        @pl.when(high < ns)
        def _():
            arrived(high, p)
            pl.when(s >= 2)(near(k, high, 1, p, False).start)
            pair(k, high, 1, p, False).start()

    def relay_parts(k, low, high):
        if 1 <= k < chips:
            each_part(low, high, functools.partial(relay, k))

    early = parts // 2
    last = chips - 1
    if last > 1:
        relay_parts(1, 0, early)
    for copy, _, receives in straight[0:2] + straight[4:6]:
        pl.when(receives)(copy.wait_recv)
    for copy, sends, _ in corners:
        pl.when(sends)(copy.start)
    for copy, _, receives in straight[2:4] + straight[6:8]:
        pl.when(receives)(copy.wait_recv)
    for copy, _, receives in corners:
        pl.when(receives)(copy.wait_recv)
    if last > 1:
        relay_parts(1, early, parts)
    own_value.wait()

    groups = heads // group
    span = group * width

    def gather(g, d):
        at = (t, slice(None), pl.ds(pl.multiple_of(g * span, span), span))
        return remote(
            mixed.at[at], mixed.at[at], mixed_send.at[d - 1, g], mixed_recv.at[t, g],
            lax.rem(t + d, nt), s,
        )

    def one_group(g, carry):
        for i in range(group):
            h = g * group + i
            lanes = pl.ds(pl.multiple_of(h * width, width), width)
            query = query_ref[:, lanes]
            key = region[0, :, :, :, lanes].reshape(keys_here, width)
            value = region[1, :, :, :, lanes].reshape(keys_here, width)
            scores = lax.dot_general(
                query, key, (((1,), (1,)), ((), ())), preferred_element_type=jnp.float32
            ) * width ** (-0.5)
            scores = scores + mask_ref[time_ref[h] * 6 + rows_ref[h] * 3 + cols_ref[h]]
            part = jnp.exp(scores - jnp.max(scores, axis=1, keepdims=True))
            sums = jnp.sum(part, axis=1, keepdims=True)
            result = jnp.dot(part.astype(jnp.bfloat16), value, preferred_element_type=jnp.float32)
            mixed[t, :, lanes] = (result / sums).astype(jnp.bfloat16)
        for d in range(1, nt):
            gather(g, d).start()
        return carry

    ahead = groups * 5 // 8
    lax.fori_loop(0, ahead, one_group, 0)
    if last > 2:
        relay_parts(2, 0, parts)
    lax.fori_loop(ahead, groups, one_group, 0)
    for k in range(3, last):
        relay_parts(k, 0, parts)

    def gathered(g, carry):
        for d in range(1, nt):
            other = lax.rem(t + d, nt)
            at = (other, slice(None), pl.ds(pl.multiple_of(g * span, span), span))
            remote(mixed.at[at], mixed.at[at], mixed_send.at[d - 1, g], mixed_recv.at[other, g], t, s).wait_recv()
        return carry

    chip_depth = 2 * depth
    piece = chip_depth * 128 // math.gcd(chip_depth, 128)

    def multiply(start, p, first):
        feature = pl.ds(pl.multiple_of(start, piece), piece)
        left = mixed[:, :, feature].reshape(nt * tokens, piece)
        product = jnp.dot(left, weights[p, feature], preferred_element_type=jnp.float32)
        if first:
            total[p] = product
        else:
            total[p] += product

    chip = s // 2
    half = lax.rem(s, 2)

    def add(k, p):
        for other in (chip - k, chip + k):
            @pl.when((other >= 0) & (other < chips))
            def _():
                arrived(2 * other + 1 - half, p)
                multiply(other * piece, p, False)

    def own_rows(owner):
        return pl.ds(pl.multiple_of(owner * tokens, tokens), tokens)

    def back(d, p):
        other = lax.rem(t + d, nt)
        return remote(
            outgoing.at[d - 1, p], incoming.at[d - 1, p], back_send.at[d - 1, p], back_recv.at[d - 1, p], other, s
        )

    def send_back(p):
        for d in range(1, nt):
            outgoing[d - 1, p] = total[p, own_rows(lax.rem(t + d, nt)), :].astype(jnp.bfloat16)
            back(d, p).start()

    def own_part(p):
        pltpu.make_async_copy(own_block(p), block(s, p), own_sem.at[p]).wait()
        arrived(partner, p)

    lax.fori_loop(0, groups, gathered, 0)
    if piece == chip_depth:
        def begin(p):
            own_part(p)
            multiply(chip * piece, p, True)
            for k in range(1, last):
                add(k, p)

        each_part(0, parts, begin)

        def conclude(p):
            if last > 0:
                relay(last, p)
                add(last, p)
            send_back(p)

        each_part(0, parts, conclude)
    else:
        def conclude(p):
            own_part(p)
            if last > 0:
                relay(last, p)
            for k in range(1, chips):
                for other in (chip - k, chip + k):
                    @pl.when((other >= 0) & (other < chips))
                    def _():
                        arrived(2 * other + 1 - half, p)
            multiply(0, p, True)

            def add_piece(i, carry):
                multiply(i * piece, p, False)
                return carry

            lax.fori_loop(1, inner // piece, add_piece, 0)
            send_back(p)

        each_part(0, parts, conclude)

    own_hidden.wait()

    def finish(owner, p, branch):
        lanes = pl.ds(pl.multiple_of(owner * cols + p * lane, lane), lane)
        out_ref[:, lanes] = (
            hidden_ref[:, lanes].astype(jnp.float32) + gate_ref[:, lanes] * branch
        ).astype(jnp.bfloat16)

    def finish_own(p):
        finish(t, p, total[p, own_rows(t), :])

    def finish_others(p):
        for d in range(1, nt):
            back(d, p).wait_recv()
            finish(lax.rem(t + nt - d, nt), p, incoming[d - 1, p].astype(jnp.float32))

    each_part(0, parts, finish_own)
    each_part(0, parts, finish_others)

    for copy, sends, _ in straight + corners:
        pl.when(sends)(copy.wait_send)
    for k in range(chips):
        low, high = s - 2 * k, s + 2 * k

        def weight_sent(p):
            pl.when((low >= 0) & (s + 2 < ns))(near(k, low, 0, p, k == 0).wait_send)
            pl.when((high < ns) & (s >= 2))(near(k, high, 1, p, k == 0).wait_send)
            pl.when(low >= 0)(pair(k, low, 0, p, k == 0).wait_send)
            if k > 0:
                pl.when(high < ns)(pair(k, high, 1, p, False).wait_send)

        each_part(0, parts, weight_sent)

    def sent(g, carry):
        for d in range(1, nt):
            gather(g, d).wait_send()
        return carry

    lax.fori_loop(0, groups, sent, 0)

    def back_sent(p):
        for d in range(1, nt):
            back(d, p).wait_send()

    each_part(0, parts, back_sent)


def ring_shards(
    hidden_in,
    queries,
    keys,
    values,
    query_gain,
    key_gain,
    reach_time,
    reach_rows,
    reach_cols,
    out_weight,
    gate,
):
    frames, rows, columns, inner = queries.shape
    width = hidden_in.shape[3]
    heads = reach_time.shape[0]
    tokens = frames * rows * columns
    nt, ns = lax.axis_size("tm"), lax.axis_size("space")
    depth, cols = out_weight.shape
    group = 5 if heads % 5 == 0 else 1
    vmem = pl.BlockSpec(memory_space=pltpu.VMEM)
    hbm = pl.BlockSpec(memory_space=pl.ANY)
    dma = pltpu.SemaphoreType.DMA
    lane = 256 if cols % 256 == 0 else 128
    parts = cols // lane
    output = pl.pallas_call(
        functools.partial(ring_kernel, heads, group),
        out_shape=jax.ShapeDtypeStruct((tokens, width), jnp.bfloat16),
        in_specs=[pl.BlockSpec(memory_space=pltpu.SMEM)] * 3 + [vmem] * 7 + [hbm] * 3,
        out_specs=vmem,
        scratch_shapes=[
            pltpu.VMEM((tokens, inner), jnp.bfloat16),
            pltpu.VMEM((len(REACHES), tokens, (frames + 2) * (rows + 2) * columns), jnp.float32),
            pltpu.VMEM((tokens, width), jnp.bfloat16),
            pltpu.VMEM((2, frames + 2, rows + 2, columns, inner), jnp.bfloat16),
            pltpu.VMEM((parts, depth * ns, lane), jnp.bfloat16),
            pltpu.VMEM((nt, tokens, inner), jnp.bfloat16),
            pltpu.VMEM((parts, nt * tokens, lane), jnp.float32),
            pltpu.VMEM((nt - 1, parts, tokens, lane), jnp.bfloat16),
            pltpu.VMEM((nt - 1, parts, tokens, lane), jnp.bfloat16),
            dma((2,)),
            dma((parts,)),
            dma((12,)),
            dma((12,)),
            dma((2, ns // 2, parts)),
            dma((2, ns // 2, parts)),
            dma((ns, parts)),
            dma((nt - 1, heads // group)),
            dma((nt, heads // group)),
            dma((nt - 1, parts)),
            dma((nt - 1, parts)),
        ],
        compiler_params=pltpu.CompilerParams(
            has_side_effects=True, vmem_limit_bytes=60 * 1024 * 1024
        ),
    )(
        reach_time,
        reach_rows,
        reach_cols,
        queries.reshape(tokens, inner),
        keys,
        query_gain.reshape(1, inner),
        key_gain.reshape(1, inner),
        places(frames, rows, columns, 0).T,
        places(frames, rows, columns, 1),
        gate.reshape(1, width),
        values,
        out_weight,
        hidden_in.reshape(tokens, width),
    )
    return output.reshape(frames, rows, columns, width)


def pair_kernel(
    heads,
    time_ref,
    rows_ref,
    cols_ref,
    query_gain_ref,
    key_gain_ref,
    query_place_ref,
    key_place_ref,
    gate_ref,
    raw_query_ref,
    raw_key_ref,
    value_ref,
    weight_ref,
    hidden_in_ref,
    out_ref,
    raw,
    normed,
    region,
    query_ref,
    mask_ref,
    mixed,
    weights,
    total,
    partial_out,
    partial_in,
    outgoing,
    incoming,
    hidden_ref,
    local_sem,
    value_sem,
    own_sem,
    swap_send,
    swap_recv,
    side_send,
    side_recv,
    corner_send,
    corner_recv,
    near_send,
    cross_send,
    pair_send,
    weight_recv,
    level_send,
    level_recv,
    mixed_send,
    mixed_recv,
    part_send,
    part_recv,
    back_send,
    back_recv,
):
    t = lax.axis_index("tm")
    s = lax.axis_index("space")
    nt = lax.axis_size("tm")
    ns = lax.axis_size("space")
    frames, rows, columns, inner = value_ref.shape
    tokens = frames * rows * columns
    depth, cols = weight_ref.shape
    width = inner // heads
    groups = ns // 2
    half = inner // 2
    blocks, parts, _, lane = weights.shape
    chips = ns // 4
    row_tokens = rows * columns
    span = 2 * frames

    p = lax.rem(t, 2)
    column_block = lax.div(t, 2)
    c = lax.rem(s, 2)
    z = lax.div(s, 2)
    level = lax.rem(z, 2)
    chip = lax.div(z, 2)
    mate = t + 1 - 2 * p
    partner = s + 1 - 2 * c
    level_mate = s + 2 - 4 * level

    has_low_t, has_high_t = t >= 2, t < nt - 2
    has_low_s, has_high_s = s > 0, s < ns - 1

    def remote(source, target, send, recv, tm, space):
        return pltpu.make_async_remote_copy(
            src_ref=source,
            dst_ref=target,
            send_sem=send,
            recv_sem=recv,
            device_id=(tm, space),
            device_id_type=pl.DeviceIdType.MESH,
        )

    def lanes_at(start, size):
        return pl.ds(pl.multiple_of(start, 128), size)

    def other_column(e):
        return lax.rem(column_block + e, blocks)

    def other_chip(d):
        return lax.rem(chip + d, chips)

    def column_device(e):
        return 2 * other_column(e) + p

    def chip_device(d):
        return 4 * other_chip(d) + 2 * level + c

    load_key = pltpu.make_async_copy(raw_key_ref, raw.at[0], local_sem.at[0])
    load_key.start()
    load_query = pltpu.make_async_copy(raw_query_ref, raw.at[1], local_sem.at[1])
    load_query.start()

    barrier = pltpu.get_barrier_semaphore()

    def greet(tm, space):
        pl.semaphore_signal(
            barrier, inc=1, device_id=(tm, space), device_id_type=pl.DeviceIdType.MESH
        )

    greet(mate, s)
    greet(t, partner)
    greet(t, level_mate)
    for e in range(1, blocks):
        greet(column_device(e), s)
    for d in range(1, chips):
        greet(t, chip_device(d))
    up, down = (c == 1) & has_high_s, (c == 0) & has_low_s

    @pl.when(up)
    def _():
        greet(t, s + 1)

    @pl.when(down)
    def _():
        greet(t, s - 1)

    pl.semaphore_wait(barrier, blocks + chips + 1 + jnp.where(up | down, 1, 0))

    own_frames = pl.ds(1 + frames * p, frames)
    own_rows = pl.ds(1, rows)

    def group_lanes(b):
        return pl.ds(b * depth, depth)

    def value_swap(b):
        source = value_ref.at[:, :, :, lanes_at((2 * b + 1 - p) * depth, depth)]
        target = region.at[1, own_frames, own_rows, :, group_lanes(b)]
        return remote(source, target, swap_send.at[1, b], swap_recv.at[1, b], mate, s)

    def key_swap(b):
        source = normed.at[0, 1 - p, :, :, :, group_lanes(b)]
        target = region.at[0, own_frames, own_rows, :, group_lanes(b)]
        return remote(source, target, swap_send.at[0, b], swap_recv.at[0, b], mate, s)

    def query_swap(b):
        source = normed.at[1, 1 - p, :, :, :, group_lanes(b)]
        target = query_ref.at[pl.ds(frames * p, frames), :, :, group_lanes(b)]
        return remote(source, target, swap_send.at[2, b], swap_recv.at[2, b], mate, s)

    def own_value(b):
        return pltpu.make_async_copy(
            value_ref.at[:, :, :, lanes_at((2 * b + p) * depth, depth)],
            region.at[1, own_frames, own_rows, :, group_lanes(b)],
            value_sem.at[b],
        )

    def own_weight(q):
        return weight_ref.at[:, pl.ds(q * lane, lane)]

    def own_weight_at(q):
        return weight_ref.at[:, lanes_at(q * lane, lane)]

    def weight_block(block, chip_index, core, q):
        start = (2 * chip_index + core) * depth
        return weights.at[block, q, pl.ds(pl.multiple_of(start, depth), depth)]

    def arrival(chip_index, core):
        return 2 * chip_index + core

    def keep_weight(q):
        return pltpu.make_async_copy(
            own_weight_at(q), weight_block(column_block, chip, c, q), own_sem.at[q]
        )

    def far_weight(d, q):
        return remote(
            own_weight_at(q), weight_block(column_block, chip, c, q),
            near_send.at[d - 1, q], weight_recv.at[column_block, arrival(chip, c), q],
            t, chip_device(d),
        )

    def cross_weight(e, d, q):
        block = weight_block(column_block, other_chip(d), c, q)
        source = own_weight_at(q) if d == 0 else block
        return remote(
            source, block, cross_send.at[e - 1, d, q],
            weight_recv.at[column_block, arrival(other_chip(d), c), q],
            column_device(e), s,
        )

    def pair_weight(e, d, q):
        block = weight_block(other_column(e), other_chip(d), c, q)
        source = own_weight_at(q) if e == 0 and d == 0 else block
        return remote(
            source, block, pair_send.at[e, d, q],
            weight_recv.at[other_column(e), arrival(other_chip(d), c), q],
            t, partner,
        )

    def weight_here(e, d, core, q):
        block = weight_block(other_column(e), other_chip(d), core, q)
        remote(
            block, block, pair_send.at[e, d, q],
            weight_recv.at[other_column(e), arrival(other_chip(d), core), q], t, partner,
        ).wait_recv()

    def send_far(q):
        for d in range(1, chips):
            far_weight(d, q).start()

    def send_cross(q):
        for e in range(1, blocks):
            cross_weight(e, 0, q).start()
        pair_weight(0, 0, q).start()

    def relay_far(q):
        for d in range(1, chips):
            weight_here(0, d, c, q)
            for e in range(1, blocks):
                cross_weight(e, d, q).start()
            pair_weight(0, d, q).start()

    def relay_cross(q, far):
        for e in range(1, blocks):
            for d in range(1, chips) if far else (0,):
                weight_here(e, d, c, q)
                pair_weight(e, d, q).start()

    value_swap(0).start()
    for b in range(groups):
        own_value(b).start()
    send_far(0)
    send_cross(0)
    for q in range(parts):
        keep_weight(q).start()
    own_hidden = pltpu.make_async_copy(hidden_in_ref, hidden_ref, local_sem.at[2])
    own_hidden.start()

    step = 16 if columns % 16 == 0 else columns

    def normalize(index, gain_ref):
        for frame in range(frames):
            for row in range(rows):
                for column in range(0, columns, step):
                    at = slice(column, column + step)
                    result = normalized(raw[index, frame, row, at], gain_ref[...])
                    for b in range(groups):
                        for core in range(2):
                            start = (2 * b + core) * depth
                            normed[index, core, frame, row, at, b * depth:(b + 1) * depth] = (
                                result[:, start:start + depth]
                            )

    load_key.wait()
    with jax.named_scope("normalize_key"):
        normalize(0, key_gain_ref)
    key_swap(0).start()
    own_key = pltpu.make_async_copy(
        normed.at[0, p], region.at[0, own_frames, own_rows], local_sem.at[3]
    )
    own_key.start()
    load_query.wait()
    with jax.named_scope("normalize_query"):
        normalize(1, query_gain_ref)
    query_swap(0).start()
    own_query = pltpu.make_async_copy(
        normed.at[1, p], query_ref.at[pl.ds(frames * p, frames)], local_sem.at[4]
    )
    own_query.start()
    for b in range(1, groups):
        value_swap(b).start()
        key_swap(b).start()
        query_swap(b).start()

    def clear_frame(frame):
        def run():
            for part in range(2):
                for row in range(rows + 2):
                    region[part, frame, row] = jnp.zeros((columns, half), jnp.bfloat16)
        return run

    def clear_row(row):
        def run():
            for part in range(2):
                for frame in range(span + 2):
                    region[part, frame, row] = jnp.zeros((columns, half), jnp.bfloat16)
        return run

    pl.when(jnp.logical_not(has_low_t))(clear_frame(0))
    pl.when(jnp.logical_not(has_high_t))(clear_frame(span + 1))
    pl.when(jnp.logical_not(has_low_s))(clear_row(0))
    pl.when(jnp.logical_not(has_high_s))(clear_row(rows + 1))

    frame_k, row_k, tile_k = key_place_ref[0:1], key_place_ref[1:2], key_place_ref[2:3]
    inside = (row_k >= -s * rows) & (row_k < (ns - s) * rows)
    row_gap = jnp.abs(query_place_ref[:, 0:1] - row_k) + jnp.where(inside, 0, 9)
    tile_gap = jnp.abs(query_place_ref[:, 1:2] - tile_k)
    low_gap = jnp.where(has_low_t, 0, 9) * (frame_k < 0).astype(jnp.int32)
    high_gap = jnp.where(has_high_t, 0, 9) * (frame_k > 0).astype(jnp.int32)
    for kind, edge in enumerate((jnp.zeros_like(low_gap), low_gap, high_gap)):
        frame_gap = jnp.abs(frame_k) + edge
        for i, (reach_t, reach_r, reach_c) in enumerate(REACHES):
            allowed = (frame_gap <= reach_t) & (row_gap <= reach_r) & (tile_gap <= reach_c)
            mask_ref[kind, i] = jnp.where(allowed, 0.0, -1e30)

    pair_frames = pl.ds(1, span)

    def row_up(b):
        return remote(
            region.at[:, pair_frames, rows, :, group_lanes(b)],
            region.at[:, pair_frames, 0, :, group_lanes(b)],
            side_send.at[0, b], side_recv.at[0, b], t, s + 1,
        )

    def row_down(b):
        return remote(
            region.at[:, pair_frames, 1, :, group_lanes(b)],
            region.at[:, pair_frames, rows + 1, :, group_lanes(b)],
            side_send.at[1, b], side_recv.at[1, b], t, s - 1,
        )

    def frame_up(b):
        return remote(
            region.at[:, span, own_rows, :, group_lanes(b)],
            region.at[:, 0, own_rows, :, group_lanes(b)],
            side_send.at[2, b], side_recv.at[2, b], t + 2, s,
        )

    def frame_down(b):
        return remote(
            region.at[:, 1, own_rows, :, group_lanes(b)],
            region.at[:, span + 1, own_rows, :, group_lanes(b)],
            side_send.at[3, b], side_recv.at[3, b], t - 2, s,
        )

    def sides(b):
        return (
            (frame_up(b), has_high_t, has_low_t),
            (frame_down(b), has_low_t, has_high_t),
            (row_up(b), has_high_s, has_low_s),
            (row_down(b), has_low_s, has_high_s),
        )

    def corners(b):
        result = []
        for i, (frame, has_frame) in enumerate(((0, has_low_t), (span + 1, has_high_t))):
            for j, (row, landing, space, sends, receives) in enumerate((
                (rows, 0, s + 1, has_high_s, has_low_s),
                (1, rows + 1, s - 1, has_low_s, has_high_s),
            )):
                copy = remote(
                    region.at[:, frame, row, :, group_lanes(b)],
                    region.at[:, frame, landing, :, group_lanes(b)],
                    corner_send.at[2 * i + j, b], corner_recv.at[2 * i + j, b], t, space,
                )
                result.append((copy, has_frame & sends, has_frame & receives))
        return result

    def feature_lanes(index, core):
        return lanes_at((2 * index + core) * depth, depth)

    def to_level_mate(j):
        at = (slice(None), feature_lanes(j, p))
        return remote(
            mixed.at[(2,) + at], mixed.at[(level,) + at],
            level_send.at[j], level_recv.at[j], t, level_mate,
        )

    def from_level_mate(j):
        at = (1 - level, slice(None), feature_lanes(j, p))
        return remote(mixed.at[at], mixed.at[at], level_send.at[j], level_recv.at[j], t, level_mate)

    def to_mate(which, j):
        at = (which, slice(None), feature_lanes(j, p))
        return remote(
            mixed.at[at], mixed.at[at], mixed_send.at[which, j], mixed_recv.at[which, j], mate, s
        )

    def from_mate(which, j):
        at = (which, slice(None), feature_lanes(j, 1 - p))
        remote(
            mixed.at[at], mixed.at[at], mixed_send.at[which, j], mixed_recv.at[which, j], mate, s
        ).wait_recv()

    def attend(b):
        in_level = level == b % 2
        place = jnp.where(in_level, level, 2)
        index = b // 2
        group = depth // width

        def one_head(i, carry):
            h = (2 * b + p) * group + i
            lanes = lanes_at(b * depth + i * width, width)
            reach = time_ref[h] * 6 + rows_ref[h] * 3 + cols_ref[h]
            target = lanes_at((2 * index + p) * depth + i * width, width)
            scores, values = [], []
            for frame in range(span):
                query = query_ref[frame, :, :, lanes].reshape(row_tokens, width)
                near = slice(frame, frame + 3)
                key = region[0, near, :, :, lanes].reshape(-1, width)
                values.append(region[1, near, :, :, lanes].reshape(-1, width))
                scores.append(lax.dot_general(
                    query, key, (((1,), (1,)), ((), ())), preferred_element_type=jnp.float32
                ))
            results = []
            for frame in range(span):
                kind = 1 if frame == 0 else 2 if frame == span - 1 else 0
                masked = scores[frame] * width ** (-0.5) + mask_ref[kind, reach]
                part = jnp.exp(masked - jnp.max(masked, axis=1, keepdims=True))
                sums = jnp.sum(part, axis=1, keepdims=True)
                result = jnp.dot(
                    part.astype(jnp.bfloat16), values[frame], preferred_element_type=jnp.float32
                )
                results.append((result / sums).astype(jnp.bfloat16))
            mixed[place, :, target] = jnp.concatenate(results, axis=0)
            return carry

        lax.fori_loop(0, group, one_head, 0)

    def send_mixed(b):
        in_level = level == b % 2
        index = b // 2
        pl.when(in_level)(to_mate(level, index).start)
        pl.when(jnp.logical_not(in_level))(to_level_mate(index).start)

    def relay_mixed(b):
        @pl.when(level == b % 2)
        def _():
            from_level_mate(b // 2).wait_recv()
            to_mate(1 - level, b // 2).start()

    def arrive(i):
        with jax.named_scope(f"wait_swap{i}"):
            value_swap(i).wait_recv()
            key_swap(i).wait_recv()
            own_value(i).wait()
            if i == 0:
                own_key.wait()
        with jax.named_scope(f"send_sides{i}"):
            for copy, sends, _ in sides(i):
                pl.when(sends)(copy.start)

    def turn(i):
        with jax.named_scope(f"wait_frames{i}"):
            for copy, _, receives in sides(i)[:2]:
                pl.when(receives)(copy.wait_recv)
        for copy, sends, _ in corners(i):
            pl.when(sends)(copy.start)

    def ready(b):
        with jax.named_scope(f"wait_query{b}"):
            query_swap(b).wait_recv()
            if b == 0:
                own_query.wait()
        with jax.named_scope(f"wait_rows{b}"):
            for copy, _, receives in sides(b)[2:]:
                pl.when(receives)(copy.wait_recv)
        with jax.named_scope(f"wait_corners{b}"):
            for copy, _, receives in corners(b):
                pl.when(receives)(copy.wait_recv)

    early = min(2, parts)
    for i in range(groups + 1):
        if i < groups:
            arrive(i)
        if i > 0:
            ready(i - 1)
            with jax.named_scope(f"attend{i - 1}"):
                attend(i - 1)
        if i < groups:
            turn(i)
        if i > 0:
            send_mixed(i - 1)
        if i == 1 and parts > 1:
            send_far(1)
        if i == groups - 1 and parts > 2:
            send_far(2)
        if i < groups:
            if i + 1 < min(groups, parts):
                send_cross(i + 1)
        else:
            if parts > 3:
                send_far(3)
            for q in range(early):
                relay_far(q)
            for q in range(groups, parts):
                send_cross(q)
        if i > 1:
            with jax.named_scope(f"relay_mixed{i}"):
                relay_mixed(i - 2)
        if i > 1 and i - 2 < parts:
            with jax.named_scope(f"relay_cross{i}"):
                relay_cross(i - 2, False)
    with jax.named_scope("relay_mixed_last"):
        relay_mixed(groups - 1)

    def each_part(low, high, run):
        def body(q, carry):
            run(q)
            return carry

        lax.fori_loop(low, high, body, 0)

    def next_far(q):
        if q < parts:
            with jax.named_scope(f"relay_far{q}"):
                relay_far(q)
            if q + 2 < parts:
                send_far(q + 2)

    next_far(early)
    with jax.named_scope("from_mate"):
        for which in range(2):
            for j in range(groups // 2):
                from_mate(which, j)

    def multiply(e, q):
        block = other_column(e)
        for d in range(chips):
            weight_here(e, d, 1 - c, q)
        left = mixed[0:2].reshape(4 * tokens, half)
        product = jnp.dot(left, weights[block, q], preferred_element_type=jnp.float32)
        total[block, q] = product.reshape(2, 2 * tokens, lane)
        partial_out[block, q] = total[block, q, 1 - level].astype(jnp.bfloat16)
        part_copy(block, q).start()

    def part_copy(block, q):
        return remote(
            partial_out.at[block, q], partial_in.at[block, q],
            part_send.at[block, q], part_recv.at[block, q], t, level_mate,
        )

    def back(block, q):
        return remote(
            outgoing.at[block, q], incoming.at[block, q],
            back_send.at[block, q], back_recv.at[block, q], mate, s,
        )

    def token_rows(side):
        return pl.ds(pl.multiple_of(side * tokens, tokens), tokens)

    def finish(column, branch):
        lanes = lanes_at(column, lane)
        out_ref[:, lanes] = (
            hidden_ref[:, lanes].astype(jnp.float32) + gate_ref[:, lanes] * branch
        ).astype(jnp.bfloat16)

    def reduce_part(q):
        for e in range(blocks):
            block = other_column(e)
            part_copy(block, q).wait_recv()
            theirs = token_rows(1 - p)
            outgoing[block, q] = (
                total[block, q, level, theirs] + partial_in[block, q, theirs].astype(jnp.float32)
            ).astype(jnp.bfloat16)
            back(block, q).start()
            ours = token_rows(p)
            branch = total[block, q, level, ours] + partial_in[block, q, ours].astype(jnp.float32)
            finish((2 * block + p) * cols + q * lane, branch)

    own_hidden.wait()
    reduced = 0
    for q in range(parts):
        if q >= groups - 1:
            relay_cross(q, False)
        keep_weight(q).wait()
        with jax.named_scope(f"multiply{q}own"):
            multiply(0, q)
        if blocks > 1:
            with jax.named_scope(f"main_cross{q}"):
                relay_cross(q, True)
            with jax.named_scope(f"multiply{q}other"):
                for e in range(1, blocks):
                    multiply(e, q)
        if q >= 1:
            next_far(early + q)
        with jax.named_scope(f"reduce{q}"):
            while reduced < q - 1:
                reduce_part(reduced)
                reduced += 1
    with jax.named_scope("reduce_last"):
        each_part(reduced, parts, reduce_part)

    def finish_others(q):
        for block in range(blocks):
            back(block, q).wait_recv()
            finish((2 * block + 1 - p) * cols + q * lane, incoming[block, q].astype(jnp.float32))

    with jax.named_scope("finish_others"):
        each_part(0, parts, finish_others)

    for b in range(groups):
        value_swap(b).wait_send()
        key_swap(b).wait_send()
        query_swap(b).wait_send()
        for copy, sends, _ in sides(b) + tuple(corners(b)):
            pl.when(sends)(copy.wait_send)
    for j in range(groups // 2):
        to_level_mate(j).wait_send()
        for which in range(2):
            to_mate(which, j).wait_send()

    def sent(q):
        for d in range(1, chips):
            far_weight(d, q).wait_send()
        for e in range(blocks):
            for d in range(chips):
                pair_weight(e, d, q).wait_send()
                if e > 0:
                    cross_weight(e, d, q).wait_send()
        for block in range(blocks):
            part_copy(block, q).wait_send()
            back(block, q).wait_send()

    each_part(0, parts, sent)


def pair_shards(
    hidden_in,
    queries,
    keys,
    values,
    query_gain,
    key_gain,
    reach_time,
    reach_rows,
    reach_cols,
    out_weight,
    gate,
):
    frames, rows, columns, inner = queries.shape
    width = hidden_in.shape[3]
    heads = reach_time.shape[0]
    tokens = frames * rows * columns
    nt, ns = lax.axis_size("tm"), lax.axis_size("space")
    depth, cols = out_weight.shape
    lane = 256 if cols % 256 == 0 else 128
    parts = cols // lane
    blocks, chips, groups = nt // 2, ns // 4, ns // 2
    half = inner // 2
    pair_tokens = 2 * tokens
    vmem = pl.BlockSpec(memory_space=pltpu.VMEM)
    hbm = pl.BlockSpec(memory_space=pl.ANY)
    dma = pltpu.SemaphoreType.DMA
    _, query_row, query_tile = places(1, rows, columns, 0)
    key_place = np.stack([axis.reshape(-1) for axis in np.meshgrid(
        np.arange(-1, 2), np.arange(-1, rows + 1), np.arange(columns) // TW, indexing="ij"
    )]).astype(np.int32)
    output = pl.pallas_call(
        functools.partial(pair_kernel, heads),
        out_shape=jax.ShapeDtypeStruct((tokens, width), jnp.bfloat16),
        in_specs=[pl.BlockSpec(memory_space=pltpu.SMEM)] * 3 + [vmem] * 5 + [hbm] * 5,
        out_specs=vmem,
        scratch_shapes=[
            pltpu.VMEM((2, frames, rows, columns, inner), jnp.bfloat16),
            pltpu.VMEM((2, 2, frames, rows, columns, half), jnp.bfloat16),
            pltpu.VMEM((2, 2 * frames + 2, rows + 2, columns, half), jnp.bfloat16),
            pltpu.VMEM((2 * frames, rows, columns, half), jnp.bfloat16),
            pltpu.VMEM((3, len(REACHES), rows * columns, 3 * (rows + 2) * columns), jnp.float32),
            pltpu.VMEM((3, pair_tokens, half), jnp.bfloat16),
            pltpu.VMEM((blocks, parts, half, lane), jnp.bfloat16),
            pltpu.VMEM((blocks, parts, 2, pair_tokens, lane), jnp.float32),
            pltpu.VMEM((blocks, parts, pair_tokens, lane), jnp.bfloat16),
            pltpu.VMEM((blocks, parts, pair_tokens, lane), jnp.bfloat16),
            pltpu.VMEM((blocks, parts, tokens, lane), jnp.bfloat16),
            pltpu.VMEM((blocks, parts, tokens, lane), jnp.bfloat16),
            pltpu.VMEM((tokens, width), jnp.bfloat16),
            dma((5,)),
            dma((groups,)),
            dma((parts,)),
            dma((3, groups)),
            dma((3, groups)),
            dma((4, groups)),
            dma((4, groups)),
            dma((4, groups)),
            dma((4, groups)),
            dma((max(chips - 1, 1), parts)),
            dma((max(blocks - 1, 1), chips, parts)),
            dma((blocks, chips, parts)),
            dma((blocks, 2 * chips, parts)),
            dma((groups // 2,)),
            dma((groups // 2,)),
            dma((2, groups // 2)),
            dma((2, groups // 2)),
            dma((blocks, parts)),
            dma((blocks, parts)),
            dma((blocks, parts)),
            dma((blocks, parts)),
        ],
        compiler_params=pltpu.CompilerParams(
            collective_id=0, has_side_effects=True, vmem_limit_bytes=60 * 1024 * 1024
        ),
    )(
        reach_time,
        reach_rows,
        reach_cols,
        query_gain.reshape(1, inner),
        key_gain.reshape(1, inner),
        np.stack([query_row, query_tile]).T,
        key_place,
        gate.reshape(1, width),
        queries,
        keys,
        values,
        out_weight,
        hidden_in.reshape(tokens, width),
    )
    return output.reshape(frames, rows, columns, width)


def shards(hidden_in, queries, keys, values, *others):
    out_weight, reach_time = others[-2], others[2]
    width = queries.shape[3] // reach_time.shape[0]
    nt, ns = lax.axis_size("tm"), lax.axis_size("space")
    whole_heads = out_weight.shape[0] % width == 0
    form = pair_shards if whole_heads and nt % 2 == 0 and ns % 4 == 0 else ring_shards
    return form(hidden_in, queries, keys, values, *others)


def solution(mesh):
    in_specs = (
        P("tm", "space", None, None),
        P("tm", "space", None, None),
        P("tm", "space", None, None),
        P("tm", "space", None, None),
        P(),
        P(),
        P(),
        P(),
        P(),
        P("space", "tm"),
        P(),
    )
    out_specs = P("tm", "space", None, None)
    return jax.shard_map(shards, mesh=mesh, in_specs=in_specs, out_specs=out_specs, check_vma=False)
```

```python
import functools
import math

import jax
import jax.numpy as jnp
import numpy as np
from jax import lax
from jax.experimental import pallas as pl
from jax.experimental.pallas import tpu as pltpu
from jax.sharding import PartitionSpec as P

TW = 8
REACHES = [(a, b, c) for a in range(2) for b in range(2) for c in range(3)]


def normalized(source, gain):
    values_f = source.astype(jnp.float32)
    mean_square = jnp.mean(values_f * values_f, axis=-1, keepdims=True)
    return (values_f * lax.rsqrt(mean_square + 1e-06) * gain).astype(jnp.bfloat16)


def places(frames, rows, columns, margin):
    grid = np.meshgrid(
        np.arange(-margin, frames + margin),
        np.arange(-margin, rows + margin),
        np.arange(columns) // TW,
        indexing="ij",
    )
    return np.stack([axis.reshape(-1) for axis in grid]).astype(np.int32)


def ring_kernel(
    heads,
    group,
    time_ref,
    rows_ref,
    cols_ref,
    raw_query_ref,
    key_ref,
    query_gain_ref,
    key_gain_ref,
    query_place_ref,
    key_place_ref,
    gate_ref,
    value_ref,
    weight_ref,
    hidden_in_ref,
    out_ref,
    query_ref,
    mask_ref,
    hidden_ref,
    region,
    weights,
    mixed,
    total,
    outgoing,
    incoming,
    local_sem,
    own_sem,
    halo_send,
    halo_recv,
    near_send,
    pair_send,
    weight_recv,
    mixed_send,
    mixed_recv,
    back_send,
    back_recv,
):
    t = lax.axis_index("tm")
    s = lax.axis_index("space")
    nt = lax.axis_size("tm")
    ns = lax.axis_size("space")
    chips = ns // 2
    frames, rows, columns, inner = value_ref.shape
    tokens = frames * rows * columns
    keys_here = (frames + 2) * (rows + 2) * columns
    width = inner // heads
    depth, cols = weight_ref.shape

    def remote(source, target, send, recv, tm, space):
        return pltpu.make_async_remote_copy(
            src_ref=source,
            dst_ref=target,
            send_sem=send,
            recv_sem=recv,
            device_id=(tm, space),
            device_id_type=pl.DeviceIdType.MESH,
        )

    has_low_t, has_high_t = t > 0, t < nt - 1
    has_low_s, has_high_s = s > 0, s < ns - 1
    own_f, own_r = pl.ds(1, frames), pl.ds(1, rows)

    def halo(i, source, target, tm, space):
        return remote(source, target, halo_send.at[i], halo_recv.at[i], tm, space)

    straight = []
    for part, whole in ((1, value_ref), (0, region.at[0, own_f, own_r])):
        straight += [
            (halo(4 * part, whole.at[frames - 1], region.at[part, 0, own_r], t + 1, s), has_high_t, has_low_t),
            (halo(4 * part + 1, whole.at[0], region.at[part, frames + 1, own_r], t - 1, s), has_low_t, has_high_t),
            (halo(4 * part + 2, whole.at[:, rows - 1], region.at[part, own_f, 0], t, s + 1), has_high_s, has_low_s),
            (halo(4 * part + 3, whole.at[:, 0], region.at[part, own_f, rows + 1], t, s - 1), has_low_s, has_high_s),
        ]
    corners = []
    for i, (frame, has_frame) in enumerate(((0, has_low_t), (frames + 1, has_high_t))):
        corners.append((
            halo(8 + 2 * i, region.at[:, frame, rows], region.at[:, frame, 0], t, s + 1),
            has_frame & has_high_s, has_frame & has_low_s,
        ))
        corners.append((
            halo(9 + 2 * i, region.at[:, frame, 1], region.at[:, frame, rows + 1], t, s - 1),
            has_frame & has_low_s, has_frame & has_high_s,
        ))
    parts, lane = weights.shape[0], weights.shape[2]

    def block(b, p):
        return weights.at[p, pl.ds(pl.multiple_of(b * depth, depth), depth)]

    def own_block(p):
        return weight_ref.at[:, pl.ds(pl.multiple_of(p * lane, lane), lane)]

    partner = s + 1 - 2 * lax.rem(s, 2)

    def near(k, b, way, p, first):
        space = s + 2 if way == 0 else s - 2
        source = own_block(p) if first else block(b, p)
        return remote(source, block(b, p), near_send.at[way, k, p], weight_recv.at[b, p], t, space)

    def pair(k, b, way, p, first):
        source = own_block(p) if first else block(b, p)
        return remote(source, block(b, p), pair_send.at[way, k, p], weight_recv.at[b, p], t, partner)

    def arrived(b, p):
        remote(block(b, p), block(b, p), pair_send.at[0, 0, p], weight_recv.at[b, p], t, partner).wait_recv()

    def each_part(low, high, run):
        def body(p, carry):
            run(p)
            return carry

        lax.fori_loop(low, high, body, 0)

    for copy, sends, _ in straight[:4]:
        pl.when(sends)(copy.start)

    def first_part(p):
        pl.when(s + 2 < ns)(near(0, s, 0, p, True).start)
        pl.when(s >= 2)(near(0, s, 1, p, True).start)
        pair(0, s, 0, p, True).start()
        pltpu.make_async_copy(own_block(p), block(s, p), own_sem.at[p]).start()

    each_part(0, parts, first_part)
    own_value = pltpu.make_async_copy(value_ref, region.at[1, own_f, own_r], local_sem.at[0])
    own_value.start()
    own_hidden = pltpu.make_async_copy(hidden_in_ref, hidden_ref, local_sem.at[1])
    own_hidden.start()

    step = 16 if columns % 16 == 0 else columns
    for frame in range(frames):
        for row in range(rows):
            for column in range(0, columns, step):
                at = slice(column, column + step)
                region[0, 1 + frame, 1 + row, at] = normalized(key_ref[frame, row, at], key_gain_ref[...])

    def query_rows(i, carry):
        at = pl.ds(pl.multiple_of(i * 16, 16), 16)
        query_ref[at] = normalized(raw_query_ref[at], query_gain_ref[...])
        return carry

    lax.fori_loop(0, tokens // 16, query_rows, 0)
    for copy, sends, _ in straight[4:]:
        pl.when(sends)(copy.start)

    def clear_frame(frame):
        def run():
            for part in range(2):
                for row in range(rows + 2):
                    region[part, frame, row] = jnp.zeros((columns, inner), jnp.bfloat16)
        return run

    def clear_row(row):
        def run():
            for part in range(2):
                for frame in range(frames + 2):
                    region[part, frame, row] = jnp.zeros((columns, inner), jnp.bfloat16)
        return run

    pl.when(jnp.logical_not(has_low_t))(clear_frame(0))
    pl.when(jnp.logical_not(has_high_t))(clear_frame(frames + 1))
    pl.when(jnp.logical_not(has_low_s))(clear_row(0))
    pl.when(jnp.logical_not(has_high_s))(clear_row(rows + 1))

    frame_k, row_k, tile_k = key_place_ref[0:1], key_place_ref[1:2], key_place_ref[2:3]
    inside = (frame_k >= -t * frames) & (frame_k < (nt - t) * frames)
    inside = inside & (row_k >= -s * rows) & (row_k < (ns - s) * rows)
    outside = jnp.where(inside, 0, 9)
    frame_gap = jnp.abs(query_place_ref[:, 0:1] - frame_k) + outside
    row_gap = jnp.abs(query_place_ref[:, 1:2] - row_k)
    tile_gap = jnp.abs(query_place_ref[:, 2:3] - tile_k)
    for i, (reach_t, reach_r, reach_c) in enumerate(REACHES):
        allowed = (frame_gap <= reach_t) & (row_gap <= reach_r) & (tile_gap <= reach_c)
        mask_ref[i] = jnp.where(allowed, 0.0, -1e30)

    def relay(k, p):
        low, high = s - 2 * k, s + 2 * k

        @pl.when(low >= 0)
        def _():
            arrived(low, p)
            pl.when(s + 2 < ns)(near(k, low, 0, p, False).start)
            pair(k, low, 0, p, False).start()

        @pl.when(high < ns)
        def _():
            arrived(high, p)
            pl.when(s >= 2)(near(k, high, 1, p, False).start)
            pair(k, high, 1, p, False).start()

    def relay_parts(k, low, high):
        if 1 <= k < chips:
            each_part(low, high, functools.partial(relay, k))

    early = parts // 2
    last = chips - 1
    if last > 1:
        relay_parts(1, 0, early)
    for copy, _, receives in straight[0:2] + straight[4:6]:
        pl.when(receives)(copy.wait_recv)
    for copy, sends, _ in corners:
        pl.when(sends)(copy.start)
    for copy, _, receives in straight[2:4] + straight[6:8]:
        pl.when(receives)(copy.wait_recv)
    for copy, _, receives in corners:
        pl.when(receives)(copy.wait_recv)
    if last > 1:
        relay_parts(1, early, parts)
    own_value.wait()

    groups = heads // group
    span = group * width

    def gather(g, d):
        at = (t, slice(None), pl.ds(pl.multiple_of(g * span, span), span))
        return remote(
            mixed.at[at], mixed.at[at], mixed_send.at[d - 1, g], mixed_recv.at[t, g],
            lax.rem(t + d, nt), s,
        )

    def one_group(g, carry):
        for i in range(group):
            h = g * group + i
            lanes = pl.ds(pl.multiple_of(h * width, width), width)
            query = query_ref[:, lanes]
            key = region[0, :, :, :, lanes].reshape(keys_here, width)
            value = region[1, :, :, :, lanes].reshape(keys_here, width)
            scores = lax.dot_general(
                query, key, (((1,), (1,)), ((), ())), preferred_element_type=jnp.float32
            ) * width ** (-0.5)
            scores = scores + mask_ref[time_ref[h] * 6 + rows_ref[h] * 3 + cols_ref[h]]
            part = jnp.exp(scores - jnp.max(scores, axis=1, keepdims=True))
            sums = jnp.sum(part, axis=1, keepdims=True)
            result = jnp.dot(part.astype(jnp.bfloat16), value, preferred_element_type=jnp.float32)
            mixed[t, :, lanes] = (result / sums).astype(jnp.bfloat16)
        for d in range(1, nt):
            gather(g, d).start()
        return carry

    ahead = groups * 5 // 8
    lax.fori_loop(0, ahead, one_group, 0)
    if last > 2:
        relay_parts(2, 0, parts)
    lax.fori_loop(ahead, groups, one_group, 0)
    for k in range(3, last):
        relay_parts(k, 0, parts)

    def gathered(g, carry):
        for d in range(1, nt):
            other = lax.rem(t + d, nt)
            at = (other, slice(None), pl.ds(pl.multiple_of(g * span, span), span))
            remote(mixed.at[at], mixed.at[at], mixed_send.at[d - 1, g], mixed_recv.at[other, g], t, s).wait_recv()
        return carry

    chip_depth = 2 * depth
    piece = chip_depth * 128 // math.gcd(chip_depth, 128)

    def multiply(start, p, first):
        feature = pl.ds(pl.multiple_of(start, piece), piece)
        left = mixed[:, :, feature].reshape(nt * tokens, piece)
        product = jnp.dot(left, weights[p, feature], preferred_element_type=jnp.float32)
        if first:
            total[p] = product
        else:
            total[p] += product

    chip = s // 2
    half = lax.rem(s, 2)

    def add(k, p):
        for other in (chip - k, chip + k):
            @pl.when((other >= 0) & (other < chips))
            def _():
                arrived(2 * other + 1 - half, p)
                multiply(other * piece, p, False)

    def own_rows(owner):
        return pl.ds(pl.multiple_of(owner * tokens, tokens), tokens)

    def back(d, p):
        other = lax.rem(t + d, nt)
        return remote(
            outgoing.at[d - 1, p], incoming.at[d - 1, p], back_send.at[d - 1, p], back_recv.at[d - 1, p], other, s
        )

    def send_back(p):
        for d in range(1, nt):
            outgoing[d - 1, p] = total[p, own_rows(lax.rem(t + d, nt)), :].astype(jnp.bfloat16)
            back(d, p).start()

    def own_part(p):
        pltpu.make_async_copy(own_block(p), block(s, p), own_sem.at[p]).wait()
        arrived(partner, p)

    lax.fori_loop(0, groups, gathered, 0)
    if piece == chip_depth:
        def begin(p):
            own_part(p)
            multiply(chip * piece, p, True)
            for k in range(1, last):
                add(k, p)

        each_part(0, parts, begin)

        def conclude(p):
            if last > 0:
                relay(last, p)
                add(last, p)
            send_back(p)

        each_part(0, parts, conclude)
    else:
        def conclude(p):
            own_part(p)
            if last > 0:
                relay(last, p)
            for k in range(1, chips):
                for other in (chip - k, chip + k):
                    @pl.when((other >= 0) & (other < chips))
                    def _():
                        arrived(2 * other + 1 - half, p)
            multiply(0, p, True)

            def add_piece(i, carry):
                multiply(i * piece, p, False)
                return carry

            lax.fori_loop(1, inner // piece, add_piece, 0)
            send_back(p)

        each_part(0, parts, conclude)

    own_hidden.wait()

    def finish(owner, p, branch):
        lanes = pl.ds(pl.multiple_of(owner * cols + p * lane, lane), lane)
        out_ref[:, lanes] = (
            hidden_ref[:, lanes].astype(jnp.float32) + gate_ref[:, lanes] * branch
        ).astype(jnp.bfloat16)

    def finish_own(p):
        finish(t, p, total[p, own_rows(t), :])

    def finish_others(p):
        for d in range(1, nt):
            back(d, p).wait_recv()
            finish(lax.rem(t + nt - d, nt), p, incoming[d - 1, p].astype(jnp.float32))

    each_part(0, parts, finish_own)
    each_part(0, parts, finish_others)

    for copy, sends, _ in straight + corners:
        pl.when(sends)(copy.wait_send)
    for k in range(chips):
        low, high = s - 2 * k, s + 2 * k

        def weight_sent(p):
            pl.when((low >= 0) & (s + 2 < ns))(near(k, low, 0, p, k == 0).wait_send)
            pl.when((high < ns) & (s >= 2))(near(k, high, 1, p, k == 0).wait_send)
            pl.when(low >= 0)(pair(k, low, 0, p, k == 0).wait_send)
            if k > 0:
                pl.when(high < ns)(pair(k, high, 1, p, False).wait_send)

        each_part(0, parts, weight_sent)

    def sent(g, carry):
        for d in range(1, nt):
            gather(g, d).wait_send()
        return carry

    lax.fori_loop(0, groups, sent, 0)

    def back_sent(p):
        for d in range(1, nt):
            back(d, p).wait_send()

    each_part(0, parts, back_sent)


def ring_shards(
    hidden_in,
    queries,
    keys,
    values,
    query_gain,
    key_gain,
    reach_time,
    reach_rows,
    reach_cols,
    out_weight,
    gate,
):
    frames, rows, columns, inner = queries.shape
    width = hidden_in.shape[3]
    heads = reach_time.shape[0]
    tokens = frames * rows * columns
    nt, ns = lax.axis_size("tm"), lax.axis_size("space")
    depth, cols = out_weight.shape
    group = 5 if heads % 5 == 0 else 1
    vmem = pl.BlockSpec(memory_space=pltpu.VMEM)
    hbm = pl.BlockSpec(memory_space=pl.ANY)
    dma = pltpu.SemaphoreType.DMA
    lane = 256 if cols % 256 == 0 else 128
    parts = cols // lane
    output = pl.pallas_call(
        functools.partial(ring_kernel, heads, group),
        out_shape=jax.ShapeDtypeStruct((tokens, width), jnp.bfloat16),
        in_specs=[pl.BlockSpec(memory_space=pltpu.SMEM)] * 3 + [vmem] * 7 + [hbm] * 3,
        out_specs=vmem,
        scratch_shapes=[
            pltpu.VMEM((tokens, inner), jnp.bfloat16),
            pltpu.VMEM((len(REACHES), tokens, (frames + 2) * (rows + 2) * columns), jnp.float32),
            pltpu.VMEM((tokens, width), jnp.bfloat16),
            pltpu.VMEM((2, frames + 2, rows + 2, columns, inner), jnp.bfloat16),
            pltpu.VMEM((parts, depth * ns, lane), jnp.bfloat16),
            pltpu.VMEM((nt, tokens, inner), jnp.bfloat16),
            pltpu.VMEM((parts, nt * tokens, lane), jnp.float32),
            pltpu.VMEM((nt - 1, parts, tokens, lane), jnp.bfloat16),
            pltpu.VMEM((nt - 1, parts, tokens, lane), jnp.bfloat16),
            dma((2,)),
            dma((parts,)),
            dma((12,)),
            dma((12,)),
            dma((2, ns // 2, parts)),
            dma((2, ns // 2, parts)),
            dma((ns, parts)),
            dma((nt - 1, heads // group)),
            dma((nt, heads // group)),
            dma((nt - 1, parts)),
            dma((nt - 1, parts)),
        ],
        compiler_params=pltpu.CompilerParams(
            has_side_effects=True, vmem_limit_bytes=60 * 1024 * 1024
        ),
    )(
        reach_time,
        reach_rows,
        reach_cols,
        queries.reshape(tokens, inner),
        keys,
        query_gain.reshape(1, inner),
        key_gain.reshape(1, inner),
        places(frames, rows, columns, 0).T,
        places(frames, rows, columns, 1),
        gate.reshape(1, width),
        values,
        out_weight,
        hidden_in.reshape(tokens, width),
    )
    return output.reshape(frames, rows, columns, width)


def pair_kernel(
    heads,
    time_ref,
    rows_ref,
    cols_ref,
    query_gain_ref,
    key_gain_ref,
    query_place_ref,
    key_place_ref,
    gate_ref,
    raw_query_ref,
    raw_key_ref,
    value_ref,
    weight_ref,
    hidden_in_ref,
    out_ref,
    raw,
    normed,
    region,
    query_ref,
    mask_ref,
    mixed,
    weights,
    total,
    partial_out,
    partial_in,
    outgoing,
    incoming,
    hidden_ref,
    staged,
    local_sem,
    value_sem,
    own_sem,
    swap_send,
    swap_recv,
    side_send,
    side_recv,
    corner_send,
    corner_recv,
    stage_recv,
    near_send,
    cross_send,
    pair_send,
    weight_recv,
    level_send,
    level_recv,
    mixed_send,
    mixed_recv,
    part_send,
    part_recv,
    back_send,
    back_recv,
):
    t = lax.axis_index("tm")
    s = lax.axis_index("space")
    nt = lax.axis_size("tm")
    ns = lax.axis_size("space")
    frames, rows, columns, inner = value_ref.shape
    tokens = frames * rows * columns
    depth, cols = weight_ref.shape
    width = inner // heads
    groups = ns // 2
    half = inner // 2
    blocks, parts, _, lane = weights.shape
    chips = ns // 4
    row_tokens = rows * columns
    span = 2 * frames

    p = lax.rem(t, 2)
    column_block = lax.div(t, 2)
    c = lax.rem(s, 2)
    z = lax.div(s, 2)
    level = lax.rem(z, 2)
    chip = lax.div(z, 2)
    mate = t + 1 - 2 * p
    partner = s + 1 - 2 * c
    level_mate = s + 2 - 4 * level

    has_low_t, has_high_t = t >= 2, t < nt - 2
    has_low_s, has_high_s = s > 0, s < ns - 1

    def remote(source, target, send, recv, tm, space):
        return pltpu.make_async_remote_copy(
            src_ref=source,
            dst_ref=target,
            send_sem=send,
            recv_sem=recv,
            device_id=(tm, space),
            device_id_type=pl.DeviceIdType.MESH,
        )

    def lanes_at(start, size):
        return pl.ds(pl.multiple_of(start, 128), size)

    def other_column(e):
        return lax.rem(column_block + e, blocks)

    def other_chip(d):
        return lax.rem(chip + d, chips)

    def column_device(e):
        return 2 * other_column(e) + p

    def chip_device(d):
        return 4 * other_chip(d) + 2 * level + c

    levels = 2 * chips
    middle = levels // 2

    def comes_late(d):
        rises = other_chip(d) < chip
        return (rises & (z <= middle)) | (jnp.logical_not(rises) & (z + 1 >= middle))

    starts = {True: z + 2 < levels, False: z >= 2}
    passes = {True: (z >= 1) & (z + 1 < levels), False: (z + 1 < levels) & (z >= 1)}
    inner = {True: z < middle, False: z >= middle}

    load_key = pltpu.make_async_copy(raw_key_ref, raw.at[0], local_sem.at[0])
    load_key.start()
    load_query = pltpu.make_async_copy(raw_query_ref, raw.at[1], local_sem.at[1])
    load_query.start()

    barrier = pltpu.get_barrier_semaphore()

    def greet(tm, space):
        pl.semaphore_signal(
            barrier, inc=1, device_id=(tm, space), device_id_type=pl.DeviceIdType.MESH
        )

    greet(mate, s)
    greet(t, partner)
    greet(t, level_mate)
    for e in range(1, blocks):
        greet(column_device(e), s)
    across = s - 2 + 4 * level
    has_across = (across >= 0) & (across < ns)
    pl.when(has_across)(functools.partial(greet, t, across))
    up, down = (c == 1) & has_high_s, (c == 0) & has_low_s

    @pl.when(up)
    def _():
        greet(t, s + 1)

    @pl.when(down)
    def _():
        greet(t, s - 1)

    pl.semaphore_wait(
        barrier, blocks + 2 + has_across.astype(jnp.int32) + (up | down).astype(jnp.int32)
    )

    own_frames = pl.ds(1 + frames * p, frames)
    own_rows = pl.ds(1, rows)

    def group_lanes(b):
        return pl.ds(b * depth, depth)

    def value_swap(b):
        source = value_ref.at[:, :, :, lanes_at((2 * b + 1 - p) * depth, depth)]
        target = region.at[1, own_frames, own_rows, :, group_lanes(b)]
        return remote(source, target, swap_send.at[1, b], swap_recv.at[1, b], mate, s)

    def key_swap(b):
        source = normed.at[0, 1 - p, :, :, :, group_lanes(b)]
        target = region.at[0, own_frames, own_rows, :, group_lanes(b)]
        return remote(source, target, swap_send.at[0, b], swap_recv.at[0, b], mate, s)

    def query_swap(b):
        source = normed.at[1, 1 - p, :, :, :, group_lanes(b)]
        target = query_ref.at[pl.ds(frames * p, frames), :, :, group_lanes(b)]
        return remote(source, target, swap_send.at[2, b], swap_recv.at[2, b], mate, s)

    def own_value(b):
        return pltpu.make_async_copy(
            value_ref.at[:, :, :, lanes_at((2 * b + p) * depth, depth)],
            region.at[1, own_frames, own_rows, :, group_lanes(b)],
            value_sem.at[b],
        )

    def own_weight(q):
        return weight_ref.at[:, pl.ds(q * lane, lane)]

    def own_weight_at(q):
        return weight_ref.at[:, lanes_at(q * lane, lane)]

    def weight_block(block, chip_index, core, q):
        start = (2 * chip_index + core) * depth
        return weights.at[block, q, pl.ds(pl.multiple_of(start, depth), depth)]

    def arrival(chip_index, core):
        return 2 * chip_index + core

    def keep_weight(q):
        return pltpu.make_async_copy(
            own_weight_at(q), weight_block(column_block, chip, c, q), own_sem.at[q]
        )

    def first_hop(rising, q):
        return remote(
            own_weight_at(q), staged.at[int(rising), q],
            near_send.at[0, int(rising), q], stage_recv.at[int(rising), q],
            t, s + 2 if rising else s - 2,
        )

    def second_hop(rising, q):
        origin = lax.div(z + levels - 1 if rising else z + levels + 1, 2) - chips
        return remote(
            staged.at[int(rising), q], weight_block(column_block, origin, c, q),
            near_send.at[1, int(rising), q],
            weight_recv.at[column_block, arrival(origin, c), q],
            t, s + 2 if rising else s - 2,
        )

    def cross_weight(e, d, q):
        block = weight_block(column_block, other_chip(d), c, q)
        source = own_weight_at(q) if d == 0 else block
        return remote(
            source, block, cross_send.at[e - 1, d, q],
            weight_recv.at[column_block, arrival(other_chip(d), c), q],
            column_device(e), s,
        )

    def pair_weight(e, d, q):
        block = weight_block(other_column(e), other_chip(d), c, q)
        source = own_weight_at(q) if e == 0 and d == 0 else block
        return remote(
            source, block, pair_send.at[e, d, q],
            weight_recv.at[other_column(e), arrival(other_chip(d), c), q],
            t, partner,
        )

    def weight_here(e, d, core, q):
        block = weight_block(other_column(e), other_chip(d), core, q)
        remote(
            block, block, pair_send.at[e, d, q],
            weight_recv.at[other_column(e), arrival(other_chip(d), core), q], t, partner,
        ).wait_recv()

    at_end = (z == 0) | (z == levels - 1)

    def send_far(q, ends, which=True):
        for rising in (True, False):
            pl.when(starts[rising] & (at_end == ends) & which)(first_hop(rising, q).start)

    def forward(q, inward, which=True):
        for rising in (True, False):
            @pl.when(passes[rising] & (inner[rising] == inward) & which)
            def _(rising=rising):
                first_hop(rising, q).wait_recv()
                second_hop(rising, q).start()

    def send_cross(q):
        for e in range(1, blocks):
            cross_weight(e, 0, q).start()
        pair_weight(0, 0, q).start()

    def relay_far(q, late):
        for d in range(1, chips):
            @pl.when(comes_late(d) if late else jnp.logical_not(comes_late(d)))
            def _(d=d):
                weight_here(0, d, c, q)
                for e in range(1, blocks):
                    cross_weight(e, d, q).start()
                pair_weight(0, d, q).start()

    def relay_cross(q, far):
        for e in range(1, blocks):
            for d in range(1, chips) if far else (0,):
                weight_here(e, d, c, q)
                pair_weight(e, d, q).start()

    value_swap(0).start()
    for b in range(groups):
        own_value(b).start()
    send_far(0, True)
    send_far(0, False)
    send_cross(0)
    for q in range(parts):
        keep_weight(q).start()
    own_hidden = pltpu.make_async_copy(hidden_in_ref, hidden_ref, local_sem.at[2])
    own_hidden.start()

    step = 16 if columns % 16 == 0 else columns

    def normalize(index, gain_ref):
        for frame in range(frames):
            for row in range(rows):
                for column in range(0, columns, step):
                    at = slice(column, column + step)
                    result = normalized(raw[index, frame, row, at], gain_ref[...])
                    for b in range(groups):
                        for core in range(2):
                            start = (2 * b + core) * depth
                            normed[index, core, frame, row, at, b * depth:(b + 1) * depth] = (
                                result[:, start:start + depth]
                            )

    load_key.wait()
    with jax.named_scope("normalize_key"):
        normalize(0, key_gain_ref)
    key_swap(0).start()
    own_key = pltpu.make_async_copy(
        normed.at[0, p], region.at[0, own_frames, own_rows], local_sem.at[3]
    )
    own_key.start()
    load_query.wait()
    with jax.named_scope("normalize_query"):
        normalize(1, query_gain_ref)
    query_swap(0).start()
    own_query = pltpu.make_async_copy(
        normed.at[1, p], query_ref.at[pl.ds(frames * p, frames)], local_sem.at[4]
    )
    own_query.start()
    for b in range(1, groups):
        value_swap(b).start()
        key_swap(b).start()
        query_swap(b).start()

    def clear_frame(frame):
        def run():
            for part in range(2):
                for row in range(rows + 2):
                    region[part, frame, row] = jnp.zeros((columns, half), jnp.bfloat16)
        return run

    def clear_row(row):
        def run():
            for part in range(2):
                for frame in range(span + 2):
                    region[part, frame, row] = jnp.zeros((columns, half), jnp.bfloat16)
        return run

    pl.when(jnp.logical_not(has_low_t))(clear_frame(0))
    pl.when(jnp.logical_not(has_high_t))(clear_frame(span + 1))
    pl.when(jnp.logical_not(has_low_s))(clear_row(0))
    pl.when(jnp.logical_not(has_high_s))(clear_row(rows + 1))

    frame_k, row_k, tile_k = key_place_ref[0:1], key_place_ref[1:2], key_place_ref[2:3]
    inside = (row_k >= -s * rows) & (row_k < (ns - s) * rows)
    row_gap = jnp.abs(query_place_ref[:, 0:1] - row_k) + jnp.where(inside, 0, 9)
    tile_gap = jnp.abs(query_place_ref[:, 1:2] - tile_k)
    low_gap = jnp.where(has_low_t, 0, 9) * (frame_k < 0).astype(jnp.int32)
    high_gap = jnp.where(has_high_t, 0, 9) * (frame_k > 0).astype(jnp.int32)
    for kind, edge in enumerate((jnp.zeros_like(low_gap), low_gap, high_gap)):
        frame_gap = jnp.abs(frame_k) + edge
        for i, (reach_t, reach_r, reach_c) in enumerate(REACHES):
            allowed = (frame_gap <= reach_t) & (row_gap <= reach_r) & (tile_gap <= reach_c)
            mask_ref[kind, i] = jnp.where(allowed, 0.0, -1e30)

    pair_frames = pl.ds(1, span)

    def row_up(b):
        return remote(
            region.at[:, pair_frames, rows, :, group_lanes(b)],
            region.at[:, pair_frames, 0, :, group_lanes(b)],
            side_send.at[0, b], side_recv.at[0, b], t, s + 1,
        )

    def row_down(b):
        return remote(
            region.at[:, pair_frames, 1, :, group_lanes(b)],
            region.at[:, pair_frames, rows + 1, :, group_lanes(b)],
            side_send.at[1, b], side_recv.at[1, b], t, s - 1,
        )

    def frame_up(b):
        return remote(
            region.at[:, span, own_rows, :, group_lanes(b)],
            region.at[:, 0, own_rows, :, group_lanes(b)],
            side_send.at[2, b], side_recv.at[2, b], t + 2, s,
        )

    def frame_down(b):
        return remote(
            region.at[:, 1, own_rows, :, group_lanes(b)],
            region.at[:, span + 1, own_rows, :, group_lanes(b)],
            side_send.at[3, b], side_recv.at[3, b], t - 2, s,
        )

    def sides(b):
        return (
            (frame_up(b), has_high_t, has_low_t),
            (frame_down(b), has_low_t, has_high_t),
            (row_up(b), has_high_s, has_low_s),
            (row_down(b), has_low_s, has_high_s),
        )

    def corners(b):
        result = []
        for i, (frame, has_frame) in enumerate(((0, has_low_t), (span + 1, has_high_t))):
            for j, (row, landing, space, sends, receives) in enumerate((
                (rows, 0, s + 1, has_high_s, has_low_s),
                (1, rows + 1, s - 1, has_low_s, has_high_s),
            )):
                copy = remote(
                    region.at[:, frame, row, :, group_lanes(b)],
                    region.at[:, frame, landing, :, group_lanes(b)],
                    corner_send.at[2 * i + j, b], corner_recv.at[2 * i + j, b], t, space,
                )
                result.append((copy, has_frame & sends, has_frame & receives))
        return result

    def feature_lanes(index, core):
        return lanes_at((2 * index + core) * depth, depth)

    def to_level_mate(j):
        at = (slice(None), feature_lanes(j, p))
        return remote(
            mixed.at[(2,) + at], mixed.at[(level,) + at],
            level_send.at[j], level_recv.at[j], t, level_mate,
        )

    def from_level_mate(j):
        at = (1 - level, slice(None), feature_lanes(j, p))
        return remote(mixed.at[at], mixed.at[at], level_send.at[j], level_recv.at[j], t, level_mate)

    def to_mate(which, j):
        at = (which, slice(None), feature_lanes(j, p))
        return remote(
            mixed.at[at], mixed.at[at], mixed_send.at[which, j], mixed_recv.at[which, j], mate, s
        )

    def from_mate(which, j):
        at = (which, slice(None), feature_lanes(j, 1 - p))
        remote(
            mixed.at[at], mixed.at[at], mixed_send.at[which, j], mixed_recv.at[which, j], mate, s
        ).wait_recv()

    def attend(b):
        in_level = level == b % 2
        place = jnp.where(in_level, level, 2)
        index = b // 2
        group = depth // width

        def one_head(i, carry):
            h = (2 * b + p) * group + i
            lanes = lanes_at(b * depth + i * width, width)
            reach = time_ref[h] * 6 + rows_ref[h] * 3 + cols_ref[h]
            target = lanes_at((2 * index + p) * depth + i * width, width)
            scores, values = [], []
            for frame in range(span):
                query = query_ref[frame, :, :, lanes].reshape(row_tokens, width)
                near = slice(frame, frame + 3)
                key = region[0, near, :, :, lanes].reshape(-1, width)
                values.append(region[1, near, :, :, lanes].reshape(-1, width))
                scores.append(lax.dot_general(
                    query, key, (((1,), (1,)), ((), ())), preferred_element_type=jnp.float32
                ))
            results = []
            for frame in range(span):
                kind = 1 if frame == 0 else 2 if frame == span - 1 else 0
                masked = scores[frame] * width ** (-0.5) + mask_ref[kind, reach]
                part = jnp.exp(masked - jnp.max(masked, axis=1, keepdims=True))
                sums = jnp.sum(part, axis=1, keepdims=True)
                result = jnp.dot(
                    part.astype(jnp.bfloat16), values[frame], preferred_element_type=jnp.float32
                )
                results.append((result / sums).astype(jnp.bfloat16))
            mixed[place, :, target] = jnp.concatenate(results, axis=0)
            return carry

        lax.fori_loop(0, group, one_head, 0)

    def send_mixed(b):
        pl.when(level != b % 2)(to_level_mate(b // 2).start)

    def relay_mixed(b):
        @pl.when(level == b % 2)
        def _():
            from_level_mate(b // 2).wait_recv()
            to_mate(1 - level, b // 2).start()
            to_mate(level, b // 2).start()

    def arrive(i):
        with jax.named_scope(f"wait_swap{i}"):
            value_swap(i).wait_recv()
            key_swap(i).wait_recv()
            own_value(i).wait()
            if i == 0:
                own_key.wait()
        with jax.named_scope(f"send_sides{i}"):
            for copy, sends, _ in sides(i):
                pl.when(sends)(copy.start)

    def turn(i):
        with jax.named_scope(f"wait_frames{i}"):
            for copy, _, receives in sides(i)[:2]:
                pl.when(receives)(copy.wait_recv)
        for copy, sends, _ in corners(i):
            pl.when(sends)(copy.start)

    def ready(b):
        with jax.named_scope(f"wait_query{b}"):
            query_swap(b).wait_recv()
            if b == 0:
                own_query.wait()
        with jax.named_scope(f"wait_rows{b}"):
            for copy, _, receives in sides(b)[2:]:
                pl.when(receives)(copy.wait_recv)
        with jax.named_scope(f"wait_corners{b}"):
            for copy, _, receives in corners(b):
                pl.when(receives)(copy.wait_recv)

    early = min(2, parts)
    actions = {
        "end": lambda q: send_far(q, True),
        "end0": lambda q: send_far(q, True, level == 0),
        "end1": lambda q: send_far(q, True, level == 1),
        "out0": lambda q: forward(q, False, level == 0),
        "out1": lambda q: forward(q, False, level == 1),
        "mid": lambda q: send_far(q, False),
        "late": lambda q: relay_far(q, True),
        "cross": send_cross,
        "out": lambda q: forward(q, False),
        "in": lambda q: forward(q, True),
        "early": lambda q: relay_far(q, False),
    }
    plan = {i: [] for i in range(groups + 1)}
    plan[0] += [("mid", 1), ("end", 1), ("cross", 1), ("out", 0)]
    plan[1] += [("mid", 2), ("end0", 2), ("cross", 2), ("out0", 1)]
    plan[2] += [("mid", 3), ("end1", 2), ("cross", 3), ("out1", 1)]
    plan[3] += [("in", 0), ("mid", 4), ("end0", 3), ("out0", 2), ("cross", 4), ("early", 0), ("early", 1)]
    plan[groups] += [("in", 1), ("end1", 3), ("end", 4), ("out1", 2), ("out", 3), ("late", 0)]
    plan[groups] += [("cross", q) for q in range(5, parts)]
    for i in range(groups + 1):
        if i < groups:
            arrive(i)
        if i > 0:
            ready(i - 1)
            with jax.named_scope(f"attend{i - 1}"):
                attend(i - 1)
        if i < groups:
            turn(i)
        if i > 0:
            send_mixed(i - 1)
        for kind, q in plan[i]:
            if q < parts:
                actions[kind](q)
        if i > 1:
            with jax.named_scope(f"relay_mixed{i}"):
                relay_mixed(i - 2)
        if i > 1 and i - 2 < parts:
            with jax.named_scope(f"relay_cross{i}"):
                relay_cross(i - 2, False)
    with jax.named_scope("relay_mixed_last"):
        relay_mixed(groups - 1)

    def each_part(low, high, run):
        def body(q, carry):
            run(q)
            return carry

        lax.fori_loop(low, high, body, 0)

    def next_far(q):
        if q < parts:
            with jax.named_scope(f"relay_far{q}"):
                relay_far(q, True)

    def multiply_theirs(e, q):
        block = other_column(e)
        for d in range(chips):
            weight_here(e, d, 1 - c, q)
        product = jnp.dot(
            mixed[1 - level], weights[block, q], preferred_element_type=jnp.float32
        )
        partial_out[block, q] = product.astype(jnp.bfloat16)
        part_copy(block, q).start()

    def multiply_ours(e, q):
        block = other_column(e)
        total[block, q] = jnp.dot(
            mixed[level], weights[block, q], preferred_element_type=jnp.float32
        )

    def part_copy(block, q):
        return remote(
            partial_out.at[block, q], partial_in.at[block, q],
            part_send.at[block, q], part_recv.at[block, q], t, level_mate,
        )

    def back(block, q):
        return remote(
            outgoing.at[block, q], incoming.at[block, q],
            back_send.at[block, q], back_recv.at[block, q], mate, s,
        )

    def token_rows(side):
        return pl.ds(pl.multiple_of(side * tokens, tokens), tokens)

    def finish(column, branch):
        lanes = lanes_at(column, lane)
        out_ref[:, lanes] = (
            hidden_ref[:, lanes].astype(jnp.float32) + gate_ref[:, lanes] * branch
        ).astype(jnp.bfloat16)

    def reduce_part(q):
        for e in range(blocks):
            block = other_column(e)
            part_copy(block, q).wait_recv()
            theirs = token_rows(1 - p)
            outgoing[block, q] = (
                total[block, q, theirs] + partial_in[block, q, theirs].astype(jnp.float32)
            ).astype(jnp.bfloat16)
            back(block, q).start()
            ours = token_rows(p)
            branch = total[block, q, ours] + partial_in[block, q, ours].astype(jnp.float32)
            finish((2 * block + p) * cols + q * lane, branch)

    def theirs(q):
        if q >= groups - 1:
            relay_cross(q, False)
        keep_weight(q).wait()
        with jax.named_scope(f"theirs{q}own"):
            multiply_theirs(0, q)
        if blocks > 1:
            with jax.named_scope(f"main_cross{q}"):
                relay_cross(q, True)
            with jax.named_scope(f"theirs{q}other"):
                for e in range(1, blocks):
                    multiply_theirs(e, q)

    def ours(q):
        with jax.named_scope(f"ours{q}"):
            for e in range(blocks):
                multiply_ours(e, q)

    forward(2, True)
    relay_far(2, False)
    forward(4, False)
    forward(3, True)
    relay_far(3, False)
    next_far(1)
    with jax.named_scope("from_mate_theirs"):
        for j in range(groups // 2):
            from_mate(1 - level, j)
    theirs(0)
    forward(4, True)
    next_far(2)
    theirs(1)
    relay_far(4, False)
    with jax.named_scope("from_mate_ours"):
        for j in range(groups // 2):
            from_mate(level, j)
    ours(0)
    own_hidden.wait()
    next_far(3)
    theirs(2)
    ours(1)
    with jax.named_scope("reduce0"):
        reduce_part(0)
    next_far(4)
    theirs(3)
    ours(2)
    with jax.named_scope("reduce1"):
        reduce_part(1)
    theirs(4)
    ours(3)
    ours(4)

    def finish_others(q):
        for block in range(blocks):
            back(block, q).wait_recv()
            finish((2 * block + 1 - p) * cols + q * lane, incoming[block, q].astype(jnp.float32))

    with jax.named_scope("reduce2"):
        reduce_part(2)
    with jax.named_scope("finish01"):
        each_part(0, 2, finish_others)
    with jax.named_scope("reduce3"):
        reduce_part(3)
    with jax.named_scope("finish2"):
        finish_others(2)
    with jax.named_scope("reduce4"):
        reduce_part(4)
    with jax.named_scope("finish34"):
        each_part(3, parts, finish_others)

    for b in range(groups):
        value_swap(b).wait_send()
        key_swap(b).wait_send()
        query_swap(b).wait_send()
        for copy, sends, _ in sides(b) + tuple(corners(b)):
            pl.when(sends)(copy.wait_send)
    for j in range(groups // 2):
        to_level_mate(j).wait_send()
        for which in range(2):
            to_mate(which, j).wait_send()

    def sent(q):
        for rising in (True, False):
            pl.when(starts[rising])(first_hop(rising, q).wait_send)
            pl.when(passes[rising])(second_hop(rising, q).wait_send)
        for e in range(blocks):
            for d in range(chips):
                pair_weight(e, d, q).wait_send()
                if e > 0:
                    cross_weight(e, d, q).wait_send()
        for block in range(blocks):
            part_copy(block, q).wait_send()
            back(block, q).wait_send()

    each_part(0, parts, sent)


def pair_shards(
    hidden_in,
    queries,
    keys,
    values,
    query_gain,
    key_gain,
    reach_time,
    reach_rows,
    reach_cols,
    out_weight,
    gate,
):
    frames, rows, columns, inner = queries.shape
    width = hidden_in.shape[3]
    heads = reach_time.shape[0]
    tokens = frames * rows * columns
    nt, ns = lax.axis_size("tm"), lax.axis_size("space")
    depth, cols = out_weight.shape
    lane = 256 if cols % 256 == 0 else 128
    parts = cols // lane
    blocks, chips, groups = nt // 2, ns // 4, ns // 2
    half = inner // 2
    pair_tokens = 2 * tokens
    vmem = pl.BlockSpec(memory_space=pltpu.VMEM)
    hbm = pl.BlockSpec(memory_space=pl.ANY)
    dma = pltpu.SemaphoreType.DMA
    _, query_row, query_tile = places(1, rows, columns, 0)
    key_place = np.stack([axis.reshape(-1) for axis in np.meshgrid(
        np.arange(-1, 2), np.arange(-1, rows + 1), np.arange(columns) // TW, indexing="ij"
    )]).astype(np.int32)
    output = pl.pallas_call(
        functools.partial(pair_kernel, heads),
        out_shape=jax.ShapeDtypeStruct((tokens, width), jnp.bfloat16),
        in_specs=[pl.BlockSpec(memory_space=pltpu.SMEM)] * 3 + [vmem] * 5 + [hbm] * 5,
        out_specs=vmem,
        scratch_shapes=[
            pltpu.VMEM((2, frames, rows, columns, inner), jnp.bfloat16),
            pltpu.VMEM((2, 2, frames, rows, columns, half), jnp.bfloat16),
            pltpu.VMEM((2, 2 * frames + 2, rows + 2, columns, half), jnp.bfloat16),
            pltpu.VMEM((2 * frames, rows, columns, half), jnp.bfloat16),
            pltpu.VMEM((3, len(REACHES), rows * columns, 3 * (rows + 2) * columns), jnp.float32),
            pltpu.VMEM((3, pair_tokens, half), jnp.bfloat16),
            pltpu.VMEM((blocks, parts, half, lane), jnp.bfloat16),
            pltpu.VMEM((blocks, parts, pair_tokens, lane), jnp.float32),
            pltpu.VMEM((blocks, parts, pair_tokens, lane), jnp.bfloat16),
            pltpu.VMEM((blocks, parts, pair_tokens, lane), jnp.bfloat16),
            pltpu.VMEM((blocks, parts, tokens, lane), jnp.bfloat16),
            pltpu.VMEM((blocks, parts, tokens, lane), jnp.bfloat16),
            pltpu.VMEM((tokens, width), jnp.bfloat16),
            pltpu.VMEM((2, parts, depth, lane), jnp.bfloat16),
            dma((5,)),
            dma((groups,)),
            dma((parts,)),
            dma((3, groups)),
            dma((3, groups)),
            dma((4, groups)),
            dma((4, groups)),
            dma((4, groups)),
            dma((4, groups)),
            dma((2, parts)),
            dma((2, 2, parts)),
            dma((max(blocks - 1, 1), chips, parts)),
            dma((blocks, chips, parts)),
            dma((blocks, 2 * chips, parts)),
            dma((groups // 2,)),
            dma((groups // 2,)),
            dma((2, groups // 2)),
            dma((2, groups // 2)),
            dma((blocks, parts)),
            dma((blocks, parts)),
            dma((blocks, parts)),
            dma((blocks, parts)),
        ],
        compiler_params=pltpu.CompilerParams(
            collective_id=0, has_side_effects=True, vmem_limit_bytes=60 * 1024 * 1024
        ),
    )(
        reach_time,
        reach_rows,
        reach_cols,
        query_gain.reshape(1, inner),
        key_gain.reshape(1, inner),
        np.stack([query_row, query_tile]).T,
        key_place,
        gate.reshape(1, width),
        queries,
        keys,
        values,
        out_weight,
        hidden_in.reshape(tokens, width),
    )
    return output.reshape(frames, rows, columns, width)


def shards(hidden_in, queries, keys, values, *others):
    out_weight, reach_time = others[-2], others[2]
    width = queries.shape[3] // reach_time.shape[0]
    nt, ns = lax.axis_size("tm"), lax.axis_size("space")
    whole_heads = out_weight.shape[0] % width == 0
    form = pair_shards if whole_heads and nt % 2 == 0 and ns // 4 == 2 else ring_shards
    return form(hidden_in, queries, keys, values, *others)


def solution(mesh):
    in_specs = (
        P("tm", "space", None, None),
        P("tm", "space", None, None),
        P("tm", "space", None, None),
        P("tm", "space", None, None),
        P(),
        P(),
        P(),
        P(),
        P(),
        P("space", "tm"),
        P(),
    )
    out_specs = P("tm", "space", None, None)
    return jax.shard_map(shards, mesh=mesh, in_specs=in_specs, out_specs=out_specs, check_vma=False)
```

```python
import functools
import math

import jax
import jax.numpy as jnp
import numpy as np
from jax import lax
from jax.experimental import pallas as pl
from jax.experimental.pallas import tpu as pltpu
from jax.sharding import PartitionSpec as P

TW = 8
REACHES = [(a, b, c) for a in range(2) for b in range(2) for c in range(3)]


def normalized(source, gain):
    values_f = source.astype(jnp.float32)
    mean_square = jnp.mean(values_f * values_f, axis=-1, keepdims=True)
    return (values_f * lax.rsqrt(mean_square + 1e-06) * gain).astype(jnp.bfloat16)


def places(frames, rows, columns, margin):
    grid = np.meshgrid(
        np.arange(-margin, frames + margin),
        np.arange(-margin, rows + margin),
        np.arange(columns) // TW,
        indexing="ij",
    )
    return np.stack([axis.reshape(-1) for axis in grid]).astype(np.int32)


def ring_kernel(
    heads,
    group,
    time_ref,
    rows_ref,
    cols_ref,
    raw_query_ref,
    key_ref,
    query_gain_ref,
    key_gain_ref,
    query_place_ref,
    key_place_ref,
    gate_ref,
    value_ref,
    weight_ref,
    hidden_in_ref,
    out_ref,
    query_ref,
    mask_ref,
    hidden_ref,
    region,
    weights,
    mixed,
    total,
    outgoing,
    incoming,
    local_sem,
    own_sem,
    halo_send,
    halo_recv,
    near_send,
    pair_send,
    weight_recv,
    mixed_send,
    mixed_recv,
    back_send,
    back_recv,
):
    t = lax.axis_index("tm")
    s = lax.axis_index("space")
    nt = lax.axis_size("tm")
    ns = lax.axis_size("space")
    chips = ns // 2
    frames, rows, columns, inner = value_ref.shape
    tokens = frames * rows * columns
    keys_here = (frames + 2) * (rows + 2) * columns
    width = inner // heads
    depth, cols = weight_ref.shape

    def remote(source, target, send, recv, tm, space):
        return pltpu.make_async_remote_copy(
            src_ref=source,
            dst_ref=target,
            send_sem=send,
            recv_sem=recv,
            device_id=(tm, space),
            device_id_type=pl.DeviceIdType.MESH,
        )

    has_low_t, has_high_t = t > 0, t < nt - 1
    has_low_s, has_high_s = s > 0, s < ns - 1
    own_f, own_r = pl.ds(1, frames), pl.ds(1, rows)

    def halo(i, source, target, tm, space):
        return remote(source, target, halo_send.at[i], halo_recv.at[i], tm, space)

    straight = []
    for part, whole in ((1, value_ref), (0, region.at[0, own_f, own_r])):
        straight += [
            (halo(4 * part, whole.at[frames - 1], region.at[part, 0, own_r], t + 1, s), has_high_t, has_low_t),
            (halo(4 * part + 1, whole.at[0], region.at[part, frames + 1, own_r], t - 1, s), has_low_t, has_high_t),
            (halo(4 * part + 2, whole.at[:, rows - 1], region.at[part, own_f, 0], t, s + 1), has_high_s, has_low_s),
            (halo(4 * part + 3, whole.at[:, 0], region.at[part, own_f, rows + 1], t, s - 1), has_low_s, has_high_s),
        ]
    corners = []
    for i, (frame, has_frame) in enumerate(((0, has_low_t), (frames + 1, has_high_t))):
        corners.append((
            halo(8 + 2 * i, region.at[:, frame, rows], region.at[:, frame, 0], t, s + 1),
            has_frame & has_high_s, has_frame & has_low_s,
        ))
        corners.append((
            halo(9 + 2 * i, region.at[:, frame, 1], region.at[:, frame, rows + 1], t, s - 1),
            has_frame & has_low_s, has_frame & has_high_s,
        ))
    parts, lane = weights.shape[0], weights.shape[2]

    def block(b, p):
        return weights.at[p, pl.ds(pl.multiple_of(b * depth, depth), depth)]

    def own_block(p):
        return weight_ref.at[:, pl.ds(pl.multiple_of(p * lane, lane), lane)]

    partner = s + 1 - 2 * lax.rem(s, 2)

    def near(k, b, way, p, first):
        space = s + 2 if way == 0 else s - 2
        source = own_block(p) if first else block(b, p)
        return remote(source, block(b, p), near_send.at[way, k, p], weight_recv.at[b, p], t, space)

    def pair(k, b, way, p, first):
        source = own_block(p) if first else block(b, p)
        return remote(source, block(b, p), pair_send.at[way, k, p], weight_recv.at[b, p], t, partner)

    def arrived(b, p):
        remote(block(b, p), block(b, p), pair_send.at[0, 0, p], weight_recv.at[b, p], t, partner).wait_recv()

    def each_part(low, high, run):
        def body(p, carry):
            run(p)
            return carry

        lax.fori_loop(low, high, body, 0)

    for copy, sends, _ in straight[:4]:
        pl.when(sends)(copy.start)

    def first_part(p):
        pl.when(s + 2 < ns)(near(0, s, 0, p, True).start)
        pl.when(s >= 2)(near(0, s, 1, p, True).start)
        pair(0, s, 0, p, True).start()
        pltpu.make_async_copy(own_block(p), block(s, p), own_sem.at[p]).start()

    each_part(0, parts, first_part)
    own_value = pltpu.make_async_copy(value_ref, region.at[1, own_f, own_r], local_sem.at[0])
    own_value.start()
    own_hidden = pltpu.make_async_copy(hidden_in_ref, hidden_ref, local_sem.at[1])
    own_hidden.start()

    step = 16 if columns % 16 == 0 else columns
    for frame in range(frames):
        for row in range(rows):
            for column in range(0, columns, step):
                at = slice(column, column + step)
                region[0, 1 + frame, 1 + row, at] = normalized(key_ref[frame, row, at], key_gain_ref[...])

    def query_rows(i, carry):
        at = pl.ds(pl.multiple_of(i * 16, 16), 16)
        query_ref[at] = normalized(raw_query_ref[at], query_gain_ref[...])
        return carry

    lax.fori_loop(0, tokens // 16, query_rows, 0)
    for copy, sends, _ in straight[4:]:
        pl.when(sends)(copy.start)

    def clear_frame(frame):
        def run():
            for part in range(2):
                for row in range(rows + 2):
                    region[part, frame, row] = jnp.zeros((columns, inner), jnp.bfloat16)
        return run

    def clear_row(row):
        def run():
            for part in range(2):
                for frame in range(frames + 2):
                    region[part, frame, row] = jnp.zeros((columns, inner), jnp.bfloat16)
        return run

    pl.when(jnp.logical_not(has_low_t))(clear_frame(0))
    pl.when(jnp.logical_not(has_high_t))(clear_frame(frames + 1))
    pl.when(jnp.logical_not(has_low_s))(clear_row(0))
    pl.when(jnp.logical_not(has_high_s))(clear_row(rows + 1))

    frame_k, row_k, tile_k = key_place_ref[0:1], key_place_ref[1:2], key_place_ref[2:3]
    inside = (frame_k >= -t * frames) & (frame_k < (nt - t) * frames)
    inside = inside & (row_k >= -s * rows) & (row_k < (ns - s) * rows)
    outside = jnp.where(inside, 0, 9)
    frame_gap = jnp.abs(query_place_ref[:, 0:1] - frame_k) + outside
    row_gap = jnp.abs(query_place_ref[:, 1:2] - row_k)
    tile_gap = jnp.abs(query_place_ref[:, 2:3] - tile_k)
    for i, (reach_t, reach_r, reach_c) in enumerate(REACHES):
        allowed = (frame_gap <= reach_t) & (row_gap <= reach_r) & (tile_gap <= reach_c)
        mask_ref[i] = jnp.where(allowed, 0.0, -1e30)

    def relay(k, p):
        low, high = s - 2 * k, s + 2 * k

        @pl.when(low >= 0)
        def _():
            arrived(low, p)
            pl.when(s + 2 < ns)(near(k, low, 0, p, False).start)
            pair(k, low, 0, p, False).start()

        @pl.when(high < ns)
        def _():
            arrived(high, p)
            pl.when(s >= 2)(near(k, high, 1, p, False).start)
            pair(k, high, 1, p, False).start()

    def relay_parts(k, low, high):
        if 1 <= k < chips:
            each_part(low, high, functools.partial(relay, k))

    early = parts // 2
    last = chips - 1
    if last > 1:
        relay_parts(1, 0, early)
    for copy, _, receives in straight[0:2] + straight[4:6]:
        pl.when(receives)(copy.wait_recv)
    for copy, sends, _ in corners:
        pl.when(sends)(copy.start)
    for copy, _, receives in straight[2:4] + straight[6:8]:
        pl.when(receives)(copy.wait_recv)
    for copy, _, receives in corners:
        pl.when(receives)(copy.wait_recv)
    if last > 1:
        relay_parts(1, early, parts)
    own_value.wait()

    groups = heads // group
    span = group * width

    def gather(g, d):
        at = (t, slice(None), pl.ds(pl.multiple_of(g * span, span), span))
        return remote(
            mixed.at[at], mixed.at[at], mixed_send.at[d - 1, g], mixed_recv.at[t, g],
            lax.rem(t + d, nt), s,
        )

    def one_group(g, carry):
        for i in range(group):
            h = g * group + i
            lanes = pl.ds(pl.multiple_of(h * width, width), width)
            query = query_ref[:, lanes]
            key = region[0, :, :, :, lanes].reshape(keys_here, width)
            value = region[1, :, :, :, lanes].reshape(keys_here, width)
            scores = lax.dot_general(
                query, key, (((1,), (1,)), ((), ())), preferred_element_type=jnp.float32
            ) * width ** (-0.5)
            scores = scores + mask_ref[time_ref[h] * 6 + rows_ref[h] * 3 + cols_ref[h]]
            part = jnp.exp(scores - jnp.max(scores, axis=1, keepdims=True))
            sums = jnp.sum(part, axis=1, keepdims=True)
            result = jnp.dot(part.astype(jnp.bfloat16), value, preferred_element_type=jnp.float32)
            mixed[t, :, lanes] = (result / sums).astype(jnp.bfloat16)
        for d in range(1, nt):
            gather(g, d).start()
        return carry

    ahead = groups * 5 // 8
    lax.fori_loop(0, ahead, one_group, 0)
    if last > 2:
        relay_parts(2, 0, parts)
    lax.fori_loop(ahead, groups, one_group, 0)
    for k in range(3, last):
        relay_parts(k, 0, parts)

    def gathered(g, carry):
        for d in range(1, nt):
            other = lax.rem(t + d, nt)
            at = (other, slice(None), pl.ds(pl.multiple_of(g * span, span), span))
            remote(mixed.at[at], mixed.at[at], mixed_send.at[d - 1, g], mixed_recv.at[other, g], t, s).wait_recv()
        return carry

    chip_depth = 2 * depth
    piece = chip_depth * 128 // math.gcd(chip_depth, 128)

    def multiply(start, p, first):
        feature = pl.ds(pl.multiple_of(start, piece), piece)
        left = mixed[:, :, feature].reshape(nt * tokens, piece)
        product = jnp.dot(left, weights[p, feature], preferred_element_type=jnp.float32)
        if first:
            total[p] = product
        else:
            total[p] += product

    chip = s // 2
    half = lax.rem(s, 2)

    def add(k, p):
        for other in (chip - k, chip + k):
            @pl.when((other >= 0) & (other < chips))
            def _():
                arrived(2 * other + 1 - half, p)
                multiply(other * piece, p, False)

    def own_rows(owner):
        return pl.ds(pl.multiple_of(owner * tokens, tokens), tokens)

    def back(d, p):
        other = lax.rem(t + d, nt)
        return remote(
            outgoing.at[d - 1, p], incoming.at[d - 1, p], back_send.at[d - 1, p], back_recv.at[d - 1, p], other, s
        )

    def send_back(p):
        for d in range(1, nt):
            outgoing[d - 1, p] = total[p, own_rows(lax.rem(t + d, nt)), :].astype(jnp.bfloat16)
            back(d, p).start()

    def own_part(p):
        pltpu.make_async_copy(own_block(p), block(s, p), own_sem.at[p]).wait()
        arrived(partner, p)

    lax.fori_loop(0, groups, gathered, 0)
    if piece == chip_depth:
        def begin(p):
            own_part(p)
            multiply(chip * piece, p, True)
            for k in range(1, last):
                add(k, p)

        each_part(0, parts, begin)

        def conclude(p):
            if last > 0:
                relay(last, p)
                add(last, p)
            send_back(p)

        each_part(0, parts, conclude)
    else:
        def conclude(p):
            own_part(p)
            if last > 0:
                relay(last, p)
            for k in range(1, chips):
                for other in (chip - k, chip + k):
                    @pl.when((other >= 0) & (other < chips))
                    def _():
                        arrived(2 * other + 1 - half, p)
            multiply(0, p, True)

            def add_piece(i, carry):
                multiply(i * piece, p, False)
                return carry

            lax.fori_loop(1, inner // piece, add_piece, 0)
            send_back(p)

        each_part(0, parts, conclude)

    own_hidden.wait()

    def finish(owner, p, branch):
        lanes = pl.ds(pl.multiple_of(owner * cols + p * lane, lane), lane)
        out_ref[:, lanes] = (
            hidden_ref[:, lanes].astype(jnp.float32) + gate_ref[:, lanes] * branch
        ).astype(jnp.bfloat16)

    def finish_own(p):
        finish(t, p, total[p, own_rows(t), :])

    def finish_others(p):
        for d in range(1, nt):
            back(d, p).wait_recv()
            finish(lax.rem(t + nt - d, nt), p, incoming[d - 1, p].astype(jnp.float32))

    each_part(0, parts, finish_own)
    each_part(0, parts, finish_others)

    for copy, sends, _ in straight + corners:
        pl.when(sends)(copy.wait_send)
    for k in range(chips):
        low, high = s - 2 * k, s + 2 * k

        def weight_sent(p):
            pl.when((low >= 0) & (s + 2 < ns))(near(k, low, 0, p, k == 0).wait_send)
            pl.when((high < ns) & (s >= 2))(near(k, high, 1, p, k == 0).wait_send)
            pl.when(low >= 0)(pair(k, low, 0, p, k == 0).wait_send)
            if k > 0:
                pl.when(high < ns)(pair(k, high, 1, p, False).wait_send)

        each_part(0, parts, weight_sent)

    def sent(g, carry):
        for d in range(1, nt):
            gather(g, d).wait_send()
        return carry

    lax.fori_loop(0, groups, sent, 0)

    def back_sent(p):
        for d in range(1, nt):
            back(d, p).wait_send()

    each_part(0, parts, back_sent)


def ring_shards(
    hidden_in,
    queries,
    keys,
    values,
    query_gain,
    key_gain,
    reach_time,
    reach_rows,
    reach_cols,
    out_weight,
    gate,
):
    frames, rows, columns, inner = queries.shape
    width = hidden_in.shape[3]
    heads = reach_time.shape[0]
    tokens = frames * rows * columns
    nt, ns = lax.axis_size("tm"), lax.axis_size("space")
    depth, cols = out_weight.shape
    group = 5 if heads % 5 == 0 else 1
    vmem = pl.BlockSpec(memory_space=pltpu.VMEM)
    hbm = pl.BlockSpec(memory_space=pl.ANY)
    dma = pltpu.SemaphoreType.DMA
    lane = 256 if cols % 256 == 0 else 128
    parts = cols // lane
    output = pl.pallas_call(
        functools.partial(ring_kernel, heads, group),
        out_shape=jax.ShapeDtypeStruct((tokens, width), jnp.bfloat16),
        in_specs=[pl.BlockSpec(memory_space=pltpu.SMEM)] * 3 + [vmem] * 7 + [hbm] * 3,
        out_specs=vmem,
        scratch_shapes=[
            pltpu.VMEM((tokens, inner), jnp.bfloat16),
            pltpu.VMEM((len(REACHES), tokens, (frames + 2) * (rows + 2) * columns), jnp.float32),
            pltpu.VMEM((tokens, width), jnp.bfloat16),
            pltpu.VMEM((2, frames + 2, rows + 2, columns, inner), jnp.bfloat16),
            pltpu.VMEM((parts, depth * ns, lane), jnp.bfloat16),
            pltpu.VMEM((nt, tokens, inner), jnp.bfloat16),
            pltpu.VMEM((parts, nt * tokens, lane), jnp.float32),
            pltpu.VMEM((nt - 1, parts, tokens, lane), jnp.bfloat16),
            pltpu.VMEM((nt - 1, parts, tokens, lane), jnp.bfloat16),
            dma((2,)),
            dma((parts,)),
            dma((12,)),
            dma((12,)),
            dma((2, ns // 2, parts)),
            dma((2, ns // 2, parts)),
            dma((ns, parts)),
            dma((nt - 1, heads // group)),
            dma((nt, heads // group)),
            dma((nt - 1, parts)),
            dma((nt - 1, parts)),
        ],
        compiler_params=pltpu.CompilerParams(
            has_side_effects=True, vmem_limit_bytes=60 * 1024 * 1024
        ),
    )(
        reach_time,
        reach_rows,
        reach_cols,
        queries.reshape(tokens, inner),
        keys,
        query_gain.reshape(1, inner),
        key_gain.reshape(1, inner),
        places(frames, rows, columns, 0).T,
        places(frames, rows, columns, 1),
        gate.reshape(1, width),
        values,
        out_weight,
        hidden_in.reshape(tokens, width),
    )
    return output.reshape(frames, rows, columns, width)


def pair_kernel(
    heads,
    time_ref,
    rows_ref,
    cols_ref,
    query_gain_ref,
    key_gain_ref,
    query_place_ref,
    key_place_ref,
    gate_ref,
    raw_query_ref,
    raw_key_ref,
    value_ref,
    weight_ref,
    hidden_in_ref,
    out_ref,
    raw,
    normed,
    region,
    query_ref,
    mask_ref,
    mixed,
    weights,
    total,
    partial_out,
    partial_in,
    outgoing,
    incoming,
    hidden_ref,
    result_ref,
    staged,
    local_sem,
    value_sem,
    own_sem,
    swap_send,
    swap_recv,
    side_send,
    side_recv,
    corner_send,
    corner_recv,
    stage_recv,
    near_send,
    cross_send,
    pair_send,
    weight_recv,
    level_send,
    level_recv,
    mixed_send,
    mixed_recv,
    part_send,
    part_recv,
    back_send,
    back_recv,
    out_sem,
):
    t = lax.axis_index("tm")
    s = lax.axis_index("space")
    nt = lax.axis_size("tm")
    ns = lax.axis_size("space")
    frames, rows, columns, inner = value_ref.shape
    tokens = frames * rows * columns
    depth, cols = weight_ref.shape
    width = inner // heads
    groups = ns // 2
    half = inner // 2
    blocks, parts, _, lane = weights.shape
    chips = ns // 4
    row_tokens = rows * columns
    span = 2 * frames

    p = lax.rem(t, 2)
    column_block = lax.div(t, 2)
    c = lax.rem(s, 2)
    z = lax.div(s, 2)
    level = lax.rem(z, 2)
    chip = lax.div(z, 2)
    mate = t + 1 - 2 * p
    partner = s + 1 - 2 * c
    level_mate = s + 2 - 4 * level

    has_low_t, has_high_t = t >= 2, t < nt - 2
    has_low_s, has_high_s = s > 0, s < ns - 1

    def remote(source, target, send, recv, tm, space):
        return pltpu.make_async_remote_copy(
            src_ref=source,
            dst_ref=target,
            send_sem=send,
            recv_sem=recv,
            device_id=(tm, space),
            device_id_type=pl.DeviceIdType.MESH,
        )

    def lanes_at(start, size):
        return pl.ds(pl.multiple_of(start, 128), size)

    def other_column(e):
        return lax.rem(column_block + e, blocks)

    def other_chip(d):
        return lax.rem(chip + d, chips)

    def column_device(e):
        return 2 * other_column(e) + p

    def chip_device(d):
        return 4 * other_chip(d) + 2 * level + c

    levels = 2 * chips
    middle = levels // 2

    def comes_late(d):
        rises = other_chip(d) < chip
        return (rises & (z <= middle)) | (jnp.logical_not(rises) & (z + 1 >= middle))

    starts = {True: z + 2 < levels, False: z >= 2}
    passes = {True: (z >= 1) & (z + 1 < levels), False: (z + 1 < levels) & (z >= 1)}
    inner = {True: z < middle, False: z >= middle}

    load_key = pltpu.make_async_copy(raw_key_ref, raw.at[0], local_sem.at[0])
    load_key.start()
    load_query = pltpu.make_async_copy(raw_query_ref, raw.at[1], local_sem.at[1])
    load_query.start()

    barrier = pltpu.get_barrier_semaphore()

    def greet(tm, space):
        pl.semaphore_signal(
            barrier, inc=1, device_id=(tm, space), device_id_type=pl.DeviceIdType.MESH
        )

    greet(mate, s)
    greet(t, partner)
    greet(t, level_mate)
    for e in range(1, blocks):
        greet(column_device(e), s)
    across = s - 2 + 4 * level
    has_across = (across >= 0) & (across < ns)
    pl.when(has_across)(functools.partial(greet, t, across))
    up, down = (c == 1) & has_high_s, (c == 0) & has_low_s

    @pl.when(up)
    def _():
        greet(t, s + 1)

    @pl.when(down)
    def _():
        greet(t, s - 1)

    pl.semaphore_wait(
        barrier, blocks + 2 + has_across.astype(jnp.int32) + (up | down).astype(jnp.int32)
    )

    own_frames = pl.ds(1 + frames * p, frames)
    own_rows = pl.ds(1, rows)

    def group_lanes(b):
        return pl.ds(b * depth, depth)

    def value_swap(b):
        source = value_ref.at[:, :, :, lanes_at((2 * b + 1 - p) * depth, depth)]
        target = region.at[1, own_frames, own_rows, :, group_lanes(b)]
        return remote(source, target, swap_send.at[1, b], swap_recv.at[1, b], mate, s)

    def key_swap(b):
        source = normed.at[0, 1 - p, :, :, :, group_lanes(b)]
        target = region.at[0, own_frames, own_rows, :, group_lanes(b)]
        return remote(source, target, swap_send.at[0, b], swap_recv.at[0, b], mate, s)

    def query_swap(b):
        source = normed.at[1, 1 - p, :, :, :, group_lanes(b)]
        target = query_ref.at[pl.ds(frames * p, frames), :, :, group_lanes(b)]
        return remote(source, target, swap_send.at[2, b], swap_recv.at[2, b], mate, s)

    def own_value(b):
        return pltpu.make_async_copy(
            value_ref.at[:, :, :, lanes_at((2 * b + p) * depth, depth)],
            region.at[1, own_frames, own_rows, :, group_lanes(b)],
            value_sem.at[b],
        )

    def own_weight(q):
        return weight_ref.at[:, pl.ds(q * lane, lane)]

    def own_weight_at(q):
        return weight_ref.at[:, lanes_at(q * lane, lane)]

    def weight_block(block, chip_index, core, q):
        start = (2 * chip_index + core) * depth
        return weights.at[block, q, pl.ds(pl.multiple_of(start, depth), depth)]

    def arrival(chip_index, core):
        return 2 * chip_index + core

    def keep_weight(q):
        return pltpu.make_async_copy(
            own_weight_at(q), weight_block(column_block, chip, c, q), own_sem.at[q]
        )

    def shares(q, d=1):
        return range(2 if d > 0 and q == parts - 1 else 1)

    def rows_of(q, k, d=1):
        count = len(shares(q, d))
        return pl.ds(k * (depth // count), depth // count)

    def first_hop(rising, q, k):
        at = rows_of(q, k)
        return remote(
            own_weight_at(q).at[at], staged.at[int(rising), q, at],
            near_send.at[0, int(rising), q + k], stage_recv.at[int(rising), q + k],
            t, s + 2 if rising else s - 2,
        )

    def second_hop(rising, q, k):
        origin = lax.div(z + levels - 1 if rising else z + levels + 1, 2) - chips
        at = rows_of(q, k)
        return remote(
            staged.at[int(rising), q, at], weight_block(column_block, origin, c, q).at[at],
            near_send.at[1, int(rising), q + k],
            weight_recv.at[column_block, arrival(origin, c), q + k],
            t, s + 2 if rising else s - 2,
        )

    def cross_weight(e, d, q, k):
        at = rows_of(q, k, d)
        block = weight_block(column_block, other_chip(d), c, q).at[at]
        source = own_weight_at(q).at[at] if d == 0 else block
        return remote(
            source, block, cross_send.at[e - 1, d, q + k],
            weight_recv.at[column_block, arrival(other_chip(d), c), q + k],
            column_device(e), s,
        )

    def pair_weight(e, d, q, k):
        at = rows_of(q, k, d)
        block = weight_block(other_column(e), other_chip(d), c, q).at[at]
        source = own_weight_at(q).at[at] if e == 0 and d == 0 else block
        return remote(
            source, block, pair_send.at[e, d, q + k],
            weight_recv.at[other_column(e), arrival(other_chip(d), c), q + k],
            t, partner,
        )

    def weight_here(e, d, core, q, k):
        block = weight_block(other_column(e), other_chip(d), core, q).at[rows_of(q, k, d)]
        remote(
            block, block, pair_send.at[e, d, q + k],
            weight_recv.at[other_column(e), arrival(other_chip(d), core), q + k], t, partner,
        ).wait_recv()

    at_end = (z == 0) | (z == levels - 1)

    def send_far(q, ends, which=True):
        for rising in (True, False):
            for k in shares(q):
                pl.when(starts[rising] & (at_end == ends) & which)(first_hop(rising, q, k).start)

    def forward(q, inward, which=True):
        for rising in (True, False):
            @pl.when(passes[rising] & (inner[rising] == inward) & which)
            def _(rising=rising):
                for k in shares(q):
                    first_hop(rising, q, k).wait_recv()
                    second_hop(rising, q, k).start()

    def send_cross(q):
        for e in range(1, blocks):
            cross_weight(e, 0, q, 0).start()
        pair_weight(0, 0, q, 0).start()

    def relay_far(q, late):
        for d in range(1, chips):
            @pl.when(comes_late(d) if late else jnp.logical_not(comes_late(d)))
            def _(d=d):
                for k in shares(q):
                    weight_here(0, d, c, q, k)
                    for e in range(1, blocks):
                        cross_weight(e, d, q, k).start()
                    pair_weight(0, d, q, k).start()

    def relay_cross(q, far):
        for e in range(1, blocks):
            for d in range(1, chips) if far else (0,):
                for k in shares(q, d):
                    weight_here(e, d, c, q, k)
                    pair_weight(e, d, q, k).start()

    value_swap(0).start()
    for b in range(groups):
        own_value(b).start()
    send_far(0, True)
    send_far(0, False)
    send_cross(0)
    for q in range(parts):
        keep_weight(q).start()
    own_hidden = pltpu.make_async_copy(hidden_in_ref, hidden_ref, local_sem.at[2])
    own_hidden.start()

    step = 16 if columns % 16 == 0 else columns

    def normalize(index, gain_ref):
        for frame in range(frames):
            for row in range(rows):
                for column in range(0, columns, step):
                    at = slice(column, column + step)
                    result = normalized(raw[index, frame, row, at], gain_ref[...])
                    for b in range(groups):
                        for core in range(2):
                            start = (2 * b + core) * depth
                            normed[index, core, frame, row, at, b * depth:(b + 1) * depth] = (
                                result[:, start:start + depth]
                            )

    load_key.wait()
    with jax.named_scope("normalize_key"):
        normalize(0, key_gain_ref)
    key_swap(0).start()
    own_key = pltpu.make_async_copy(
        normed.at[0, p], region.at[0, own_frames, own_rows], local_sem.at[3]
    )
    own_key.start()
    load_query.wait()
    with jax.named_scope("normalize_query"):
        normalize(1, query_gain_ref)
    query_swap(0).start()
    own_query = pltpu.make_async_copy(
        normed.at[1, p], query_ref.at[pl.ds(frames * p, frames)], local_sem.at[4]
    )
    own_query.start()
    for b in range(1, groups):
        value_swap(b).start()
        key_swap(b).start()
        query_swap(b).start()

    def clear_frame(frame):
        def run():
            for part in range(2):
                for row in range(rows + 2):
                    region[part, frame, row] = jnp.zeros((columns, half), jnp.bfloat16)
        return run

    def clear_row(row):
        def run():
            for part in range(2):
                for frame in range(span + 2):
                    region[part, frame, row] = jnp.zeros((columns, half), jnp.bfloat16)
        return run

    pl.when(jnp.logical_not(has_low_t))(clear_frame(0))
    pl.when(jnp.logical_not(has_high_t))(clear_frame(span + 1))
    pl.when(jnp.logical_not(has_low_s))(clear_row(0))
    pl.when(jnp.logical_not(has_high_s))(clear_row(rows + 1))

    frame_k, row_k, tile_k = key_place_ref[0:1], key_place_ref[1:2], key_place_ref[2:3]
    inside = (row_k >= -s * rows) & (row_k < (ns - s) * rows)
    row_gap = jnp.abs(query_place_ref[:, 0:1] - row_k) + jnp.where(inside, 0, 9)
    tile_gap = jnp.abs(query_place_ref[:, 1:2] - tile_k)
    low_gap = jnp.where(has_low_t, 0, 9) * (frame_k < 0).astype(jnp.int32)
    high_gap = jnp.where(has_high_t, 0, 9) * (frame_k > 0).astype(jnp.int32)
    for kind, edge in enumerate((jnp.zeros_like(low_gap), low_gap, high_gap)):
        frame_gap = jnp.abs(frame_k) + edge
        for i, (reach_t, reach_r, reach_c) in enumerate(REACHES):
            allowed = (frame_gap <= reach_t) & (row_gap <= reach_r) & (tile_gap <= reach_c)
            mask_ref[kind, i] = jnp.where(allowed, 0.0, -1e30)

    pair_frames = pl.ds(1, span)

    def row_up(b):
        return remote(
            region.at[:, pair_frames, rows, :, group_lanes(b)],
            region.at[:, pair_frames, 0, :, group_lanes(b)],
            side_send.at[0, b], side_recv.at[0, b], t, s + 1,
        )

    def row_down(b):
        return remote(
            region.at[:, pair_frames, 1, :, group_lanes(b)],
            region.at[:, pair_frames, rows + 1, :, group_lanes(b)],
            side_send.at[1, b], side_recv.at[1, b], t, s - 1,
        )

    def frame_up(b):
        return remote(
            region.at[:, span, own_rows, :, group_lanes(b)],
            region.at[:, 0, own_rows, :, group_lanes(b)],
            side_send.at[2, b], side_recv.at[2, b], t + 2, s,
        )

    def frame_down(b):
        return remote(
            region.at[:, 1, own_rows, :, group_lanes(b)],
            region.at[:, span + 1, own_rows, :, group_lanes(b)],
            side_send.at[3, b], side_recv.at[3, b], t - 2, s,
        )

    def sides(b):
        return (
            (frame_up(b), has_high_t, has_low_t),
            (frame_down(b), has_low_t, has_high_t),
            (row_up(b), has_high_s, has_low_s),
            (row_down(b), has_low_s, has_high_s),
        )

    def corners(b):
        result = []
        for i, (frame, has_frame) in enumerate(((0, has_low_t), (span + 1, has_high_t))):
            for j, (row, landing, space, sends, receives) in enumerate((
                (rows, 0, s + 1, has_high_s, has_low_s),
                (1, rows + 1, s - 1, has_low_s, has_high_s),
            )):
                copy = remote(
                    region.at[:, frame, row, :, group_lanes(b)],
                    region.at[:, frame, landing, :, group_lanes(b)],
                    corner_send.at[2 * i + j, b], corner_recv.at[2 * i + j, b], t, space,
                )
                result.append((copy, has_frame & sends, has_frame & receives))
        return result

    def feature_lanes(index, core):
        return lanes_at((2 * index + core) * depth, depth)

    def to_level_mate(j):
        at = (slice(None), feature_lanes(j, p))
        return remote(
            mixed.at[(2,) + at], mixed.at[(level,) + at],
            level_send.at[j], level_recv.at[j], t, level_mate,
        )

    def from_level_mate(j):
        at = (1 - level, slice(None), feature_lanes(j, p))
        return remote(mixed.at[at], mixed.at[at], level_send.at[j], level_recv.at[j], t, level_mate)

    def to_mate(which, j):
        at = (which, slice(None), feature_lanes(j, p))
        return remote(
            mixed.at[at], mixed.at[at], mixed_send.at[which, j], mixed_recv.at[which, j], mate, s
        )

    def from_mate(which, j):
        at = (which, slice(None), feature_lanes(j, 1 - p))
        remote(
            mixed.at[at], mixed.at[at], mixed_send.at[which, j], mixed_recv.at[which, j], mate, s
        ).wait_recv()

    def attend(b):
        in_level = level == b % 2
        place = jnp.where(in_level, level, 2)
        index = b // 2
        group = depth // width

        def one_head(i, carry):
            h = (2 * b + p) * group + i
            lanes = lanes_at(b * depth + i * width, width)
            reach = time_ref[h] * 6 + rows_ref[h] * 3 + cols_ref[h]
            target = lanes_at((2 * index + p) * depth + i * width, width)
            scores, values = [], []
            for frame in range(span):
                query = query_ref[frame, :, :, lanes].reshape(row_tokens, width)
                near = slice(frame, frame + 3)
                key = region[0, near, :, :, lanes].reshape(-1, width)
                values.append(region[1, near, :, :, lanes].reshape(-1, width))
                scores.append(lax.dot_general(
                    query, key, (((1,), (1,)), ((), ())), preferred_element_type=jnp.float32
                ))
            results = []
            for frame in range(span):
                kind = 1 if frame == 0 else 2 if frame == span - 1 else 0
                masked = scores[frame] * width ** (-0.5) + mask_ref[kind, reach]
                part = jnp.exp(masked - jnp.max(masked, axis=1, keepdims=True))
                sums = jnp.sum(part, axis=1, keepdims=True)
                result = jnp.dot(
                    part.astype(jnp.bfloat16), values[frame], preferred_element_type=jnp.float32
                )
                results.append((result / sums).astype(jnp.bfloat16))
            mixed[place, :, target] = jnp.concatenate(results, axis=0)
            return carry

        lax.fori_loop(0, group, one_head, 0)

    def send_mixed(b):
        pl.when(level != b % 2)(to_level_mate(b // 2).start)

    def relay_mixed(b):
        @pl.when(level == b % 2)
        def _():
            from_level_mate(b // 2).wait_recv()
            to_mate(1 - level, b // 2).start()
            to_mate(level, b // 2).start()

    def arrive(i):
        with jax.named_scope(f"wait_swap{i}"):
            value_swap(i).wait_recv()
            key_swap(i).wait_recv()
            own_value(i).wait()
            if i == 0:
                own_key.wait()
        with jax.named_scope(f"send_sides{i}"):
            for copy, sends, _ in sides(i):
                pl.when(sends)(copy.start)

    def turn(i):
        with jax.named_scope(f"wait_frames{i}"):
            for copy, _, receives in sides(i)[:2]:
                pl.when(receives)(copy.wait_recv)
        for copy, sends, _ in corners(i):
            pl.when(sends)(copy.start)

    def ready(b):
        with jax.named_scope(f"wait_query{b}"):
            query_swap(b).wait_recv()
            if b == 0:
                own_query.wait()
        with jax.named_scope(f"wait_rows{b}"):
            for copy, _, receives in sides(b)[2:]:
                pl.when(receives)(copy.wait_recv)
        with jax.named_scope(f"wait_corners{b}"):
            for copy, _, receives in corners(b):
                pl.when(receives)(copy.wait_recv)

    early = min(2, parts)
    actions = {
        "end": lambda q: send_far(q, True),
        "end0": lambda q: send_far(q, True, level == 0),
        "end1": lambda q: send_far(q, True, level == 1),
        "out0": lambda q: forward(q, False, level == 0),
        "out1": lambda q: forward(q, False, level == 1),
        "mid": lambda q: send_far(q, False),
        "late": lambda q: relay_far(q, True),
        "cross": send_cross,
        "out": lambda q: forward(q, False),
        "in": lambda q: forward(q, True),
        "early": lambda q: relay_far(q, False),
    }
    plan = {i: [] for i in range(groups + 1)}
    plan[0] += [("mid", 1), ("end", 1), ("cross", 1), ("out", 0)]
    plan[1] += [("mid", 2), ("end0", 2), ("cross", 2), ("out0", 1)]
    plan[2] += [("mid", 3), ("end1", 2), ("cross", 3), ("out1", 1)]
    plan[3] += [("in", 0), ("end0", 3), ("out0", 2), ("cross", 4), ("early", 0), ("early", 1)]
    plan[groups] += [("mid", 4), ("in", 1), ("end1", 3), ("end", 4), ("out1", 2), ("out", 3), ("late", 0)]
    plan[groups] += [("cross", q) for q in range(5, parts)]
    for i in range(groups + 1):
        if i < groups:
            arrive(i)
        if i > 0:
            ready(i - 1)
            with jax.named_scope(f"attend{i - 1}"):
                attend(i - 1)
        if i < groups:
            turn(i)
        if i > 0:
            send_mixed(i - 1)
        for kind, q in plan[i]:
            if q < parts:
                actions[kind](q)
        if i > 1:
            with jax.named_scope(f"relay_mixed{i}"):
                relay_mixed(i - 2)
        if i > 1 and i - 2 < parts:
            with jax.named_scope(f"relay_cross{i}"):
                relay_cross(i - 2, False)
    with jax.named_scope("relay_mixed_last"):
        relay_mixed(groups - 1)

    def each_part(low, high, run):
        def body(q, carry):
            run(q)
            return carry

        lax.fori_loop(low, high, body, 0)

    def next_far(q):
        if q < parts:
            with jax.named_scope(f"relay_far{q}"):
                relay_far(q, True)

    def multiply_theirs(e, q):
        block = other_column(e)
        for d in range(chips):
            for k in shares(q, d):
                weight_here(e, d, 1 - c, q, k)
        product = jnp.dot(
            mixed[1 - level], weights[block, q], preferred_element_type=jnp.float32
        )
        partial_out[block, q] = product.astype(jnp.bfloat16)
        part_copy(block, q).start()

    def multiply_ours(e, q):
        block = other_column(e)
        total[block, q] = jnp.dot(
            mixed[level], weights[block, q], preferred_element_type=jnp.float32
        )

    def part_copy(block, q):
        return remote(
            partial_out.at[block, q], partial_in.at[block, q],
            part_send.at[block, q], part_recv.at[block, q], t, level_mate,
        )

    def back(block, q):
        return remote(
            outgoing.at[block, q], incoming.at[block, q],
            back_send.at[block, q], back_recv.at[block, q], mate, s,
        )

    def token_rows(side):
        return pl.ds(pl.multiple_of(side * tokens, tokens), tokens)

    def finish(column, branch, index, q):
        lanes = lanes_at(column, lane)
        result_ref[:, lanes] = (
            hidden_ref[:, lanes].astype(jnp.float32) + gate_ref[:, lanes] * branch
        ).astype(jnp.bfloat16)
        write_out(column, index, q).start()

    def write_out(column, index, q):
        lanes = lanes_at(column, lane)
        return pltpu.make_async_copy(
            result_ref.at[:, lanes], out_ref.at[:, lanes], out_sem.at[index, q]
        )

    def reduce_part(q):
        for e in range(blocks):
            block = other_column(e)
            part_copy(block, q).wait_recv()
            theirs = token_rows(1 - p)
            outgoing[block, q] = (
                total[block, q, theirs] + partial_in[block, q, theirs].astype(jnp.float32)
            ).astype(jnp.bfloat16)
            back(block, q).start()
            ours = token_rows(p)
            branch = total[block, q, ours] + partial_in[block, q, ours].astype(jnp.float32)
            finish((2 * block + p) * cols + q * lane, branch, 2 * block + p, q)

    def theirs(q):
        if q >= groups - 1:
            relay_cross(q, False)
        keep_weight(q).wait()
        with jax.named_scope(f"theirs{q}own"):
            multiply_theirs(0, q)
        if blocks > 1:
            with jax.named_scope(f"main_cross{q}"):
                relay_cross(q, True)
            with jax.named_scope(f"theirs{q}other"):
                for e in range(1, blocks):
                    multiply_theirs(e, q)

    def ours(q):
        with jax.named_scope(f"ours{q}"):
            for e in range(blocks):
                multiply_ours(e, q)

    forward(2, True)
    relay_far(2, False)
    forward(4, False)
    forward(3, True)
    relay_far(3, False)
    next_far(1)
    with jax.named_scope("from_mate_theirs"):
        for j in range(groups // 2):
            from_mate(1 - level, j)
    theirs(0)
    forward(4, True)
    next_far(2)
    theirs(1)
    relay_far(4, False)
    with jax.named_scope("from_mate_ours"):
        for j in range(groups // 2):
            from_mate(level, j)
    ours(0)
    own_hidden.wait()
    next_far(3)
    theirs(2)
    next_far(4)
    ours(1)
    with jax.named_scope("reduce01"):
        reduce_part(0)
        reduce_part(1)
    theirs(3)
    ours(2)
    ours(3)
    with jax.named_scope("reduce2"):
        reduce_part(2)
    with jax.named_scope("reduce3a"):
        pl.when(jnp.logical_not(at_end))(functools.partial(reduce_part, 3))
    theirs(4)
    ours(4)

    def finish_others(q):
        for block in range(blocks):
            back(block, q).wait_recv()
            finish(
                (2 * block + 1 - p) * cols + q * lane,
                incoming[block, q].astype(jnp.float32), 2 * block + 1 - p, q,
            )

    with jax.named_scope("reduce3b"):
        pl.when(at_end)(functools.partial(reduce_part, 3))
    with jax.named_scope("finish01"):
        each_part(0, 2, finish_others)
    with jax.named_scope("reduce4"):
        reduce_part(4)
    with jax.named_scope("finish2"):
        each_part(2, parts, finish_others)

    for b in range(groups):
        value_swap(b).wait_send()
        key_swap(b).wait_send()
        query_swap(b).wait_send()
        for copy, sends, _ in sides(b) + tuple(corners(b)):
            pl.when(sends)(copy.wait_send)
    for j in range(groups // 2):
        to_level_mate(j).wait_send()
        for which in range(2):
            to_mate(which, j).wait_send()

    def weight_sent(q):
        for k in shares(q):
            for rising in (True, False):
                pl.when(starts[rising])(first_hop(rising, q, k).wait_send)
                pl.when(passes[rising])(second_hop(rising, q, k).wait_send)
        for e in range(blocks):
            for d in range(chips):
                for k in shares(q, d):
                    pair_weight(e, d, q, k).wait_send()
                    if e > 0:
                        cross_weight(e, d, q, k).wait_send()

    for q in range(parts):
        weight_sent(q)

    def sent(q):
        for block in range(blocks):
            part_copy(block, q).wait_send()
            back(block, q).wait_send()
        for index in range(nt):
            write_out(index * cols + q * lane, index, q).wait()

    each_part(0, parts, sent)


def pair_shards(
    hidden_in,
    queries,
    keys,
    values,
    query_gain,
    key_gain,
    reach_time,
    reach_rows,
    reach_cols,
    out_weight,
    gate,
):
    frames, rows, columns, inner = queries.shape
    width = hidden_in.shape[3]
    heads = reach_time.shape[0]
    tokens = frames * rows * columns
    nt, ns = lax.axis_size("tm"), lax.axis_size("space")
    depth, cols = out_weight.shape
    lane = 256 if cols % 256 == 0 else 128
    parts = cols // lane
    blocks, chips, groups = nt // 2, ns // 4, ns // 2
    half = inner // 2
    pair_tokens = 2 * tokens
    vmem = pl.BlockSpec(memory_space=pltpu.VMEM)
    hbm = pl.BlockSpec(memory_space=pl.ANY)
    dma = pltpu.SemaphoreType.DMA
    _, query_row, query_tile = places(1, rows, columns, 0)
    key_place = np.stack([axis.reshape(-1) for axis in np.meshgrid(
        np.arange(-1, 2), np.arange(-1, rows + 1), np.arange(columns) // TW, indexing="ij"
    )]).astype(np.int32)
    output = pl.pallas_call(
        functools.partial(pair_kernel, heads),
        out_shape=jax.ShapeDtypeStruct((tokens, width), jnp.bfloat16),
        in_specs=[pl.BlockSpec(memory_space=pltpu.SMEM)] * 3 + [vmem] * 5 + [hbm] * 5,
        out_specs=hbm,
        scratch_shapes=[
            pltpu.VMEM((2, frames, rows, columns, inner), jnp.bfloat16),
            pltpu.VMEM((2, 2, frames, rows, columns, half), jnp.bfloat16),
            pltpu.VMEM((2, 2 * frames + 2, rows + 2, columns, half), jnp.bfloat16),
            pltpu.VMEM((2 * frames, rows, columns, half), jnp.bfloat16),
            pltpu.VMEM((3, len(REACHES), rows * columns, 3 * (rows + 2) * columns), jnp.float32),
            pltpu.VMEM((3, pair_tokens, half), jnp.bfloat16),
            pltpu.VMEM((blocks, parts, half, lane), jnp.bfloat16),
            pltpu.VMEM((blocks, parts, pair_tokens, lane), jnp.float32),
            pltpu.VMEM((blocks, parts, pair_tokens, lane), jnp.bfloat16),
            pltpu.VMEM((blocks, parts, pair_tokens, lane), jnp.bfloat16),
            pltpu.VMEM((blocks, parts, tokens, lane), jnp.bfloat16),
            pltpu.VMEM((blocks, parts, tokens, lane), jnp.bfloat16),
            pltpu.VMEM((tokens, width), jnp.bfloat16),
            pltpu.VMEM((tokens, width), jnp.bfloat16),
            pltpu.VMEM((2, parts, depth, lane), jnp.bfloat16),
            dma((5,)),
            dma((groups,)),
            dma((parts,)),
            dma((3, groups)),
            dma((3, groups)),
            dma((4, groups)),
            dma((4, groups)),
            dma((4, groups)),
            dma((4, groups)),
            dma((2, parts + 1)),
            dma((2, 2, parts + 1)),
            dma((max(blocks - 1, 1), chips, parts + 1)),
            dma((blocks, chips, parts + 1)),
            dma((blocks, 2 * chips, parts + 1)),
            dma((groups // 2,)),
            dma((groups // 2,)),
            dma((2, groups // 2)),
            dma((2, groups // 2)),
            dma((blocks, parts)),
            dma((blocks, parts)),
            dma((blocks, parts)),
            dma((blocks, parts)),
            dma((nt, parts)),
        ],
        compiler_params=pltpu.CompilerParams(
            collective_id=0, has_side_effects=True, vmem_limit_bytes=60 * 1024 * 1024
        ),
    )(
        reach_time,
        reach_rows,
        reach_cols,
        query_gain.reshape(1, inner),
        key_gain.reshape(1, inner),
        np.stack([query_row, query_tile]).T,
        key_place,
        gate.reshape(1, width),
        queries,
        keys,
        values,
        out_weight,
        hidden_in.reshape(tokens, width),
    )
    return output.reshape(frames, rows, columns, width)


def shards(hidden_in, queries, keys, values, *others):
    out_weight, reach_time = others[-2], others[2]
    width = queries.shape[3] // reach_time.shape[0]
    nt, ns = lax.axis_size("tm"), lax.axis_size("space")
    whole_heads = out_weight.shape[0] % width == 0
    form = pair_shards if whole_heads and nt % 2 == 0 and ns // 4 == 2 else ring_shards
    return form(hidden_in, queries, keys, values, *others)


def solution(mesh):
    in_specs = (
        P("tm", "space", None, None),
        P("tm", "space", None, None),
        P("tm", "space", None, None),
        P("tm", "space", None, None),
        P(),
        P(),
        P(),
        P(),
        P(),
        P("space", "tm"),
        P(),
    )
    out_specs = P("tm", "space", None, None)
    return jax.shard_map(shards, mesh=mesh, in_specs=in_specs, out_specs=out_specs, check_vma=False)
```

```python
import functools
import math

import jax
import jax.numpy as jnp
import numpy as np
from jax import lax
from jax.experimental import pallas as pl
from jax.experimental.pallas import tpu as pltpu
from jax.sharding import PartitionSpec as P

TW = 8
REACHES = [(a, b, c) for a in range(2) for b in range(2) for c in range(3)]


def normalized(source, gain):
    values_f = source.astype(jnp.float32)
    mean_square = jnp.mean(values_f * values_f, axis=-1, keepdims=True)
    return (values_f * lax.rsqrt(mean_square + 1e-06) * gain).astype(jnp.bfloat16)


def places(frames, rows, columns, margin):
    grid = np.meshgrid(
        np.arange(-margin, frames + margin),
        np.arange(-margin, rows + margin),
        np.arange(columns) // TW,
        indexing="ij",
    )
    return np.stack([axis.reshape(-1) for axis in grid]).astype(np.int32)


def ring_kernel(
    heads,
    group,
    time_ref,
    rows_ref,
    cols_ref,
    raw_query_ref,
    key_ref,
    query_gain_ref,
    key_gain_ref,
    query_place_ref,
    key_place_ref,
    gate_ref,
    value_ref,
    weight_ref,
    hidden_in_ref,
    out_ref,
    query_ref,
    mask_ref,
    hidden_ref,
    region,
    weights,
    mixed,
    total,
    outgoing,
    incoming,
    local_sem,
    own_sem,
    halo_send,
    halo_recv,
    near_send,
    pair_send,
    weight_recv,
    mixed_send,
    mixed_recv,
    back_send,
    back_recv,
):
    t = lax.axis_index("tm")
    s = lax.axis_index("space")
    nt = lax.axis_size("tm")
    ns = lax.axis_size("space")
    chips = ns // 2
    frames, rows, columns, inner = value_ref.shape
    tokens = frames * rows * columns
    keys_here = (frames + 2) * (rows + 2) * columns
    width = inner // heads
    depth, cols = weight_ref.shape

    def remote(source, target, send, recv, tm, space):
        return pltpu.make_async_remote_copy(
            src_ref=source,
            dst_ref=target,
            send_sem=send,
            recv_sem=recv,
            device_id=(tm, space),
            device_id_type=pl.DeviceIdType.MESH,
        )

    has_low_t, has_high_t = t > 0, t < nt - 1
    has_low_s, has_high_s = s > 0, s < ns - 1
    own_f, own_r = pl.ds(1, frames), pl.ds(1, rows)

    def halo(i, source, target, tm, space):
        return remote(source, target, halo_send.at[i], halo_recv.at[i], tm, space)

    straight = []
    for part, whole in ((1, value_ref), (0, region.at[0, own_f, own_r])):
        straight += [
            (halo(4 * part, whole.at[frames - 1], region.at[part, 0, own_r], t + 1, s), has_high_t, has_low_t),
            (halo(4 * part + 1, whole.at[0], region.at[part, frames + 1, own_r], t - 1, s), has_low_t, has_high_t),
            (halo(4 * part + 2, whole.at[:, rows - 1], region.at[part, own_f, 0], t, s + 1), has_high_s, has_low_s),
            (halo(4 * part + 3, whole.at[:, 0], region.at[part, own_f, rows + 1], t, s - 1), has_low_s, has_high_s),
        ]
    corners = []
    for i, (frame, has_frame) in enumerate(((0, has_low_t), (frames + 1, has_high_t))):
        corners.append((
            halo(8 + 2 * i, region.at[:, frame, rows], region.at[:, frame, 0], t, s + 1),
            has_frame & has_high_s, has_frame & has_low_s,
        ))
        corners.append((
            halo(9 + 2 * i, region.at[:, frame, 1], region.at[:, frame, rows + 1], t, s - 1),
            has_frame & has_low_s, has_frame & has_high_s,
        ))
    parts, lane = weights.shape[0], weights.shape[2]

    def block(b, p):
        return weights.at[p, pl.ds(pl.multiple_of(b * depth, depth), depth)]

    def own_block(p):
        return weight_ref.at[:, pl.ds(pl.multiple_of(p * lane, lane), lane)]

    partner = s + 1 - 2 * lax.rem(s, 2)

    def near(k, b, way, p, first):
        space = s + 2 if way == 0 else s - 2
        source = own_block(p) if first else block(b, p)
        return remote(source, block(b, p), near_send.at[way, k, p], weight_recv.at[b, p], t, space)

    def pair(k, b, way, p, first):
        source = own_block(p) if first else block(b, p)
        return remote(source, block(b, p), pair_send.at[way, k, p], weight_recv.at[b, p], t, partner)

    def arrived(b, p):
        remote(block(b, p), block(b, p), pair_send.at[0, 0, p], weight_recv.at[b, p], t, partner).wait_recv()

    def each_part(low, high, run):
        def body(p, carry):
            run(p)
            return carry

        lax.fori_loop(low, high, body, 0)

    for copy, sends, _ in straight[:4]:
        pl.when(sends)(copy.start)

    def first_part(p):
        pl.when(s + 2 < ns)(near(0, s, 0, p, True).start)
        pl.when(s >= 2)(near(0, s, 1, p, True).start)
        pair(0, s, 0, p, True).start()
        pltpu.make_async_copy(own_block(p), block(s, p), own_sem.at[p]).start()

    each_part(0, parts, first_part)
    own_value = pltpu.make_async_copy(value_ref, region.at[1, own_f, own_r], local_sem.at[0])
    own_value.start()
    own_hidden = pltpu.make_async_copy(hidden_in_ref, hidden_ref, local_sem.at[1])
    own_hidden.start()

    step = 16 if columns % 16 == 0 else columns
    for frame in range(frames):
        for row in range(rows):
            for column in range(0, columns, step):
                at = slice(column, column + step)
                region[0, 1 + frame, 1 + row, at] = normalized(key_ref[frame, row, at], key_gain_ref[...])

    def query_rows(i, carry):
        at = pl.ds(pl.multiple_of(i * 16, 16), 16)
        query_ref[at] = normalized(raw_query_ref[at], query_gain_ref[...])
        return carry

    lax.fori_loop(0, tokens // 16, query_rows, 0)
    for copy, sends, _ in straight[4:]:
        pl.when(sends)(copy.start)

    def clear_frame(frame):
        def run():
            for part in range(2):
                for row in range(rows + 2):
                    region[part, frame, row] = jnp.zeros((columns, inner), jnp.bfloat16)
        return run

    def clear_row(row):
        def run():
            for part in range(2):
                for frame in range(frames + 2):
                    region[part, frame, row] = jnp.zeros((columns, inner), jnp.bfloat16)
        return run

    pl.when(jnp.logical_not(has_low_t))(clear_frame(0))
    pl.when(jnp.logical_not(has_high_t))(clear_frame(frames + 1))
    pl.when(jnp.logical_not(has_low_s))(clear_row(0))
    pl.when(jnp.logical_not(has_high_s))(clear_row(rows + 1))

    frame_k, row_k, tile_k = key_place_ref[0:1], key_place_ref[1:2], key_place_ref[2:3]
    inside = (frame_k >= -t * frames) & (frame_k < (nt - t) * frames)
    inside = inside & (row_k >= -s * rows) & (row_k < (ns - s) * rows)
    outside = jnp.where(inside, 0, 9)
    frame_gap = jnp.abs(query_place_ref[:, 0:1] - frame_k) + outside
    row_gap = jnp.abs(query_place_ref[:, 1:2] - row_k)
    tile_gap = jnp.abs(query_place_ref[:, 2:3] - tile_k)
    for i, (reach_t, reach_r, reach_c) in enumerate(REACHES):
        allowed = (frame_gap <= reach_t) & (row_gap <= reach_r) & (tile_gap <= reach_c)
        mask_ref[i] = jnp.where(allowed, 0.0, -1e30)

    def relay(k, p):
        low, high = s - 2 * k, s + 2 * k

        @pl.when(low >= 0)
        def _():
            arrived(low, p)
            pl.when(s + 2 < ns)(near(k, low, 0, p, False).start)
            pair(k, low, 0, p, False).start()

        @pl.when(high < ns)
        def _():
            arrived(high, p)
            pl.when(s >= 2)(near(k, high, 1, p, False).start)
            pair(k, high, 1, p, False).start()

    def relay_parts(k, low, high):
        if 1 <= k < chips:
            each_part(low, high, functools.partial(relay, k))

    early = parts // 2
    last = chips - 1
    if last > 1:
        relay_parts(1, 0, early)
    for copy, _, receives in straight[0:2] + straight[4:6]:
        pl.when(receives)(copy.wait_recv)
    for copy, sends, _ in corners:
        pl.when(sends)(copy.start)
    for copy, _, receives in straight[2:4] + straight[6:8]:
        pl.when(receives)(copy.wait_recv)
    for copy, _, receives in corners:
        pl.when(receives)(copy.wait_recv)
    if last > 1:
        relay_parts(1, early, parts)
    own_value.wait()

    groups = heads // group
    span = group * width

    def gather(g, d):
        at = (t, slice(None), pl.ds(pl.multiple_of(g * span, span), span))
        return remote(
            mixed.at[at], mixed.at[at], mixed_send.at[d - 1, g], mixed_recv.at[t, g],
            lax.rem(t + d, nt), s,
        )

    def one_group(g, carry):
        for i in range(group):
            h = g * group + i
            lanes = pl.ds(pl.multiple_of(h * width, width), width)
            query = query_ref[:, lanes]
            key = region[0, :, :, :, lanes].reshape(keys_here, width)
            value = region[1, :, :, :, lanes].reshape(keys_here, width)
            scores = lax.dot_general(
                query, key, (((1,), (1,)), ((), ())), preferred_element_type=jnp.float32
            ) * width ** (-0.5)
            scores = scores + mask_ref[time_ref[h] * 6 + rows_ref[h] * 3 + cols_ref[h]]
            part = jnp.exp(scores - jnp.max(scores, axis=1, keepdims=True))
            sums = jnp.sum(part, axis=1, keepdims=True)
            result = jnp.dot(part.astype(jnp.bfloat16), value, preferred_element_type=jnp.float32)
            mixed[t, :, lanes] = (result / sums).astype(jnp.bfloat16)
        for d in range(1, nt):
            gather(g, d).start()
        return carry

    ahead = groups * 5 // 8
    lax.fori_loop(0, ahead, one_group, 0)
    if last > 2:
        relay_parts(2, 0, parts)
    lax.fori_loop(ahead, groups, one_group, 0)
    for k in range(3, last):
        relay_parts(k, 0, parts)

    def gathered(g, carry):
        for d in range(1, nt):
            other = lax.rem(t + d, nt)
            at = (other, slice(None), pl.ds(pl.multiple_of(g * span, span), span))
            remote(mixed.at[at], mixed.at[at], mixed_send.at[d - 1, g], mixed_recv.at[other, g], t, s).wait_recv()
        return carry

    chip_depth = 2 * depth
    piece = chip_depth * 128 // math.gcd(chip_depth, 128)

    def multiply(start, p, first):
        feature = pl.ds(pl.multiple_of(start, piece), piece)
        left = mixed[:, :, feature].reshape(nt * tokens, piece)
        product = jnp.dot(left, weights[p, feature], preferred_element_type=jnp.float32)
        if first:
            total[p] = product
        else:
            total[p] += product

    chip = s // 2
    half = lax.rem(s, 2)

    def add(k, p):
        for other in (chip - k, chip + k):
            @pl.when((other >= 0) & (other < chips))
            def _():
                arrived(2 * other + 1 - half, p)
                multiply(other * piece, p, False)

    def own_rows(owner):
        return pl.ds(pl.multiple_of(owner * tokens, tokens), tokens)

    def back(d, p):
        other = lax.rem(t + d, nt)
        return remote(
            outgoing.at[d - 1, p], incoming.at[d - 1, p], back_send.at[d - 1, p], back_recv.at[d - 1, p], other, s
        )

    def send_back(p):
        for d in range(1, nt):
            outgoing[d - 1, p] = total[p, own_rows(lax.rem(t + d, nt)), :].astype(jnp.bfloat16)
            back(d, p).start()

    def own_part(p):
        pltpu.make_async_copy(own_block(p), block(s, p), own_sem.at[p]).wait()
        arrived(partner, p)

    lax.fori_loop(0, groups, gathered, 0)
    if piece == chip_depth:
        def begin(p):
            own_part(p)
            multiply(chip * piece, p, True)
            for k in range(1, last):
                add(k, p)

        each_part(0, parts, begin)

        def conclude(p):
            if last > 0:
                relay(last, p)
                add(last, p)
            send_back(p)

        each_part(0, parts, conclude)
    else:
        def conclude(p):
            own_part(p)
            if last > 0:
                relay(last, p)
            for k in range(1, chips):
                for other in (chip - k, chip + k):
                    @pl.when((other >= 0) & (other < chips))
                    def _():
                        arrived(2 * other + 1 - half, p)
            multiply(0, p, True)

            def add_piece(i, carry):
                multiply(i * piece, p, False)
                return carry

            lax.fori_loop(1, inner // piece, add_piece, 0)
            send_back(p)

        each_part(0, parts, conclude)

    own_hidden.wait()

    def finish(owner, p, branch):
        lanes = pl.ds(pl.multiple_of(owner * cols + p * lane, lane), lane)
        out_ref[:, lanes] = (
            hidden_ref[:, lanes].astype(jnp.float32) + gate_ref[:, lanes] * branch
        ).astype(jnp.bfloat16)

    def finish_own(p):
        finish(t, p, total[p, own_rows(t), :])

    def finish_others(p):
        for d in range(1, nt):
            back(d, p).wait_recv()
            finish(lax.rem(t + nt - d, nt), p, incoming[d - 1, p].astype(jnp.float32))

    each_part(0, parts, finish_own)
    each_part(0, parts, finish_others)

    for copy, sends, _ in straight + corners:
        pl.when(sends)(copy.wait_send)
    for k in range(chips):
        low, high = s - 2 * k, s + 2 * k

        def weight_sent(p):
            pl.when((low >= 0) & (s + 2 < ns))(near(k, low, 0, p, k == 0).wait_send)
            pl.when((high < ns) & (s >= 2))(near(k, high, 1, p, k == 0).wait_send)
            pl.when(low >= 0)(pair(k, low, 0, p, k == 0).wait_send)
            if k > 0:
                pl.when(high < ns)(pair(k, high, 1, p, False).wait_send)

        each_part(0, parts, weight_sent)

    def sent(g, carry):
        for d in range(1, nt):
            gather(g, d).wait_send()
        return carry

    lax.fori_loop(0, groups, sent, 0)

    def back_sent(p):
        for d in range(1, nt):
            back(d, p).wait_send()

    each_part(0, parts, back_sent)


def ring_shards(
    hidden_in,
    queries,
    keys,
    values,
    query_gain,
    key_gain,
    reach_time,
    reach_rows,
    reach_cols,
    out_weight,
    gate,
):
    frames, rows, columns, inner = queries.shape
    width = hidden_in.shape[3]
    heads = reach_time.shape[0]
    tokens = frames * rows * columns
    nt, ns = lax.axis_size("tm"), lax.axis_size("space")
    depth, cols = out_weight.shape
    group = 5 if heads % 5 == 0 else 1
    vmem = pl.BlockSpec(memory_space=pltpu.VMEM)
    hbm = pl.BlockSpec(memory_space=pl.ANY)
    dma = pltpu.SemaphoreType.DMA
    lane = 256 if cols % 256 == 0 else 128
    parts = cols // lane
    output = pl.pallas_call(
        functools.partial(ring_kernel, heads, group),
        out_shape=jax.ShapeDtypeStruct((tokens, width), jnp.bfloat16),
        in_specs=[pl.BlockSpec(memory_space=pltpu.SMEM)] * 3 + [vmem] * 7 + [hbm] * 3,
        out_specs=vmem,
        scratch_shapes=[
            pltpu.VMEM((tokens, inner), jnp.bfloat16),
            pltpu.VMEM((len(REACHES), tokens, (frames + 2) * (rows + 2) * columns), jnp.float32),
            pltpu.VMEM((tokens, width), jnp.bfloat16),
            pltpu.VMEM((2, frames + 2, rows + 2, columns, inner), jnp.bfloat16),
            pltpu.VMEM((parts, depth * ns, lane), jnp.bfloat16),
            pltpu.VMEM((nt, tokens, inner), jnp.bfloat16),
            pltpu.VMEM((parts, nt * tokens, lane), jnp.float32),
            pltpu.VMEM((nt - 1, parts, tokens, lane), jnp.bfloat16),
            pltpu.VMEM((nt - 1, parts, tokens, lane), jnp.bfloat16),
            dma((2,)),
            dma((parts,)),
            dma((12,)),
            dma((12,)),
            dma((2, ns // 2, parts)),
            dma((2, ns // 2, parts)),
            dma((ns, parts)),
            dma((nt - 1, heads // group)),
            dma((nt, heads // group)),
            dma((nt - 1, parts)),
            dma((nt - 1, parts)),
        ],
        compiler_params=pltpu.CompilerParams(
            has_side_effects=True, vmem_limit_bytes=60 * 1024 * 1024
        ),
    )(
        reach_time,
        reach_rows,
        reach_cols,
        queries.reshape(tokens, inner),
        keys,
        query_gain.reshape(1, inner),
        key_gain.reshape(1, inner),
        places(frames, rows, columns, 0).T,
        places(frames, rows, columns, 1),
        gate.reshape(1, width),
        values,
        out_weight,
        hidden_in.reshape(tokens, width),
    )
    return output.reshape(frames, rows, columns, width)


def pair_kernel(
    heads,
    time_ref,
    rows_ref,
    cols_ref,
    query_gain_ref,
    key_gain_ref,
    query_place_ref,
    key_place_ref,
    gate_ref,
    raw_query_ref,
    raw_key_ref,
    value_ref,
    weight_ref,
    hidden_in_ref,
    out_ref,
    raw,
    normed,
    region,
    query_ref,
    mask_ref,
    mixed,
    weights,
    total,
    partial_out,
    partial_in,
    outgoing,
    incoming,
    hidden_ref,
    result_ref,
    staged,
    local_sem,
    value_sem,
    own_sem,
    swap_send,
    swap_recv,
    side_send,
    side_recv,
    corner_send,
    corner_recv,
    stage_recv,
    near_send,
    cross_send,
    pair_send,
    weight_recv,
    level_send,
    level_recv,
    mixed_send,
    mixed_recv,
    part_send,
    part_recv,
    back_send,
    back_recv,
    out_sem,
):
    t = lax.axis_index("tm")
    s = lax.axis_index("space")
    nt = lax.axis_size("tm")
    ns = lax.axis_size("space")
    frames, rows, columns, inner = value_ref.shape
    tokens = frames * rows * columns
    depth, cols = weight_ref.shape
    width = inner // heads
    groups = ns // 2
    half = inner // 2
    blocks, parts, _, lane = weights.shape
    chips = ns // 4
    row_tokens = rows * columns
    span = 2 * frames

    p = lax.rem(t, 2)
    column_block = lax.div(t, 2)
    c = lax.rem(s, 2)
    z = lax.div(s, 2)
    level = lax.rem(z, 2)
    chip = lax.div(z, 2)
    mate = t + 1 - 2 * p
    partner = s + 1 - 2 * c
    level_mate = s + 2 - 4 * level

    has_low_t, has_high_t = t >= 2, t < nt - 2
    has_low_s, has_high_s = s > 0, s < ns - 1

    def remote(source, target, send, recv, tm, space):
        return pltpu.make_async_remote_copy(
            src_ref=source,
            dst_ref=target,
            send_sem=send,
            recv_sem=recv,
            device_id=(tm, space),
            device_id_type=pl.DeviceIdType.MESH,
        )

    def lanes_at(start, size):
        return pl.ds(pl.multiple_of(start, 128), size)

    def other_column(e):
        return lax.rem(column_block + e, blocks)

    def other_chip(d):
        return lax.rem(chip + d, chips)

    def column_device(e):
        return 2 * other_column(e) + p

    def chip_device(d):
        return 4 * other_chip(d) + 2 * level + c

    levels = 2 * chips
    middle = levels // 2

    def comes_late(d):
        rises = other_chip(d) < chip
        return (rises & (z <= middle)) | (jnp.logical_not(rises) & (z + 1 >= middle))

    starts = {True: z + 2 < levels, False: z >= 2}
    passes = {True: (z >= 1) & (z + 1 < levels), False: (z + 1 < levels) & (z >= 1)}
    inner = {True: z < middle, False: z >= middle}

    load_key = pltpu.make_async_copy(raw_key_ref, raw.at[0], local_sem.at[0])
    load_key.start()
    load_query = pltpu.make_async_copy(raw_query_ref, raw.at[1], local_sem.at[1])
    load_query.start()

    barrier = pltpu.get_barrier_semaphore()

    def greet(tm, space):
        pl.semaphore_signal(
            barrier, inc=1, device_id=(tm, space), device_id_type=pl.DeviceIdType.MESH
        )

    greet(mate, s)
    greet(t, partner)
    greet(t, level_mate)
    for e in range(1, blocks):
        greet(column_device(e), s)
    across = s - 2 + 4 * level
    has_across = (across >= 0) & (across < ns)
    pl.when(has_across)(functools.partial(greet, t, across))
    up, down = (c == 1) & has_high_s, (c == 0) & has_low_s

    @pl.when(up)
    def _():
        greet(t, s + 1)

    @pl.when(down)
    def _():
        greet(t, s - 1)

    pl.semaphore_wait(
        barrier, blocks + 2 + has_across.astype(jnp.int32) + (up | down).astype(jnp.int32)
    )

    own_frames = pl.ds(1 + frames * p, frames)
    own_rows = pl.ds(1, rows)

    def group_lanes(b):
        return pl.ds(b * depth, depth)

    def value_swap(b):
        source = value_ref.at[:, :, :, lanes_at((2 * b + 1 - p) * depth, depth)]
        target = region.at[1, own_frames, own_rows, :, group_lanes(b)]
        return remote(source, target, swap_send.at[1, b], swap_recv.at[1, b], mate, s)

    def key_swap(b):
        source = normed.at[0, 1 - p, :, :, :, group_lanes(b)]
        target = region.at[0, own_frames, own_rows, :, group_lanes(b)]
        return remote(source, target, swap_send.at[0, b], swap_recv.at[0, b], mate, s)

    def query_swap(b):
        source = normed.at[1, 1 - p, :, :, :, group_lanes(b)]
        target = query_ref.at[pl.ds(frames * p, frames), :, :, group_lanes(b)]
        return remote(source, target, swap_send.at[2, b], swap_recv.at[2, b], mate, s)

    def own_value(b):
        return pltpu.make_async_copy(
            value_ref.at[:, :, :, lanes_at((2 * b + p) * depth, depth)],
            region.at[1, own_frames, own_rows, :, group_lanes(b)],
            value_sem.at[b],
        )

    def own_weight(q):
        return weight_ref.at[:, pl.ds(q * lane, lane)]

    def own_weight_at(q):
        return weight_ref.at[:, lanes_at(q * lane, lane)]

    def weight_block(block, chip_index, core, q):
        start = (2 * chip_index + core) * depth
        return weights.at[block, q, pl.ds(pl.multiple_of(start, depth), depth)]

    def arrival(chip_index, core):
        return 2 * chip_index + core

    def keep_weight(q):
        return pltpu.make_async_copy(
            own_weight_at(q), weight_block(column_block, chip, c, q), own_sem.at[q]
        )

    def shares(q, d=1):
        return range(2 if d > 0 and q == parts - 1 else 1)

    def rows_of(q, k, d=1):
        count = len(shares(q, d))
        return pl.ds(k * (depth // count), depth // count)

    def first_hop(rising, q, k):
        at = rows_of(q, k)
        return remote(
            own_weight_at(q).at[at], staged.at[int(rising), q, at],
            near_send.at[0, int(rising), q + k], stage_recv.at[int(rising), q + k],
            t, s + 2 if rising else s - 2,
        )

    def second_hop(rising, q, k):
        origin = lax.div(z + levels - 1 if rising else z + levels + 1, 2) - chips
        at = rows_of(q, k)
        return remote(
            staged.at[int(rising), q, at], weight_block(column_block, origin, c, q).at[at],
            near_send.at[1, int(rising), q + k],
            weight_recv.at[column_block, arrival(origin, c), q + k],
            t, s + 2 if rising else s - 2,
        )

    def cross_weight(e, d, q, k):
        at = rows_of(q, k, d)
        block = weight_block(column_block, other_chip(d), c, q).at[at]
        source = own_weight_at(q).at[at] if d == 0 else block
        return remote(
            source, block, cross_send.at[e - 1, d, q + k],
            weight_recv.at[column_block, arrival(other_chip(d), c), q + k],
            column_device(e), s,
        )

    def pair_weight(e, d, q, k):
        at = rows_of(q, k, d)
        block = weight_block(other_column(e), other_chip(d), c, q).at[at]
        source = own_weight_at(q).at[at] if e == 0 and d == 0 else block
        return remote(
            source, block, pair_send.at[e, d, q + k],
            weight_recv.at[other_column(e), arrival(other_chip(d), c), q + k],
            t, partner,
        )

    def weight_here(e, d, core, q, k):
        block = weight_block(other_column(e), other_chip(d), core, q).at[rows_of(q, k, d)]
        remote(
            block, block, pair_send.at[e, d, q + k],
            weight_recv.at[other_column(e), arrival(other_chip(d), core), q + k], t, partner,
        ).wait_recv()

    at_end = (z == 0) | (z == levels - 1)

    def send_far(q, ends, which=True):
        for rising in (True, False):
            for k in shares(q):
                pl.when(starts[rising] & (at_end == ends) & which)(first_hop(rising, q, k).start)

    def forward(q, inward, which=True):
        for rising in (True, False):
            @pl.when(passes[rising] & (inner[rising] == inward) & which)
            def _(rising=rising):
                for k in shares(q):
                    first_hop(rising, q, k).wait_recv()
                    second_hop(rising, q, k).start()

    def send_cross(q):
        for e in range(1, blocks):
            cross_weight(e, 0, q, 0).start()
        pair_weight(0, 0, q, 0).start()

    def relay_far(q, late):
        for d in range(1, chips):
            @pl.when(comes_late(d) if late else jnp.logical_not(comes_late(d)))
            def _(d=d):
                for k in shares(q):
                    weight_here(0, d, c, q, k)
                    for e in range(1, blocks):
                        cross_weight(e, d, q, k).start()
                    pair_weight(0, d, q, k).start()

    def relay_cross(q, far):
        for e in range(1, blocks):
            for d in range(1, chips) if far else (0,):
                for k in shares(q, d):
                    weight_here(e, d, c, q, k)
                    pair_weight(e, d, q, k).start()

    value_swap(0).start()
    for b in range(groups):
        own_value(b).start()
    send_far(0, True)
    send_far(0, False)
    send_far(1, False)
    send_cross(0)
    for q in range(parts):
        keep_weight(q).start()
    own_hidden = pltpu.make_async_copy(hidden_in_ref, hidden_ref, local_sem.at[2])
    own_hidden.start()

    step = 16 if columns % 16 == 0 else columns

    def normalize(index, gain_ref):
        for frame in range(frames):
            for row in range(rows):
                for column in range(0, columns, step):
                    at = slice(column, column + step)
                    result = normalized(raw[index, frame, row, at], gain_ref[...])
                    for b in range(groups):
                        for core in range(2):
                            start = (2 * b + core) * depth
                            normed[index, core, frame, row, at, b * depth:(b + 1) * depth] = (
                                result[:, start:start + depth]
                            )

    load_key.wait()
    with jax.named_scope("normalize_key"):
        normalize(0, key_gain_ref)
    key_swap(0).start()
    own_key = pltpu.make_async_copy(
        normed.at[0, p], region.at[0, own_frames, own_rows], local_sem.at[3]
    )
    own_key.start()
    load_query.wait()
    with jax.named_scope("normalize_query"):
        normalize(1, query_gain_ref)
    query_swap(0).start()
    own_query = pltpu.make_async_copy(
        normed.at[1, p], query_ref.at[pl.ds(frames * p, frames)], local_sem.at[4]
    )
    own_query.start()
    for b in range(1, groups):
        value_swap(b).start()
        key_swap(b).start()
        query_swap(b).start()

    def clear_frame(frame):
        def run():
            for part in range(2):
                for row in range(rows + 2):
                    region[part, frame, row] = jnp.zeros((columns, half), jnp.bfloat16)
        return run

    def clear_row(row):
        def run():
            for part in range(2):
                for frame in range(span + 2):
                    region[part, frame, row] = jnp.zeros((columns, half), jnp.bfloat16)
        return run

    pl.when(jnp.logical_not(has_low_t))(clear_frame(0))
    pl.when(jnp.logical_not(has_high_t))(clear_frame(span + 1))
    pl.when(jnp.logical_not(has_low_s))(clear_row(0))
    pl.when(jnp.logical_not(has_high_s))(clear_row(rows + 1))

    frame_k, row_k, tile_k = key_place_ref[0:1], key_place_ref[1:2], key_place_ref[2:3]
    inside = (row_k >= -s * rows) & (row_k < (ns - s) * rows)
    row_gap = jnp.abs(query_place_ref[:, 0:1] - row_k) + jnp.where(inside, 0, 9)
    tile_gap = jnp.abs(query_place_ref[:, 1:2] - tile_k)
    low_gap = jnp.where(has_low_t, 0, 9) * (frame_k < 0).astype(jnp.int32)
    high_gap = jnp.where(has_high_t, 0, 9) * (frame_k > 0).astype(jnp.int32)
    for kind, edge in enumerate((jnp.zeros_like(low_gap), low_gap, high_gap)):
        frame_gap = jnp.abs(frame_k) + edge
        for i, (reach_t, reach_r, reach_c) in enumerate(REACHES):
            allowed = (frame_gap <= reach_t) & (row_gap <= reach_r) & (tile_gap <= reach_c)
            mask_ref[kind, i] = jnp.where(allowed, 0.0, -1e30)

    pair_frames = pl.ds(1, span)

    def row_up(b):
        return remote(
            region.at[:, pair_frames, rows, :, group_lanes(b)],
            region.at[:, pair_frames, 0, :, group_lanes(b)],
            side_send.at[0, b], side_recv.at[0, b], t, s + 1,
        )

    def row_down(b):
        return remote(
            region.at[:, pair_frames, 1, :, group_lanes(b)],
            region.at[:, pair_frames, rows + 1, :, group_lanes(b)],
            side_send.at[1, b], side_recv.at[1, b], t, s - 1,
        )

    def frame_up(b):
        return remote(
            region.at[:, span, own_rows, :, group_lanes(b)],
            region.at[:, 0, own_rows, :, group_lanes(b)],
            side_send.at[2, b], side_recv.at[2, b], t + 2, s,
        )

    def frame_down(b):
        return remote(
            region.at[:, 1, own_rows, :, group_lanes(b)],
            region.at[:, span + 1, own_rows, :, group_lanes(b)],
            side_send.at[3, b], side_recv.at[3, b], t - 2, s,
        )

    def sides(b):
        return (
            (frame_up(b), has_high_t, has_low_t),
            (frame_down(b), has_low_t, has_high_t),
            (row_up(b), has_high_s, has_low_s),
            (row_down(b), has_low_s, has_high_s),
        )

    def corners(b):
        result = []
        for i, (frame, has_frame) in enumerate(((0, has_low_t), (span + 1, has_high_t))):
            for j, (row, landing, space, sends, receives) in enumerate((
                (rows, 0, s + 1, has_high_s, has_low_s),
                (1, rows + 1, s - 1, has_low_s, has_high_s),
            )):
                copy = remote(
                    region.at[:, frame, row, :, group_lanes(b)],
                    region.at[:, frame, landing, :, group_lanes(b)],
                    corner_send.at[2 * i + j, b], corner_recv.at[2 * i + j, b], t, space,
                )
                result.append((copy, has_frame & sends, has_frame & receives))
        return result

    def feature_lanes(index, core):
        return lanes_at((2 * index + core) * depth, depth)

    def to_level_mate(j):
        at = (slice(None), feature_lanes(j, p))
        return remote(
            mixed.at[(2,) + at], mixed.at[(level,) + at],
            level_send.at[j], level_recv.at[j], t, level_mate,
        )

    def from_level_mate(j):
        at = (1 - level, slice(None), feature_lanes(j, p))
        return remote(mixed.at[at], mixed.at[at], level_send.at[j], level_recv.at[j], t, level_mate)

    def to_mate(which, j):
        at = (which, slice(None), feature_lanes(j, p))
        return remote(
            mixed.at[at], mixed.at[at], mixed_send.at[which, j], mixed_recv.at[which, j], mate, s
        )

    def from_mate(which, j):
        at = (which, slice(None), feature_lanes(j, 1 - p))
        remote(
            mixed.at[at], mixed.at[at], mixed_send.at[which, j], mixed_recv.at[which, j], mate, s
        ).wait_recv()

    def attend(b):
        in_level = level == b % 2
        place = jnp.where(in_level, level, 2)
        index = b // 2
        group = depth // width

        def one_head(i, carry):
            h = (2 * b + p) * group + i
            lanes = lanes_at(b * depth + i * width, width)
            reach = time_ref[h] * 6 + rows_ref[h] * 3 + cols_ref[h]
            target = lanes_at((2 * index + p) * depth + i * width, width)
            scores, values = [], []
            for frame in range(span):
                query = query_ref[frame, :, :, lanes].reshape(row_tokens, width)
                near = slice(frame, frame + 3)
                key = region[0, near, :, :, lanes].reshape(-1, width)
                values.append(region[1, near, :, :, lanes].reshape(-1, width))
                scores.append(lax.dot_general(
                    query, key, (((1,), (1,)), ((), ())), preferred_element_type=jnp.float32
                ))
            results = []
            for frame in range(span):
                kind = 1 if frame == 0 else 2 if frame == span - 1 else 0
                masked = scores[frame] * width ** (-0.5) + mask_ref[kind, reach]
                part = jnp.exp(masked - jnp.max(masked, axis=1, keepdims=True))
                sums = jnp.sum(part, axis=1, keepdims=True)
                result = jnp.dot(
                    part.astype(jnp.bfloat16), values[frame], preferred_element_type=jnp.float32
                )
                results.append((result / sums).astype(jnp.bfloat16))
            mixed[place, :, target] = jnp.concatenate(results, axis=0)
            return carry

        lax.fori_loop(0, group, one_head, 0)

    def send_mixed(b):
        pl.when(level != b % 2)(to_level_mate(b // 2).start)

    def relay_mixed(b):
        @pl.when(level == b % 2)
        def _():
            from_level_mate(b // 2).wait_recv()
            to_mate(1 - level, b // 2).start()
            to_mate(level, b // 2).start()

    def arrive(i):
        with jax.named_scope(f"wait_swap{i}"):
            value_swap(i).wait_recv()
            key_swap(i).wait_recv()
            own_value(i).wait()
            if i == 0:
                own_key.wait()
        with jax.named_scope(f"send_sides{i}"):
            for copy, sends, _ in sides(i):
                pl.when(sends)(copy.start)

    def turn(i):
        with jax.named_scope(f"wait_frames{i}"):
            for copy, _, receives in sides(i)[:2]:
                pl.when(receives)(copy.wait_recv)
        for copy, sends, _ in corners(i):
            pl.when(sends)(copy.start)

    def ready(b):
        with jax.named_scope(f"wait_query{b}"):
            query_swap(b).wait_recv()
            if b == 0:
                own_query.wait()
        with jax.named_scope(f"wait_rows{b}"):
            for copy, _, receives in sides(b)[2:]:
                pl.when(receives)(copy.wait_recv)
        with jax.named_scope(f"wait_corners{b}"):
            for copy, _, receives in corners(b):
                pl.when(receives)(copy.wait_recv)

    early = min(2, parts)
    actions = {
        "end": lambda q: send_far(q, True),
        "end0": lambda q: send_far(q, True, level == 0),
        "end1": lambda q: send_far(q, True, level == 1),
        "out0": lambda q: forward(q, False, level == 0),
        "out1": lambda q: forward(q, False, level == 1),
        "mid": lambda q: send_far(q, False),
        "late": lambda q: relay_far(q, True),
        "cross": send_cross,
        "out": lambda q: forward(q, False),
        "in": lambda q: forward(q, True),
        "early": lambda q: relay_far(q, False),
    }
    plan = {i: [] for i in range(groups + 1)}
    plan[0] += [("mid", 2), ("end", 1), ("cross", 1), ("out", 0)]
    plan[1] += [("mid", 3), ("end0", 2), ("cross", 2), ("out0", 1)]
    plan[2] += [("end1", 2), ("cross", 3), ("out1", 1)]
    plan[3] += [("in", 0), ("mid", 4), ("end0", 3), ("out0", 2), ("cross", 4), ("early", 0), ("early", 1)]
    plan[groups] += [("in", 1), ("end1", 3), ("end", 4), ("out1", 2), ("out", 3), ("late", 0)]
    plan[groups] += [("cross", q) for q in range(5, parts)]
    for i in range(groups + 1):
        if i < groups:
            arrive(i)
        if i > 0:
            ready(i - 1)
            with jax.named_scope(f"attend{i - 1}"):
                attend(i - 1)
        if i < groups:
            turn(i)
        if i > 0:
            send_mixed(i - 1)
        for kind, q in plan[i]:
            if q < parts:
                actions[kind](q)
        if i > 1:
            with jax.named_scope(f"relay_mixed{i}"):
                relay_mixed(i - 2)
        if i > 1 and i - 2 < parts:
            with jax.named_scope(f"relay_cross{i}"):
                relay_cross(i - 2, False)
    with jax.named_scope("relay_mixed_last"):
        relay_mixed(groups - 1)

    def each_part(low, high, run):
        def body(q, carry):
            run(q)
            return carry

        lax.fori_loop(low, high, body, 0)

    def next_far(q):
        if q < parts:
            with jax.named_scope(f"relay_far{q}"):
                relay_far(q, True)

    def multiply_theirs(e, q):
        block = other_column(e)
        for d in range(chips):
            for k in shares(q, d):
                weight_here(e, d, 1 - c, q, k)
        product = jnp.dot(
            mixed[1 - level], weights[block, q], preferred_element_type=jnp.float32
        )
        partial_out[block, q] = product.astype(jnp.bfloat16)
        part_copy(block, q).start()

    def multiply_ours(e, q):
        block = other_column(e)
        total[block, q] = jnp.dot(
            mixed[level], weights[block, q], preferred_element_type=jnp.float32
        )

    def part_copy(block, q):
        return remote(
            partial_out.at[block, q], partial_in.at[block, q],
            part_send.at[block, q], part_recv.at[block, q], t, level_mate,
        )

    def back(block, q):
        return remote(
            outgoing.at[block, q], incoming.at[block, q],
            back_send.at[block, q], back_recv.at[block, q], mate, s,
        )

    def token_rows(side):
        return pl.ds(pl.multiple_of(side * tokens, tokens), tokens)

    def finish(column, branch, index, q):
        lanes = lanes_at(column, lane)
        result_ref[:, lanes] = (
            hidden_ref[:, lanes].astype(jnp.float32) + gate_ref[:, lanes] * branch
        ).astype(jnp.bfloat16)
        write_out(column, index, q).start()

    def write_out(column, index, q):
        lanes = lanes_at(column, lane)
        return pltpu.make_async_copy(
            result_ref.at[:, lanes], out_ref.at[:, lanes], out_sem.at[index, q]
        )

    def reduce_part(q):
        for e in range(blocks):
            block = other_column(e)
            part_copy(block, q).wait_recv()
            theirs = token_rows(1 - p)
            outgoing[block, q] = (
                total[block, q, theirs] + partial_in[block, q, theirs].astype(jnp.float32)
            ).astype(jnp.bfloat16)
            back(block, q).start()
            ours = token_rows(p)
            branch = total[block, q, ours] + partial_in[block, q, ours].astype(jnp.float32)
            finish((2 * block + p) * cols + q * lane, branch, 2 * block + p, q)

    def theirs(q):
        if q >= groups - 1:
            relay_cross(q, False)
        keep_weight(q).wait()
        with jax.named_scope(f"theirs{q}own"):
            multiply_theirs(0, q)
        if blocks > 1:
            with jax.named_scope(f"main_cross{q}"):
                relay_cross(q, True)
            with jax.named_scope(f"theirs{q}other"):
                for e in range(1, blocks):
                    multiply_theirs(e, q)

    def ours(q):
        with jax.named_scope(f"ours{q}"):
            for e in range(blocks):
                multiply_ours(e, q)

    forward(2, True)
    relay_far(2, False)
    forward(4, False)
    forward(3, True)
    relay_far(3, False)
    next_far(1)
    with jax.named_scope("from_mate_theirs"):
        for j in range(groups // 2):
            from_mate(1 - level, j)
    theirs(0)
    forward(4, True)
    next_far(2)
    theirs(1)
    relay_far(4, False)
    with jax.named_scope("from_mate_ours"):
        for j in range(groups // 2):
            from_mate(level, j)
    ours(0)
    own_hidden.wait()
    next_far(3)
    theirs(2)
    next_far(4)
    ours(1)
    with jax.named_scope("reduce01"):
        reduce_part(0)
        reduce_part(1)
    theirs(3)
    ours(2)
    ours(3)
    with jax.named_scope("reduce2"):
        reduce_part(2)
    with jax.named_scope("reduce3a"):
        pl.when(jnp.logical_not(at_end))(functools.partial(reduce_part, 3))
    theirs(4)
    ours(4)

    def finish_others(q):
        for block in range(blocks):
            back(block, q).wait_recv()
            finish(
                (2 * block + 1 - p) * cols + q * lane,
                incoming[block, q].astype(jnp.float32), 2 * block + 1 - p, q,
            )

    with jax.named_scope("reduce3b"):
        pl.when(at_end)(functools.partial(reduce_part, 3))
    with jax.named_scope("finish01"):
        each_part(0, 2, finish_others)
    with jax.named_scope("reduce4"):
        reduce_part(4)
    with jax.named_scope("finish2"):
        each_part(2, parts, finish_others)

    for b in range(groups):
        value_swap(b).wait_send()
        key_swap(b).wait_send()
        query_swap(b).wait_send()
        for copy, sends, _ in sides(b) + tuple(corners(b)):
            pl.when(sends)(copy.wait_send)
    for j in range(groups // 2):
        to_level_mate(j).wait_send()
        for which in range(2):
            to_mate(which, j).wait_send()

    def weight_sent(q):
        for k in shares(q):
            for rising in (True, False):
                pl.when(starts[rising])(first_hop(rising, q, k).wait_send)
                pl.when(passes[rising])(second_hop(rising, q, k).wait_send)
        for e in range(blocks):
            for d in range(chips):
                for k in shares(q, d):
                    pair_weight(e, d, q, k).wait_send()
                    if e > 0:
                        cross_weight(e, d, q, k).wait_send()

    for q in range(parts):
        weight_sent(q)

    def sent(q):
        for block in range(blocks):
            part_copy(block, q).wait_send()
            back(block, q).wait_send()
        for index in range(nt):
            write_out(index * cols + q * lane, index, q).wait()

    each_part(0, parts, sent)


def pair_shards(
    hidden_in,
    queries,
    keys,
    values,
    query_gain,
    key_gain,
    reach_time,
    reach_rows,
    reach_cols,
    out_weight,
    gate,
):
    frames, rows, columns, inner = queries.shape
    width = hidden_in.shape[3]
    heads = reach_time.shape[0]
    tokens = frames * rows * columns
    nt, ns = lax.axis_size("tm"), lax.axis_size("space")
    depth, cols = out_weight.shape
    lane = 256 if cols % 256 == 0 else 128
    parts = cols // lane
    blocks, chips, groups = nt // 2, ns // 4, ns // 2
    half = inner // 2
    pair_tokens = 2 * tokens
    vmem = pl.BlockSpec(memory_space=pltpu.VMEM)
    hbm = pl.BlockSpec(memory_space=pl.ANY)
    dma = pltpu.SemaphoreType.DMA
    _, query_row, query_tile = places(1, rows, columns, 0)
    key_place = np.stack([axis.reshape(-1) for axis in np.meshgrid(
        np.arange(-1, 2), np.arange(-1, rows + 1), np.arange(columns) // TW, indexing="ij"
    )]).astype(np.int32)
    output = pl.pallas_call(
        functools.partial(pair_kernel, heads),
        out_shape=jax.ShapeDtypeStruct((tokens, width), jnp.bfloat16),
        in_specs=[pl.BlockSpec(memory_space=pltpu.SMEM)] * 3 + [vmem] * 5 + [hbm] * 5,
        out_specs=hbm,
        scratch_shapes=[
            pltpu.VMEM((2, frames, rows, columns, inner), jnp.bfloat16),
            pltpu.VMEM((2, 2, frames, rows, columns, half), jnp.bfloat16),
            pltpu.VMEM((2, 2 * frames + 2, rows + 2, columns, half), jnp.bfloat16),
            pltpu.VMEM((2 * frames, rows, columns, half), jnp.bfloat16),
            pltpu.VMEM((3, len(REACHES), rows * columns, 3 * (rows + 2) * columns), jnp.float32),
            pltpu.VMEM((3, pair_tokens, half), jnp.bfloat16),
            pltpu.VMEM((blocks, parts, half, lane), jnp.bfloat16),
            pltpu.VMEM((blocks, parts, pair_tokens, lane), jnp.float32),
            pltpu.VMEM((blocks, parts, pair_tokens, lane), jnp.bfloat16),
            pltpu.VMEM((blocks, parts, pair_tokens, lane), jnp.bfloat16),
            pltpu.VMEM((blocks, parts, tokens, lane), jnp.bfloat16),
            pltpu.VMEM((blocks, parts, tokens, lane), jnp.bfloat16),
            pltpu.VMEM((tokens, width), jnp.bfloat16),
            pltpu.VMEM((tokens, width), jnp.bfloat16),
            pltpu.VMEM((2, parts, depth, lane), jnp.bfloat16),
            dma((5,)),
            dma((groups,)),
            dma((parts,)),
            dma((3, groups)),
            dma((3, groups)),
            dma((4, groups)),
            dma((4, groups)),
            dma((4, groups)),
            dma((4, groups)),
            dma((2, parts + 1)),
            dma((2, 2, parts + 1)),
            dma((max(blocks - 1, 1), chips, parts + 1)),
            dma((blocks, chips, parts + 1)),
            dma((blocks, 2 * chips, parts + 1)),
            dma((groups // 2,)),
            dma((groups // 2,)),
            dma((2, groups // 2)),
            dma((2, groups // 2)),
            dma((blocks, parts)),
            dma((blocks, parts)),
            dma((blocks, parts)),
            dma((blocks, parts)),
            dma((nt, parts)),
        ],
        compiler_params=pltpu.CompilerParams(
            collective_id=0, has_side_effects=True, vmem_limit_bytes=60 * 1024 * 1024
        ),
    )(
        reach_time,
        reach_rows,
        reach_cols,
        query_gain.reshape(1, inner),
        key_gain.reshape(1, inner),
        np.stack([query_row, query_tile]).T,
        key_place,
        gate.reshape(1, width),
        queries,
        keys,
        values,
        out_weight,
        hidden_in.reshape(tokens, width),
    )
    return output.reshape(frames, rows, columns, width)


def shards(hidden_in, queries, keys, values, *others):
    out_weight, reach_time = others[-2], others[2]
    width = queries.shape[3] // reach_time.shape[0]
    nt, ns = lax.axis_size("tm"), lax.axis_size("space")
    whole_heads = out_weight.shape[0] % width == 0
    form = pair_shards if whole_heads and nt % 2 == 0 and ns // 4 == 2 else ring_shards
    return form(hidden_in, queries, keys, values, *others)


def solution(mesh):
    in_specs = (
        P("tm", "space", None, None),
        P("tm", "space", None, None),
        P("tm", "space", None, None),
        P("tm", "space", None, None),
        P(),
        P(),
        P(),
        P(),
        P(),
        P("space", "tm"),
        P(),
    )
    out_specs = P("tm", "space", None, None)
    return jax.shard_map(shards, mesh=mesh, in_specs=in_specs, out_specs=out_specs, check_vma=False)
```

```python
import functools
import math

import jax
import jax.numpy as jnp
import numpy as np
from jax import lax
from jax.experimental import pallas as pl
from jax.experimental.pallas import tpu as pltpu
from jax.sharding import PartitionSpec as P

TW = 8
REACHES = [(a, b, c) for a in range(2) for b in range(2) for c in range(3)]


def normalized(source, gain):
    values_f = source.astype(jnp.float32)
    mean_square = jnp.mean(values_f * values_f, axis=-1, keepdims=True)
    return (values_f * lax.rsqrt(mean_square + 1e-06) * gain).astype(jnp.bfloat16)


def places(frames, rows, columns, margin):
    grid = np.meshgrid(
        np.arange(-margin, frames + margin),
        np.arange(-margin, rows + margin),
        np.arange(columns) // TW,
        indexing="ij",
    )
    return np.stack([axis.reshape(-1) for axis in grid]).astype(np.int32)


def ring_kernel(
    heads,
    group,
    time_ref,
    rows_ref,
    cols_ref,
    raw_query_ref,
    key_ref,
    query_gain_ref,
    key_gain_ref,
    query_place_ref,
    key_place_ref,
    gate_ref,
    value_ref,
    weight_ref,
    hidden_in_ref,
    out_ref,
    query_ref,
    mask_ref,
    hidden_ref,
    region,
    weights,
    mixed,
    total,
    outgoing,
    incoming,
    local_sem,
    own_sem,
    halo_send,
    halo_recv,
    near_send,
    pair_send,
    weight_recv,
    mixed_send,
    mixed_recv,
    back_send,
    back_recv,
):
    t = lax.axis_index("tm")
    s = lax.axis_index("space")
    nt = lax.axis_size("tm")
    ns = lax.axis_size("space")
    chips = ns // 2
    frames, rows, columns, inner = value_ref.shape
    tokens = frames * rows * columns
    keys_here = (frames + 2) * (rows + 2) * columns
    width = inner // heads
    depth, cols = weight_ref.shape

    def remote(source, target, send, recv, tm, space):
        return pltpu.make_async_remote_copy(
            src_ref=source,
            dst_ref=target,
            send_sem=send,
            recv_sem=recv,
            device_id=(tm, space),
            device_id_type=pl.DeviceIdType.MESH,
        )

    has_low_t, has_high_t = t > 0, t < nt - 1
    has_low_s, has_high_s = s > 0, s < ns - 1
    own_f, own_r = pl.ds(1, frames), pl.ds(1, rows)

    def halo(i, source, target, tm, space):
        return remote(source, target, halo_send.at[i], halo_recv.at[i], tm, space)

    straight = []
    for part, whole in ((1, value_ref), (0, region.at[0, own_f, own_r])):
        straight += [
            (halo(4 * part, whole.at[frames - 1], region.at[part, 0, own_r], t + 1, s), has_high_t, has_low_t),
            (halo(4 * part + 1, whole.at[0], region.at[part, frames + 1, own_r], t - 1, s), has_low_t, has_high_t),
            (halo(4 * part + 2, whole.at[:, rows - 1], region.at[part, own_f, 0], t, s + 1), has_high_s, has_low_s),
            (halo(4 * part + 3, whole.at[:, 0], region.at[part, own_f, rows + 1], t, s - 1), has_low_s, has_high_s),
        ]
    corners = []
    for i, (frame, has_frame) in enumerate(((0, has_low_t), (frames + 1, has_high_t))):
        corners.append((
            halo(8 + 2 * i, region.at[:, frame, rows], region.at[:, frame, 0], t, s + 1),
            has_frame & has_high_s, has_frame & has_low_s,
        ))
        corners.append((
            halo(9 + 2 * i, region.at[:, frame, 1], region.at[:, frame, rows + 1], t, s - 1),
            has_frame & has_low_s, has_frame & has_high_s,
        ))
    parts, lane = weights.shape[0], weights.shape[2]

    def block(b, p):
        return weights.at[p, pl.ds(pl.multiple_of(b * depth, depth), depth)]

    def own_block(p):
        return weight_ref.at[:, pl.ds(pl.multiple_of(p * lane, lane), lane)]

    partner = s + 1 - 2 * lax.rem(s, 2)

    def near(k, b, way, p, first):
        space = s + 2 if way == 0 else s - 2
        source = own_block(p) if first else block(b, p)
        return remote(source, block(b, p), near_send.at[way, k, p], weight_recv.at[b, p], t, space)

    def pair(k, b, way, p, first):
        source = own_block(p) if first else block(b, p)
        return remote(source, block(b, p), pair_send.at[way, k, p], weight_recv.at[b, p], t, partner)

    def arrived(b, p):
        remote(block(b, p), block(b, p), pair_send.at[0, 0, p], weight_recv.at[b, p], t, partner).wait_recv()

    def each_part(low, high, run):
        def body(p, carry):
            run(p)
            return carry

        lax.fori_loop(low, high, body, 0)

    for copy, sends, _ in straight[:4]:
        pl.when(sends)(copy.start)

    def first_part(p):
        pl.when(s + 2 < ns)(near(0, s, 0, p, True).start)
        pl.when(s >= 2)(near(0, s, 1, p, True).start)
        pair(0, s, 0, p, True).start()
        pltpu.make_async_copy(own_block(p), block(s, p), own_sem.at[p]).start()

    each_part(0, parts, first_part)
    own_value = pltpu.make_async_copy(value_ref, region.at[1, own_f, own_r], local_sem.at[0])
    own_value.start()
    own_hidden = pltpu.make_async_copy(hidden_in_ref, hidden_ref, local_sem.at[1])
    own_hidden.start()

    step = 16 if columns % 16 == 0 else columns
    for frame in range(frames):
        for row in range(rows):
            for column in range(0, columns, step):
                at = slice(column, column + step)
                region[0, 1 + frame, 1 + row, at] = normalized(key_ref[frame, row, at], key_gain_ref[...])

    def query_rows(i, carry):
        at = pl.ds(pl.multiple_of(i * 16, 16), 16)
        query_ref[at] = normalized(raw_query_ref[at], query_gain_ref[...])
        return carry

    lax.fori_loop(0, tokens // 16, query_rows, 0)
    for copy, sends, _ in straight[4:]:
        pl.when(sends)(copy.start)

    def clear_frame(frame):
        def run():
            for part in range(2):
                for row in range(rows + 2):
                    region[part, frame, row] = jnp.zeros((columns, inner), jnp.bfloat16)
        return run

    def clear_row(row):
        def run():
            for part in range(2):
                for frame in range(frames + 2):
                    region[part, frame, row] = jnp.zeros((columns, inner), jnp.bfloat16)
        return run

    pl.when(jnp.logical_not(has_low_t))(clear_frame(0))
    pl.when(jnp.logical_not(has_high_t))(clear_frame(frames + 1))
    pl.when(jnp.logical_not(has_low_s))(clear_row(0))
    pl.when(jnp.logical_not(has_high_s))(clear_row(rows + 1))

    frame_k, row_k, tile_k = key_place_ref[0:1], key_place_ref[1:2], key_place_ref[2:3]
    inside = (frame_k >= -t * frames) & (frame_k < (nt - t) * frames)
    inside = inside & (row_k >= -s * rows) & (row_k < (ns - s) * rows)
    outside = jnp.where(inside, 0, 9)
    frame_gap = jnp.abs(query_place_ref[:, 0:1] - frame_k) + outside
    row_gap = jnp.abs(query_place_ref[:, 1:2] - row_k)
    tile_gap = jnp.abs(query_place_ref[:, 2:3] - tile_k)
    for i, (reach_t, reach_r, reach_c) in enumerate(REACHES):
        allowed = (frame_gap <= reach_t) & (row_gap <= reach_r) & (tile_gap <= reach_c)
        mask_ref[i] = jnp.where(allowed, 0.0, -1e30)

    def relay(k, p):
        low, high = s - 2 * k, s + 2 * k

        @pl.when(low >= 0)
        def _():
            arrived(low, p)
            pl.when(s + 2 < ns)(near(k, low, 0, p, False).start)
            pair(k, low, 0, p, False).start()

        @pl.when(high < ns)
        def _():
            arrived(high, p)
            pl.when(s >= 2)(near(k, high, 1, p, False).start)
            pair(k, high, 1, p, False).start()

    def relay_parts(k, low, high):
        if 1 <= k < chips:
            each_part(low, high, functools.partial(relay, k))

    early = parts // 2
    last = chips - 1
    if last > 1:
        relay_parts(1, 0, early)
    for copy, _, receives in straight[0:2] + straight[4:6]:
        pl.when(receives)(copy.wait_recv)
    for copy, sends, _ in corners:
        pl.when(sends)(copy.start)
    for copy, _, receives in straight[2:4] + straight[6:8]:
        pl.when(receives)(copy.wait_recv)
    for copy, _, receives in corners:
        pl.when(receives)(copy.wait_recv)
    if last > 1:
        relay_parts(1, early, parts)
    own_value.wait()

    groups = heads // group
    span = group * width

    def gather(g, d):
        at = (t, slice(None), pl.ds(pl.multiple_of(g * span, span), span))
        return remote(
            mixed.at[at], mixed.at[at], mixed_send.at[d - 1, g], mixed_recv.at[t, g],
            lax.rem(t + d, nt), s,
        )

    def one_group(g, carry):
        for i in range(group):
            h = g * group + i
            lanes = pl.ds(pl.multiple_of(h * width, width), width)
            query = query_ref[:, lanes]
            key = region[0, :, :, :, lanes].reshape(keys_here, width)
            value = region[1, :, :, :, lanes].reshape(keys_here, width)
            scores = lax.dot_general(
                query, key, (((1,), (1,)), ((), ())), preferred_element_type=jnp.float32
            ) * width ** (-0.5)
            scores = scores + mask_ref[time_ref[h] * 6 + rows_ref[h] * 3 + cols_ref[h]]
            part = jnp.exp(scores - jnp.max(scores, axis=1, keepdims=True))
            sums = jnp.sum(part, axis=1, keepdims=True)
            result = jnp.dot(part.astype(jnp.bfloat16), value, preferred_element_type=jnp.float32)
            mixed[t, :, lanes] = (result / sums).astype(jnp.bfloat16)
        for d in range(1, nt):
            gather(g, d).start()
        return carry

    ahead = groups * 5 // 8
    lax.fori_loop(0, ahead, one_group, 0)
    if last > 2:
        relay_parts(2, 0, parts)
    lax.fori_loop(ahead, groups, one_group, 0)
    for k in range(3, last):
        relay_parts(k, 0, parts)

    def gathered(g, carry):
        for d in range(1, nt):
            other = lax.rem(t + d, nt)
            at = (other, slice(None), pl.ds(pl.multiple_of(g * span, span), span))
            remote(mixed.at[at], mixed.at[at], mixed_send.at[d - 1, g], mixed_recv.at[other, g], t, s).wait_recv()
        return carry

    chip_depth = 2 * depth
    piece = chip_depth * 128 // math.gcd(chip_depth, 128)

    def multiply(start, p, first):
        feature = pl.ds(pl.multiple_of(start, piece), piece)
        left = mixed[:, :, feature].reshape(nt * tokens, piece)
        product = jnp.dot(left, weights[p, feature], preferred_element_type=jnp.float32)
        if first:
            total[p] = product
        else:
            total[p] += product

    chip = s // 2
    half = lax.rem(s, 2)

    def add(k, p):
        for other in (chip - k, chip + k):
            @pl.when((other >= 0) & (other < chips))
            def _():
                arrived(2 * other + 1 - half, p)
                multiply(other * piece, p, False)

    def own_rows(owner):
        return pl.ds(pl.multiple_of(owner * tokens, tokens), tokens)

    def back(d, p):
        other = lax.rem(t + d, nt)
        return remote(
            outgoing.at[d - 1, p], incoming.at[d - 1, p], back_send.at[d - 1, p], back_recv.at[d - 1, p], other, s
        )

    def send_back(p):
        for d in range(1, nt):
            outgoing[d - 1, p] = total[p, own_rows(lax.rem(t + d, nt)), :].astype(jnp.bfloat16)
            back(d, p).start()

    def own_part(p):
        pltpu.make_async_copy(own_block(p), block(s, p), own_sem.at[p]).wait()
        arrived(partner, p)

    lax.fori_loop(0, groups, gathered, 0)
    if piece == chip_depth:
        def begin(p):
            own_part(p)
            multiply(chip * piece, p, True)
            for k in range(1, last):
                add(k, p)

        each_part(0, parts, begin)

        def conclude(p):
            if last > 0:
                relay(last, p)
                add(last, p)
            send_back(p)

        each_part(0, parts, conclude)
    else:
        def conclude(p):
            own_part(p)
            if last > 0:
                relay(last, p)
            for k in range(1, chips):
                for other in (chip - k, chip + k):
                    @pl.when((other >= 0) & (other < chips))
                    def _():
                        arrived(2 * other + 1 - half, p)
            multiply(0, p, True)

            def add_piece(i, carry):
                multiply(i * piece, p, False)
                return carry

            lax.fori_loop(1, inner // piece, add_piece, 0)
            send_back(p)

        each_part(0, parts, conclude)

    own_hidden.wait()

    def finish(owner, p, branch):
        lanes = pl.ds(pl.multiple_of(owner * cols + p * lane, lane), lane)
        out_ref[:, lanes] = (
            hidden_ref[:, lanes].astype(jnp.float32) + gate_ref[:, lanes] * branch
        ).astype(jnp.bfloat16)

    def finish_own(p):
        finish(t, p, total[p, own_rows(t), :])

    def finish_others(p):
        for d in range(1, nt):
            back(d, p).wait_recv()
            finish(lax.rem(t + nt - d, nt), p, incoming[d - 1, p].astype(jnp.float32))

    each_part(0, parts, finish_own)
    each_part(0, parts, finish_others)

    for copy, sends, _ in straight + corners:
        pl.when(sends)(copy.wait_send)
    for k in range(chips):
        low, high = s - 2 * k, s + 2 * k

        def weight_sent(p):
            pl.when((low >= 0) & (s + 2 < ns))(near(k, low, 0, p, k == 0).wait_send)
            pl.when((high < ns) & (s >= 2))(near(k, high, 1, p, k == 0).wait_send)
            pl.when(low >= 0)(pair(k, low, 0, p, k == 0).wait_send)
            if k > 0:
                pl.when(high < ns)(pair(k, high, 1, p, False).wait_send)

        each_part(0, parts, weight_sent)

    def sent(g, carry):
        for d in range(1, nt):
            gather(g, d).wait_send()
        return carry

    lax.fori_loop(0, groups, sent, 0)

    def back_sent(p):
        for d in range(1, nt):
            back(d, p).wait_send()

    each_part(0, parts, back_sent)


def ring_shards(
    hidden_in,
    queries,
    keys,
    values,
    query_gain,
    key_gain,
    reach_time,
    reach_rows,
    reach_cols,
    out_weight,
    gate,
):
    frames, rows, columns, inner = queries.shape
    width = hidden_in.shape[3]
    heads = reach_time.shape[0]
    tokens = frames * rows * columns
    nt, ns = lax.axis_size("tm"), lax.axis_size("space")
    depth, cols = out_weight.shape
    group = 5 if heads % 5 == 0 else 1
    vmem = pl.BlockSpec(memory_space=pltpu.VMEM)
    hbm = pl.BlockSpec(memory_space=pl.ANY)
    dma = pltpu.SemaphoreType.DMA
    lane = 256 if cols % 256 == 0 else 128
    parts = cols // lane
    output = pl.pallas_call(
        functools.partial(ring_kernel, heads, group),
        out_shape=jax.ShapeDtypeStruct((tokens, width), jnp.bfloat16),
        in_specs=[pl.BlockSpec(memory_space=pltpu.SMEM)] * 3 + [vmem] * 7 + [hbm] * 3,
        out_specs=vmem,
        scratch_shapes=[
            pltpu.VMEM((tokens, inner), jnp.bfloat16),
            pltpu.VMEM((len(REACHES), tokens, (frames + 2) * (rows + 2) * columns), jnp.float32),
            pltpu.VMEM((tokens, width), jnp.bfloat16),
            pltpu.VMEM((2, frames + 2, rows + 2, columns, inner), jnp.bfloat16),
            pltpu.VMEM((parts, depth * ns, lane), jnp.bfloat16),
            pltpu.VMEM((nt, tokens, inner), jnp.bfloat16),
            pltpu.VMEM((parts, nt * tokens, lane), jnp.float32),
            pltpu.VMEM((nt - 1, parts, tokens, lane), jnp.bfloat16),
            pltpu.VMEM((nt - 1, parts, tokens, lane), jnp.bfloat16),
            dma((2,)),
            dma((parts,)),
            dma((12,)),
            dma((12,)),
            dma((2, ns // 2, parts)),
            dma((2, ns // 2, parts)),
            dma((ns, parts)),
            dma((nt - 1, heads // group)),
            dma((nt, heads // group)),
            dma((nt - 1, parts)),
            dma((nt - 1, parts)),
        ],
        compiler_params=pltpu.CompilerParams(
            has_side_effects=True, vmem_limit_bytes=60 * 1024 * 1024
        ),
    )(
        reach_time,
        reach_rows,
        reach_cols,
        queries.reshape(tokens, inner),
        keys,
        query_gain.reshape(1, inner),
        key_gain.reshape(1, inner),
        places(frames, rows, columns, 0).T,
        places(frames, rows, columns, 1),
        gate.reshape(1, width),
        values,
        out_weight,
        hidden_in.reshape(tokens, width),
    )
    return output.reshape(frames, rows, columns, width)


def pair_kernel(
    heads,
    time_ref,
    rows_ref,
    cols_ref,
    query_gain_ref,
    key_gain_ref,
    query_place_ref,
    key_place_ref,
    gate_ref,
    raw_query_ref,
    raw_key_ref,
    value_ref,
    weight_ref,
    hidden_in_ref,
    out_ref,
    raw,
    normed,
    region,
    query_ref,
    mask_ref,
    mixed,
    weights,
    total,
    partial_out,
    partial_in,
    outgoing,
    incoming,
    hidden_ref,
    result_ref,
    staged,
    local_sem,
    value_sem,
    own_sem,
    swap_send,
    swap_recv,
    side_send,
    side_recv,
    corner_send,
    corner_recv,
    stage_recv,
    near_send,
    cross_send,
    pair_send,
    weight_recv,
    level_send,
    level_recv,
    mixed_send,
    mixed_recv,
    part_send,
    part_recv,
    back_send,
    back_recv,
    out_sem,
):
    t = lax.axis_index("tm")
    s = lax.axis_index("space")
    nt = lax.axis_size("tm")
    ns = lax.axis_size("space")
    frames, rows, columns, inner = value_ref.shape
    tokens = frames * rows * columns
    depth, cols = weight_ref.shape
    width = inner // heads
    groups = ns // 2
    half = inner // 2
    blocks, parts, _, lane = weights.shape
    chips = ns // 4
    row_tokens = rows * columns
    span = 2 * frames

    p = lax.rem(t, 2)
    column_block = lax.div(t, 2)
    c = lax.rem(s, 2)
    z = lax.div(s, 2)
    level = lax.rem(z, 2)
    chip = lax.div(z, 2)
    mate = t + 1 - 2 * p
    partner = s + 1 - 2 * c
    level_mate = s + 2 - 4 * level

    has_low_t, has_high_t = t >= 2, t < nt - 2
    has_low_s, has_high_s = s > 0, s < ns - 1

    def remote(source, target, send, recv, tm, space):
        return pltpu.make_async_remote_copy(
            src_ref=source,
            dst_ref=target,
            send_sem=send,
            recv_sem=recv,
            device_id=(tm, space),
            device_id_type=pl.DeviceIdType.MESH,
        )

    def lanes_at(start, size):
        return pl.ds(pl.multiple_of(start, 128), size)

    def other_column(e):
        return lax.rem(column_block + e, blocks)

    def other_chip(d):
        return lax.rem(chip + d, chips)

    def column_device(e):
        return 2 * other_column(e) + p

    def chip_device(d):
        return 4 * other_chip(d) + 2 * level + c

    levels = 2 * chips
    middle = levels // 2

    def comes_late(d):
        rises = other_chip(d) < chip
        return (rises & (z <= middle)) | (jnp.logical_not(rises) & (z + 1 >= middle))

    starts = {True: z + 2 < levels, False: z >= 2}
    passes = {True: (z >= 1) & (z + 1 < levels), False: (z + 1 < levels) & (z >= 1)}
    inner = {True: z < middle, False: z >= middle}

    load_key = pltpu.make_async_copy(raw_key_ref, raw.at[0], local_sem.at[0])
    load_key.start()
    load_query = pltpu.make_async_copy(raw_query_ref, raw.at[1], local_sem.at[1])
    load_query.start()

    barrier = pltpu.get_barrier_semaphore()

    def greet(tm, space):
        pl.semaphore_signal(
            barrier, inc=1, device_id=(tm, space), device_id_type=pl.DeviceIdType.MESH
        )

    greet(mate, s)
    greet(t, partner)
    greet(t, level_mate)
    for e in range(1, blocks):
        greet(column_device(e), s)
    across = s - 2 + 4 * level
    has_across = (across >= 0) & (across < ns)
    pl.when(has_across)(functools.partial(greet, t, across))
    up, down = (c == 1) & has_high_s, (c == 0) & has_low_s

    @pl.when(up)
    def _():
        greet(t, s + 1)

    @pl.when(down)
    def _():
        greet(t, s - 1)

    pl.semaphore_wait(
        barrier, blocks + 2 + has_across.astype(jnp.int32) + (up | down).astype(jnp.int32)
    )

    own_frames = pl.ds(1 + frames * p, frames)
    own_rows = pl.ds(1, rows)

    def group_lanes(b):
        return pl.ds(b * depth, depth)

    def value_swap(b):
        source = value_ref.at[:, :, :, lanes_at((2 * b + 1 - p) * depth, depth)]
        target = region.at[1, own_frames, own_rows, :, group_lanes(b)]
        return remote(source, target, swap_send.at[1, b], swap_recv.at[1, b], mate, s)

    def key_swap(b):
        source = normed.at[0, 1 - p, :, :, :, group_lanes(b)]
        target = region.at[0, own_frames, own_rows, :, group_lanes(b)]
        return remote(source, target, swap_send.at[0, b], swap_recv.at[0, b], mate, s)

    def query_swap(b):
        source = normed.at[1, 1 - p, :, :, :, group_lanes(b)]
        target = query_ref.at[pl.ds(frames * p, frames), :, :, group_lanes(b)]
        return remote(source, target, swap_send.at[2, b], swap_recv.at[2, b], mate, s)

    def own_value(b):
        return pltpu.make_async_copy(
            value_ref.at[:, :, :, lanes_at((2 * b + p) * depth, depth)],
            region.at[1, own_frames, own_rows, :, group_lanes(b)],
            value_sem.at[b],
        )

    def own_weight(q):
        return weight_ref.at[:, pl.ds(q * lane, lane)]

    def own_weight_at(q):
        return weight_ref.at[:, lanes_at(q * lane, lane)]

    def weight_block(block, chip_index, core, q):
        start = (2 * chip_index + core) * depth
        return weights.at[block, q, pl.ds(pl.multiple_of(start, depth), depth)]

    def arrival(chip_index, core):
        return 2 * chip_index + core

    def keep_weight(q):
        return pltpu.make_async_copy(
            own_weight_at(q), weight_block(column_block, chip, c, q), own_sem.at[q]
        )

    def shares(q, d=1):
        return range(2 if d > 0 and q == parts - 1 else 1)

    def rows_of(q, k, d=1):
        count = len(shares(q, d))
        return pl.ds(k * (depth // count), depth // count)

    def first_hop(rising, q, k):
        at = rows_of(q, k)
        return remote(
            own_weight_at(q).at[at], staged.at[int(rising), q, at],
            near_send.at[0, int(rising), q + k], stage_recv.at[int(rising), q + k],
            t, s + 2 if rising else s - 2,
        )

    def second_hop(rising, q, k):
        origin = lax.div(z + levels - 1 if rising else z + levels + 1, 2) - chips
        at = rows_of(q, k)
        return remote(
            staged.at[int(rising), q, at], weight_block(column_block, origin, c, q).at[at],
            near_send.at[1, int(rising), q + k],
            weight_recv.at[column_block, arrival(origin, c), q + k],
            t, s + 2 if rising else s - 2,
        )

    def cross_weight(e, d, q, k):
        at = rows_of(q, k, d)
        block = weight_block(column_block, other_chip(d), c, q).at[at]
        source = own_weight_at(q).at[at] if d == 0 else block
        return remote(
            source, block, cross_send.at[e - 1, d, q + k],
            weight_recv.at[column_block, arrival(other_chip(d), c), q + k],
            column_device(e), s,
        )

    def pair_weight(e, d, q, k):
        at = rows_of(q, k, d)
        block = weight_block(other_column(e), other_chip(d), c, q).at[at]
        source = own_weight_at(q).at[at] if e == 0 and d == 0 else block
        return remote(
            source, block, pair_send.at[e, d, q + k],
            weight_recv.at[other_column(e), arrival(other_chip(d), c), q + k],
            t, partner,
        )

    def weight_here(e, d, core, q, k):
        block = weight_block(other_column(e), other_chip(d), core, q).at[rows_of(q, k, d)]
        remote(
            block, block, pair_send.at[e, d, q + k],
            weight_recv.at[other_column(e), arrival(other_chip(d), core), q + k], t, partner,
        ).wait_recv()

    at_end = (z == 0) | (z == levels - 1)

    def send_far(q, ends, which=True):
        for rising in (True, False):
            for k in shares(q):
                pl.when(starts[rising] & (at_end == ends) & which)(first_hop(rising, q, k).start)

    def forward(q, inward, which=True):
        for rising in (True, False):
            @pl.when(passes[rising] & (inner[rising] == inward) & which)
            def _(rising=rising):
                for k in shares(q):
                    first_hop(rising, q, k).wait_recv()
                    second_hop(rising, q, k).start()

    def send_cross(q):
        for e in range(1, blocks):
            cross_weight(e, 0, q, 0).start()
        pair_weight(0, 0, q, 0).start()

    def relay_far(q, late):
        for d in range(1, chips):
            @pl.when(comes_late(d) if late else jnp.logical_not(comes_late(d)))
            def _(d=d):
                for k in shares(q):
                    weight_here(0, d, c, q, k)
                    for e in range(1, blocks):
                        cross_weight(e, d, q, k).start()
                    pair_weight(0, d, q, k).start()

    def relay_cross(q, far):
        for e in range(1, blocks):
            for d in range(1, chips) if far else (0,):
                for k in shares(q, d):
                    weight_here(e, d, c, q, k)
                    pair_weight(e, d, q, k).start()

    value_swap(0).start()
    for b in range(groups):
        own_value(b).start()
    send_far(0, True)
    send_far(0, False)
    send_far(1, False)
    send_far(1, True)
    send_cross(0)
    for q in range(parts):
        keep_weight(q).start()
    own_hidden = pltpu.make_async_copy(hidden_in_ref, hidden_ref, local_sem.at[2])
    own_hidden.start()

    step = 16 if columns % 16 == 0 else columns

    def normalize(index, gain_ref):
        for frame in range(frames):
            for row in range(rows):
                for column in range(0, columns, step):
                    at = slice(column, column + step)
                    result = normalized(raw[index, frame, row, at], gain_ref[...])
                    for b in range(groups):
                        for core in range(2):
                            start = (2 * b + core) * depth
                            normed[index, core, frame, row, at, b * depth:(b + 1) * depth] = (
                                result[:, start:start + depth]
                            )

    load_key.wait()
    with jax.named_scope("normalize_key"):
        normalize(0, key_gain_ref)
    key_swap(0).start()
    own_key = pltpu.make_async_copy(
        normed.at[0, p], region.at[0, own_frames, own_rows], local_sem.at[3]
    )
    own_key.start()
    load_query.wait()
    with jax.named_scope("normalize_query"):
        normalize(1, query_gain_ref)
    query_swap(0).start()
    own_query = pltpu.make_async_copy(
        normed.at[1, p], query_ref.at[pl.ds(frames * p, frames)], local_sem.at[4]
    )
    own_query.start()
    for b in range(1, groups):
        value_swap(b).start()
        key_swap(b).start()
        query_swap(b).start()

    def clear_frame(frame):
        def run():
            for part in range(2):
                for row in range(rows + 2):
                    region[part, frame, row] = jnp.zeros((columns, half), jnp.bfloat16)
        return run

    def clear_row(row):
        def run():
            for part in range(2):
                for frame in range(span + 2):
                    region[part, frame, row] = jnp.zeros((columns, half), jnp.bfloat16)
        return run

    pl.when(jnp.logical_not(has_low_t))(clear_frame(0))
    pl.when(jnp.logical_not(has_high_t))(clear_frame(span + 1))
    pl.when(jnp.logical_not(has_low_s))(clear_row(0))
    pl.when(jnp.logical_not(has_high_s))(clear_row(rows + 1))

    frame_k, row_k, tile_k = key_place_ref[0:1], key_place_ref[1:2], key_place_ref[2:3]
    inside = (row_k >= -s * rows) & (row_k < (ns - s) * rows)
    row_gap = jnp.abs(query_place_ref[:, 0:1] - row_k) + jnp.where(inside, 0, 9)
    tile_gap = jnp.abs(query_place_ref[:, 1:2] - tile_k)
    low_gap = jnp.where(has_low_t, 0, 9) * (frame_k < 0).astype(jnp.int32)
    high_gap = jnp.where(has_high_t, 0, 9) * (frame_k > 0).astype(jnp.int32)
    for kind, edge in enumerate((jnp.zeros_like(low_gap), low_gap, high_gap)):
        frame_gap = jnp.abs(frame_k) + edge
        for i, (reach_t, reach_r, reach_c) in enumerate(REACHES):
            allowed = (frame_gap <= reach_t) & (row_gap <= reach_r) & (tile_gap <= reach_c)
            mask_ref[kind, i] = jnp.where(allowed, 0.0, -1e30)

    pair_frames = pl.ds(1, span)

    def row_up(b):
        return remote(
            region.at[:, pair_frames, rows, :, group_lanes(b)],
            region.at[:, pair_frames, 0, :, group_lanes(b)],
            side_send.at[0, b], side_recv.at[0, b], t, s + 1,
        )

    def row_down(b):
        return remote(
            region.at[:, pair_frames, 1, :, group_lanes(b)],
            region.at[:, pair_frames, rows + 1, :, group_lanes(b)],
            side_send.at[1, b], side_recv.at[1, b], t, s - 1,
        )

    def frame_up(b):
        return remote(
            region.at[:, span, own_rows, :, group_lanes(b)],
            region.at[:, 0, own_rows, :, group_lanes(b)],
            side_send.at[2, b], side_recv.at[2, b], t + 2, s,
        )

    def frame_down(b):
        return remote(
            region.at[:, 1, own_rows, :, group_lanes(b)],
            region.at[:, span + 1, own_rows, :, group_lanes(b)],
            side_send.at[3, b], side_recv.at[3, b], t - 2, s,
        )

    def sides(b):
        return (
            (frame_up(b), has_high_t, has_low_t),
            (frame_down(b), has_low_t, has_high_t),
            (row_up(b), has_high_s, has_low_s),
            (row_down(b), has_low_s, has_high_s),
        )

    def corners(b):
        result = []
        for i, (frame, has_frame) in enumerate(((0, has_low_t), (span + 1, has_high_t))):
            for j, (row, landing, space, sends, receives) in enumerate((
                (rows, 0, s + 1, has_high_s, has_low_s),
                (1, rows + 1, s - 1, has_low_s, has_high_s),
            )):
                copy = remote(
                    region.at[:, frame, row, :, group_lanes(b)],
                    region.at[:, frame, landing, :, group_lanes(b)],
                    corner_send.at[2 * i + j, b], corner_recv.at[2 * i + j, b], t, space,
                )
                result.append((copy, has_frame & sends, has_frame & receives))
        return result

    def feature_lanes(index, core):
        return lanes_at((2 * index + core) * depth, depth)

    def to_level_mate(j):
        at = (slice(None), feature_lanes(j, p))
        return remote(
            mixed.at[(2,) + at], mixed.at[(level,) + at],
            level_send.at[j], level_recv.at[j], t, level_mate,
        )

    def from_level_mate(j):
        at = (1 - level, slice(None), feature_lanes(j, p))
        return remote(mixed.at[at], mixed.at[at], level_send.at[j], level_recv.at[j], t, level_mate)

    def to_mate(which, j):
        at = (which, slice(None), feature_lanes(j, p))
        return remote(
            mixed.at[at], mixed.at[at], mixed_send.at[which, j], mixed_recv.at[which, j], mate, s
        )

    def from_mate(which, j):
        at = (which, slice(None), feature_lanes(j, 1 - p))
        remote(
            mixed.at[at], mixed.at[at], mixed_send.at[which, j], mixed_recv.at[which, j], mate, s
        ).wait_recv()

    def attend(b):
        in_level = level == b % 2
        place = jnp.where(in_level, level, 2)
        index = b // 2
        group = depth // width

        def one_head(i, carry):
            h = (2 * b + p) * group + i
            lanes = lanes_at(b * depth + i * width, width)
            reach = time_ref[h] * 6 + rows_ref[h] * 3 + cols_ref[h]
            target = lanes_at((2 * index + p) * depth + i * width, width)
            scores, values = [], []
            for frame in range(span):
                query = query_ref[frame, :, :, lanes].reshape(row_tokens, width)
                near = slice(frame, frame + 3)
                key = region[0, near, :, :, lanes].reshape(-1, width)
                values.append(region[1, near, :, :, lanes].reshape(-1, width))
                scores.append(lax.dot_general(
                    query, key, (((1,), (1,)), ((), ())), preferred_element_type=jnp.float32
                ))
            results = []
            for frame in range(span):
                kind = 1 if frame == 0 else 2 if frame == span - 1 else 0
                masked = scores[frame] * width ** (-0.5) + mask_ref[kind, reach]
                part = jnp.exp(masked - jnp.max(masked, axis=1, keepdims=True))
                sums = jnp.sum(part, axis=1, keepdims=True)
                result = jnp.dot(
                    part.astype(jnp.bfloat16), values[frame], preferred_element_type=jnp.float32
                )
                results.append((result / sums).astype(jnp.bfloat16))
            mixed[place, :, target] = jnp.concatenate(results, axis=0)
            return carry

        lax.fori_loop(0, group, one_head, 0)

    def send_mixed(b):
        pl.when(level != b % 2)(to_level_mate(b // 2).start)

    def relay_mixed(b):
        @pl.when(level == b % 2)
        def _():
            from_level_mate(b // 2).wait_recv()
            to_mate(1 - level, b // 2).start()
            to_mate(level, b // 2).start()

    def arrive(i):
        with jax.named_scope(f"wait_swap{i}"):
            value_swap(i).wait_recv()
            key_swap(i).wait_recv()
            own_value(i).wait()
            if i == 0:
                own_key.wait()
        with jax.named_scope(f"send_sides{i}"):
            for copy, sends, _ in sides(i):
                pl.when(sends)(copy.start)

    def turn(i):
        with jax.named_scope(f"wait_frames{i}"):
            for copy, _, receives in sides(i)[:2]:
                pl.when(receives)(copy.wait_recv)
        for copy, sends, _ in corners(i):
            pl.when(sends)(copy.start)

    def ready(b):
        with jax.named_scope(f"wait_query{b}"):
            query_swap(b).wait_recv()
            if b == 0:
                own_query.wait()
        with jax.named_scope(f"wait_rows{b}"):
            for copy, _, receives in sides(b)[2:]:
                pl.when(receives)(copy.wait_recv)
        with jax.named_scope(f"wait_corners{b}"):
            for copy, _, receives in corners(b):
                pl.when(receives)(copy.wait_recv)

    early = min(2, parts)
    actions = {
        "end": lambda q: send_far(q, True),
        "end0": lambda q: send_far(q, True, level == 0),
        "end1": lambda q: send_far(q, True, level == 1),
        "out0": lambda q: forward(q, False, level == 0),
        "out1": lambda q: forward(q, False, level == 1),
        "mid": lambda q: send_far(q, False),
        "late": lambda q: relay_far(q, True),
        "cross": send_cross,
        "out": lambda q: forward(q, False),
        "in": lambda q: forward(q, True),
        "early": lambda q: relay_far(q, False),
    }
    plan = {i: [] for i in range(groups + 1)}
    plan[0] += [("mid", 2), ("cross", 1), ("out", 0)]
    plan[1] += [("mid", 3), ("end0", 2), ("cross", 2), ("out0", 1)]
    plan[2] += [("end1", 2), ("cross", 3), ("out1", 1)]
    plan[3] += [("in", 0), ("mid", 4), ("end0", 3), ("out0", 2), ("cross", 4), ("early", 0), ("early", 1)]
    plan[groups] += [("in", 1), ("end1", 3), ("end", 4), ("out1", 2), ("out", 3), ("late", 0)]
    plan[groups] += [("cross", q) for q in range(5, parts)]
    for i in range(groups + 1):
        if i < groups:
            arrive(i)
        if i > 0:
            ready(i - 1)
            with jax.named_scope(f"attend{i - 1}"):
                attend(i - 1)
        if i < groups:
            turn(i)
        if i > 0:
            send_mixed(i - 1)
        for kind, q in plan[i]:
            if q < parts:
                actions[kind](q)
        if i > 1:
            with jax.named_scope(f"relay_mixed{i}"):
                relay_mixed(i - 2)
        if i > 1 and i - 2 < parts:
            with jax.named_scope(f"relay_cross{i}"):
                relay_cross(i - 2, False)
    with jax.named_scope("relay_mixed_last"):
        relay_mixed(groups - 1)

    def each_part(low, high, run):
        def body(q, carry):
            run(q)
            return carry

        lax.fori_loop(low, high, body, 0)

    def next_far(q):
        if q < parts:
            with jax.named_scope(f"relay_far{q}"):
                relay_far(q, True)

    def multiply_theirs(e, q):
        block = other_column(e)
        for d in range(chips):
            for k in shares(q, d):
                weight_here(e, d, 1 - c, q, k)
        product = jnp.dot(
            mixed[1 - level], weights[block, q], preferred_element_type=jnp.float32
        )
        partial_out[block, q] = product.astype(jnp.bfloat16)
        part_copy(block, q).start()

    def multiply_ours(e, q):
        block = other_column(e)
        total[block, q] = jnp.dot(
            mixed[level], weights[block, q], preferred_element_type=jnp.float32
        )

    def part_copy(block, q):
        return remote(
            partial_out.at[block, q], partial_in.at[block, q],
            part_send.at[block, q], part_recv.at[block, q], t, level_mate,
        )

    def back(block, q):
        return remote(
            outgoing.at[block, q], incoming.at[block, q],
            back_send.at[block, q], back_recv.at[block, q], mate, s,
        )

    def token_rows(side):
        return pl.ds(pl.multiple_of(side * tokens, tokens), tokens)

    def finish(column, branch, index, q):
        lanes = lanes_at(column, lane)
        result_ref[:, lanes] = (
            hidden_ref[:, lanes].astype(jnp.float32) + gate_ref[:, lanes] * branch
        ).astype(jnp.bfloat16)
        write_out(column, index, q).start()

    def write_out(column, index, q):
        lanes = lanes_at(column, lane)
        return pltpu.make_async_copy(
            result_ref.at[:, lanes], out_ref.at[:, lanes], out_sem.at[index, q]
        )

    def reduce_part(q):
        for e in range(blocks):
            block = other_column(e)
            part_copy(block, q).wait_recv()
            theirs = token_rows(1 - p)
            outgoing[block, q] = (
                total[block, q, theirs] + partial_in[block, q, theirs].astype(jnp.float32)
            ).astype(jnp.bfloat16)
            back(block, q).start()
            ours = token_rows(p)
            branch = total[block, q, ours] + partial_in[block, q, ours].astype(jnp.float32)
            finish((2 * block + p) * cols + q * lane, branch, 2 * block + p, q)

    def theirs(q):
        if q >= groups - 1:
            relay_cross(q, False)
        keep_weight(q).wait()
        with jax.named_scope(f"theirs{q}own"):
            multiply_theirs(0, q)
        if blocks > 1:
            with jax.named_scope(f"main_cross{q}"):
                relay_cross(q, True)
            with jax.named_scope(f"theirs{q}other"):
                for e in range(1, blocks):
                    multiply_theirs(e, q)

    def ours(q):
        with jax.named_scope(f"ours{q}"):
            for e in range(blocks):
                multiply_ours(e, q)

    forward(2, True)
    relay_far(2, False)
    forward(4, False)
    forward(3, True)
    relay_far(3, False)
    next_far(1)
    with jax.named_scope("from_mate_theirs"):
        for j in range(groups // 2):
            from_mate(1 - level, j)
    theirs(0)
    forward(4, True)
    next_far(2)
    theirs(1)
    relay_far(4, False)
    with jax.named_scope("from_mate_ours"):
        for j in range(groups // 2):
            from_mate(level, j)
    ours(0)
    own_hidden.wait()
    next_far(3)
    theirs(2)
    next_far(4)
    ours(1)
    with jax.named_scope("reduce01"):
        reduce_part(0)
        reduce_part(1)
    theirs(3)
    ours(2)
    ours(3)
    with jax.named_scope("reduce2"):
        reduce_part(2)
    with jax.named_scope("reduce3a"):
        pl.when(jnp.logical_not(at_end))(functools.partial(reduce_part, 3))
    theirs(4)
    ours(4)

    def finish_others(q):
        for block in range(blocks):
            back(block, q).wait_recv()
            finish(
                (2 * block + 1 - p) * cols + q * lane,
                incoming[block, q].astype(jnp.float32), 2 * block + 1 - p, q,
            )

    with jax.named_scope("reduce3b"):
        pl.when(at_end)(functools.partial(reduce_part, 3))
    with jax.named_scope("finish01"):
        each_part(0, 2, finish_others)
    with jax.named_scope("reduce4"):
        reduce_part(4)
    with jax.named_scope("finish2"):
        each_part(2, parts, finish_others)

    for b in range(groups):
        value_swap(b).wait_send()
        key_swap(b).wait_send()
        query_swap(b).wait_send()
        for copy, sends, _ in sides(b) + tuple(corners(b)):
            pl.when(sends)(copy.wait_send)
    for j in range(groups // 2):
        to_level_mate(j).wait_send()
        for which in range(2):
            to_mate(which, j).wait_send()

    def weight_sent(q):
        for k in shares(q):
            for rising in (True, False):
                pl.when(starts[rising])(first_hop(rising, q, k).wait_send)
                pl.when(passes[rising])(second_hop(rising, q, k).wait_send)
        for e in range(blocks):
            for d in range(chips):
                for k in shares(q, d):
                    pair_weight(e, d, q, k).wait_send()
                    if e > 0:
                        cross_weight(e, d, q, k).wait_send()

    for q in range(parts):
        weight_sent(q)

    def sent(q):
        for block in range(blocks):
            part_copy(block, q).wait_send()
            back(block, q).wait_send()
        for index in range(nt):
            write_out(index * cols + q * lane, index, q).wait()

    each_part(0, parts, sent)


def pair_shards(
    hidden_in,
    queries,
    keys,
    values,
    query_gain,
    key_gain,
    reach_time,
    reach_rows,
    reach_cols,
    out_weight,
    gate,
):
    frames, rows, columns, inner = queries.shape
    width = hidden_in.shape[3]
    heads = reach_time.shape[0]
    tokens = frames * rows * columns
    nt, ns = lax.axis_size("tm"), lax.axis_size("space")
    depth, cols = out_weight.shape
    lane = 256 if cols % 256 == 0 else 128
    parts = cols // lane
    blocks, chips, groups = nt // 2, ns // 4, ns // 2
    half = inner // 2
    pair_tokens = 2 * tokens
    vmem = pl.BlockSpec(memory_space=pltpu.VMEM)
    hbm = pl.BlockSpec(memory_space=pl.ANY)
    dma = pltpu.SemaphoreType.DMA
    _, query_row, query_tile = places(1, rows, columns, 0)
    key_place = np.stack([axis.reshape(-1) for axis in np.meshgrid(
        np.arange(-1, 2), np.arange(-1, rows + 1), np.arange(columns) // TW, indexing="ij"
    )]).astype(np.int32)
    output = pl.pallas_call(
        functools.partial(pair_kernel, heads),
        out_shape=jax.ShapeDtypeStruct((tokens, width), jnp.bfloat16),
        in_specs=[pl.BlockSpec(memory_space=pltpu.SMEM)] * 3 + [vmem] * 5 + [hbm] * 5,
        out_specs=hbm,
        scratch_shapes=[
            pltpu.VMEM((2, frames, rows, columns, inner), jnp.bfloat16),
            pltpu.VMEM((2, 2, frames, rows, columns, half), jnp.bfloat16),
            pltpu.VMEM((2, 2 * frames + 2, rows + 2, columns, half), jnp.bfloat16),
            pltpu.VMEM((2 * frames, rows, columns, half), jnp.bfloat16),
            pltpu.VMEM((3, len(REACHES), rows * columns, 3 * (rows + 2) * columns), jnp.float32),
            pltpu.VMEM((3, pair_tokens, half), jnp.bfloat16),
            pltpu.VMEM((blocks, parts, half, lane), jnp.bfloat16),
            pltpu.VMEM((blocks, parts, pair_tokens, lane), jnp.float32),
            pltpu.VMEM((blocks, parts, pair_tokens, lane), jnp.bfloat16),
            pltpu.VMEM((blocks, parts, pair_tokens, lane), jnp.bfloat16),
            pltpu.VMEM((blocks, parts, tokens, lane), jnp.bfloat16),
            pltpu.VMEM((blocks, parts, tokens, lane), jnp.bfloat16),
            pltpu.VMEM((tokens, width), jnp.bfloat16),
            pltpu.VMEM((tokens, width), jnp.bfloat16),
            pltpu.VMEM((2, parts, depth, lane), jnp.bfloat16),
            dma((5,)),
            dma((groups,)),
            dma((parts,)),
            dma((3, groups)),
            dma((3, groups)),
            dma((4, groups)),
            dma((4, groups)),
            dma((4, groups)),
            dma((4, groups)),
            dma((2, parts + 1)),
            dma((2, 2, parts + 1)),
            dma((max(blocks - 1, 1), chips, parts + 1)),
            dma((blocks, chips, parts + 1)),
            dma((blocks, 2 * chips, parts + 1)),
            dma((groups // 2,)),
            dma((groups // 2,)),
            dma((2, groups // 2)),
            dma((2, groups // 2)),
            dma((blocks, parts)),
            dma((blocks, parts)),
            dma((blocks, parts)),
            dma((blocks, parts)),
            dma((nt, parts)),
        ],
        compiler_params=pltpu.CompilerParams(
            collective_id=0, has_side_effects=True, vmem_limit_bytes=60 * 1024 * 1024
        ),
    )(
        reach_time,
        reach_rows,
        reach_cols,
        query_gain.reshape(1, inner),
        key_gain.reshape(1, inner),
        np.stack([query_row, query_tile]).T,
        key_place,
        gate.reshape(1, width),
        queries,
        keys,
        values,
        out_weight,
        hidden_in.reshape(tokens, width),
    )
    return output.reshape(frames, rows, columns, width)


def shards(hidden_in, queries, keys, values, *others):
    out_weight, reach_time = others[-2], others[2]
    width = queries.shape[3] // reach_time.shape[0]
    nt, ns = lax.axis_size("tm"), lax.axis_size("space")
    whole_heads = out_weight.shape[0] % width == 0
    form = pair_shards if whole_heads and nt % 2 == 0 and ns // 4 == 2 else ring_shards
    return form(hidden_in, queries, keys, values, *others)


def solution(mesh):
    in_specs = (
        P("tm", "space", None, None),
        P("tm", "space", None, None),
        P("tm", "space", None, None),
        P("tm", "space", None, None),
        P(),
        P(),
        P(),
        P(),
        P(),
        P("space", "tm"),
        P(),
    )
    out_specs = P("tm", "space", None, None)
    return jax.shard_map(shards, mesh=mesh, in_specs=in_specs, out_specs=out_specs, check_vma=False)
```
